8 devices in a mesh: slab: 1 (over z), coil: 2 (over y), rows: 4 (over x, core).
Axes of the slice: x: 2, y: 2, z: 1, core: 2. Of those that a mesh axis runs over, the one named last changes fastest.
Arguments:
- kspace: float32 [2, 8, 8192], P(None, 'coil', ('slab', 'rows'))
- weight_row: float32 [6, 8192], P(None, ('slab', 'rows'))
- weight_col: float32 [6, 8192], P(None, ('slab', 'rows'))
- grid_row: int32 [8192], P(('slab', 'rows'))
- grid_col: int32 [8192], P(('slab', 'rows'))
- valid_count: int32 [4], P(('slab', 'rows'))
- coil_maps: float32 [2, 8, 512, 512], P(None, 'coil', 'slab', 'rows')
- deapod: float32 [512], replicated
Outputs:
- output: float32 [2, 512, 512], P(None, ('slab', 'coil'), 'rows')
All inputs are finite; a program needn't handle non-finite values.
Results may differ from the reference program's by a relative error of at most 0.001.
Values are sent between devices in bfloat16 or wider.
A program may use at most 1 GiB of HBM per device.

```python
import math
import jax
import jax.numpy as jnp
from jax import lax

IMAGE_SIZE = 512
KERNEL_WIDTH = 6
NUM_COILS = 8
ROW_BLOCKS = 4
PER_BLOCK = 2048

GRID_SIZE = 2 * IMAGE_SIZE
HALF_WIDTH = KERNEL_WIDTH // 2
BLOCK_ROWS = GRID_SIZE // ROW_BLOCKS
SAMPLES = ROW_BLOCKS * PER_BLOCK


def draw_layout(layout_key):
    key_count, key_short, key_ra, key_rb, key_ca, key_cb, key_sign = jax.random.split(layout_key, 7)
    blocks = jnp.arange(ROW_BLOCKS)
    centre_block = ROW_BLOCKS // 2
    low_counts = jax.random.randint(key_count, (ROW_BLOCKS,), PER_BLOCK // 8, PER_BLOCK // 2 + 1)
    short_by = jax.random.randint(key_short, (), 0, PER_BLOCK // 4 + 1)
    counts = jnp.where(blocks == centre_block, PER_BLOCK, jnp.where(blocks == centre_block - 1, PER_BLOCK - short_by, low_counts))
    row_depth = (jax.random.randint(key_ra, (ROW_BLOCKS, PER_BLOCK), 0, BLOCK_ROWS) * jax.random.randint(key_rb, (ROW_BLOCKS, PER_BLOCK), 0, BLOCK_ROWS)) // BLOCK_ROWS
    upper_half = blocks >= centre_block
    edge_row = jnp.where(upper_half, blocks * BLOCK_ROWS, (blocks + 1) * BLOCK_ROWS - 1)
    direction = jnp.where(upper_half, 1, -1)
    grid_row = (edge_row[:, None] + direction[:, None] * row_depth).reshape(SAMPLES)
    spread_col = (jax.random.randint(key_ca, (SAMPLES,), 0, IMAGE_SIZE) * jax.random.randint(key_cb, (SAMPLES,), 0, IMAGE_SIZE)) // IMAGE_SIZE
    col_sign = 2 * jax.random.randint(key_sign, (SAMPLES,), 0, 2) - 1
    grid_col = jnp.mod(IMAGE_SIZE + col_sign * spread_col, GRID_SIZE)
    return counts.astype(jnp.int32), grid_row.astype(jnp.int32), grid_col.astype(jnp.int32)


def kernel_weights(weight_key):
    tap_pos = jnp.arange(KERNEL_WIDTH, dtype=jnp.float32) - (KERNEL_WIDTH - 1) / 2.0
    profile = jnp.exp(-(tap_pos / (0.35 * KERNEL_WIDTH)) ** 2)
    jitter = jax.random.uniform(weight_key, (KERNEL_WIDTH, SAMPLES), jnp.float32, 0.5, 1.5)
    return (profile / jnp.sum(profile))[:, None] * jitter


def draw_maps(map_key):
    key_angle, key_phase, key_grad_y, key_grad_x, key_noise = jax.random.split(map_key, 5)
    pixel_pos = (jnp.arange(IMAGE_SIZE, dtype=jnp.float32) - IMAGE_SIZE // 2) / IMAGE_SIZE
    coil_angle = 2.0 * math.pi * (jnp.arange(NUM_COILS, dtype=jnp.float32) + jax.random.uniform(key_angle, (NUM_COILS,), jnp.float32)) / NUM_COILS
    centre_y = 0.6 * jnp.cos(coil_angle)
    centre_x = 0.6 * jnp.sin(coil_angle)
    dist_sq = (pixel_pos[None, :, None] - centre_y[:, None, None]) ** 2 + (pixel_pos[None, None, :] - centre_x[:, None, None]) ** 2
    magnitude = jnp.exp(-dist_sq / 0.4) * (1.0 + 0.1 * jax.random.normal(key_noise, (NUM_COILS, IMAGE_SIZE, IMAGE_SIZE), jnp.float32))
    grad_y = jax.random.uniform(key_grad_y, (NUM_COILS,), jnp.float32, -1.0, 1.0)
    grad_x = jax.random.uniform(key_grad_x, (NUM_COILS,), jnp.float32, -1.0, 1.0)
    base_phase = 2.0 * math.pi * jax.random.uniform(key_phase, (NUM_COILS,), jnp.float32)
    coil_phase = base_phase[:, None, None] + math.pi * (grad_y[:, None, None] * pixel_pos[None, :, None] + grad_x[:, None, None] * pixel_pos[None, None, :])
    return jnp.stack([magnitude * jnp.cos(coil_phase), magnitude * jnp.sin(coil_phase)])


def setup_inputs(seed: int = 0, part: int = 0) -> dict:
    base_key = jax.random.key(seed)
    shared_key, root_key = jax.random.split(base_key)
    part_key = jax.random.fold_in(root_key, part)
    key_layout, key_y, key_wr, key_wc, key_map = jax.random.split(part_key, 5)
    valid_count, grid_row, grid_col = draw_layout(key_layout)
    centre_dist = (jnp.abs(grid_row - IMAGE_SIZE) + jnp.abs(grid_col - IMAGE_SIZE)).astype(jnp.float32) / GRID_SIZE
    amplitude = 1.0 / (1.0 + 8.0 * centre_dist)
    kspace = jax.random.normal(key_y, (2, NUM_COILS, SAMPLES), jnp.float32) * amplitude[None, None, :] * (3.0 / math.sqrt(NUM_COILS * SAMPLES))
    pixel_pos = (jnp.arange(IMAGE_SIZE, dtype=jnp.float32) - IMAGE_SIZE // 2) / IMAGE_SIZE
    deapod = (1.0 + 2.0 * pixel_pos * pixel_pos) * jax.random.uniform(shared_key, (IMAGE_SIZE,), jnp.float32, 0.8, 1.2)
    return dict(kspace=kspace, weight_row=kernel_weights(key_wr), weight_col=kernel_weights(key_wc), grid_row=grid_row, grid_col=grid_col, valid_count=valid_count, coil_maps=draw_maps(key_map), deapod=deapod)


def make_table():
    freq_index = jnp.arange(GRID_SIZE, dtype=jnp.int32) - IMAGE_SIZE
    pixel_index = jnp.arange(IMAGE_SIZE, dtype=jnp.int32) - IMAGE_SIZE // 2
    angle_grid = jnp.mod(freq_index[:, None] * pixel_index[None, :], GRID_SIZE).astype(jnp.float32) * (2.0 * math.pi / GRID_SIZE)
    cos_part = jnp.cos(angle_grid)
    sin_part = jnp.sin(angle_grid)
    return jnp.stack([jnp.stack([cos_part, sin_part], axis=1), jnp.stack([-sin_part, cos_part], axis=1)], axis=0).astype(jnp.bfloat16)


def reference(kspace, weight_row, weight_col, grid_row, grid_col, valid_count, coil_maps, deapod):
    slot_index = jnp.tile(jnp.arange(PER_BLOCK), ROW_BLOCKS)
    keep_mask = (slot_index < jnp.repeat(valid_count, PER_BLOCK)).astype(jnp.float32)
    row_coef = (kspace[:, :, None, :] * (weight_row * keep_mask)[None, None, :, :]).astype(jnp.bfloat16).astype(jnp.float32)
    col_coef = weight_col.astype(jnp.bfloat16).astype(jnp.float32)
    dft_table = make_table().astype(jnp.float32)
    offsets = jnp.arange(KERNEL_WIDTH * KERNEL_WIDTH)

    def one_coil(coil_args):
        coil_coef, coil_map = coil_args

        def add_offset(flat_grid, offset):
            row_off = offset // KERNEL_WIDTH
            col_off = offset % KERNEL_WIDTH
            row_index = jnp.mod(grid_row + row_off - HALF_WIDTH, GRID_SIZE)
            col_index = jnp.mod(grid_col + col_off - HALF_WIDTH, GRID_SIZE)
            contrib = lax.dynamic_index_in_dim(coil_coef, row_off, axis=1, keepdims=False) * lax.dynamic_index_in_dim(col_coef, col_off, axis=0, keepdims=False)[None, :]
            flat_grid = flat_grid + jax.ops.segment_sum(contrib.T, row_index * GRID_SIZE + col_index, num_segments=GRID_SIZE * GRID_SIZE)
            return flat_grid, None

        flat_grid = lax.scan(add_offset, jnp.zeros((GRID_SIZE * GRID_SIZE, 2), jnp.float32), offsets)[0]
        grid_bf = flat_grid.T.reshape(2, GRID_SIZE, GRID_SIZE).astype(jnp.bfloat16).astype(jnp.float32)
        half_image = jnp.einsum('qyk,qkbj->byj', grid_bf, dft_table).astype(jnp.bfloat16).astype(jnp.float32)
        coil_image = jnp.einsum('byj,byei->eij', half_image, dft_table)
        real_part = coil_map[0] * coil_image[0] + coil_map[1] * coil_image[1]
        imag_part = coil_map[0] * coil_image[1] - coil_map[1] * coil_image[0]
        return jnp.stack([real_part, imag_part])

    per_coil = lax.map(one_coil, (jnp.swapaxes(row_coef, 0, 1), jnp.swapaxes(coil_maps, 0, 1)))
    return jnp.sum(per_coil, axis=0) * (deapod[:, None] * deapod[None, :])[None]
```

```python
import math
import functools
import numpy as np
import jax
import jax.numpy as jnp
from jax import lax
from jax.experimental import pallas as pl
from jax.experimental.pallas import tpu as pltpu
from jax.sharding import PartitionSpec as P

F32 = jnp.float32
BF = jnp.bfloat16
NT = (((1,), (1,)), ((), ()))
KC = 512


def tables(n_img):
    n_grid = 2 * n_img
    pix = np.arange(n_img) - n_img // 2
    freq = np.arange(n_grid) - n_img
    ang = np.mod(pix[:, None] * freq[None, :], n_grid) * (2.0 * math.pi / n_grid)
    return np.stack([np.cos(ang), np.sin(ang)]).astype(np.float32).astype(BF)


def spread_kernel(pk, tab, h_ref, e_ref, acc, a_buf, b_buf, g_buf, hs, t_buf, sem):
    n_grid = 1024
    x_id = lax.axis_index('rows') // 2
    my_cols = pl.ds(pl.multiple_of(x_id * 256, 256), 256)
    copies = [
        pltpu.make_async_copy(tab.at[0, my_cols], t_buf.at[0, :, pl.ds(0, n_grid)], sem.at[0]),
        pltpu.make_async_copy(tab.at[1, my_cols], t_buf.at[1, :, pl.ds(0, n_grid)], sem.at[1]),
        pltpu.make_async_copy(tab.at[0, my_cols], t_buf.at[1, :, pl.ds(n_grid, n_grid)], sem.at[2]),
    ]
    for cp in copies:
        cp.start()
    valid = jnp.max(pk[22:23, 0:128]).astype(jnp.int32)
    n_chunk = (valid + (KC - 1)) // KC

    def build(s):
        cols = pl.ds(pl.multiple_of(s * KC, KC), KC)
        sub = lax.broadcasted_iota(jnp.int32, (16, KC), 0)
        keep = (lax.broadcasted_iota(jnp.int32, (1, KC), 1) + s * KC) < valid
        r0 = pk[20:21, cols].astype(jnp.int32) + 1
        u = jnp.broadcast_to((r0 >> 2).astype(F32), (16, KC)).astype(BF)
        t = (sub >> 2) - (r0 & 3)
        es = []
        for q in range(2):
            y16 = jnp.zeros((16, KC), F32)
            for c in range(4):
                y16 = jnp.where((sub & 3) == c, pk[4 * q + c:4 * q + c + 1, cols], y16)
            coef = [jnp.where(keep, y16 * pk[8 + a:9 + a, cols], 0.0) for a in range(6)]
            row = []
            for j in range(3):
                e = jnp.zeros((16, KC), F32)
                for a in range(6):
                    if -3 <= a - 4 * j <= 3:
                        e = jnp.where(t == a - 4 * j, coef[a], e)
                row.append(e.astype(BF))
            es.append(row)
        zero = jnp.zeros((16, KC), BF)
        for g in range(66):
            m0 = u == jnp.array(g, BF)
            m1 = u == jnp.array(g - 1, BF)
            m2 = u == jnp.array(g - 2, BF)
            for q in range(2):
                a_buf[1056 * q + 16 * g:1056 * q + 16 * g + 16, :] = jnp.where(m0, es[q][0], jnp.where(m1, es[q][1], jnp.where(m2, es[q][2], zero)))
        c0 = (pk[21:22, cols].astype(jnp.int32) + (n_grid - 3)) & (n_grid - 1)
        uc = jnp.broadcast_to((c0 >> 4).astype(F32), (16, KC)).astype(BF)
        tc = sub - (c0 & 15)
        eb = []
        for j in range(2):
            e = jnp.zeros((16, KC), F32)
            for b in range(6):
                e = jnp.where(tc == b - 16 * j, pk[14 + b:15 + b, cols], e)
            eb.append(e.astype(BF))
        for g in range(64):
            m0 = uc == jnp.array(g, BF)
            m1 = uc == jnp.array((g - 1) % 64, BF)
            b_buf[16 * g:16 * g + 16, :] = jnp.where(m0, eb[0], jnp.where(m1, eb[1], zero))

    def mults(first):
        @pl.loop(0, 2)
        def _(q):
            rows = pl.ds(pl.multiple_of(q * 1056, 16), 1056)
            prod = lax.dot_general(a_buf[rows, :], b_buf[...], NT, preferred_element_type=F32)
            if first:
                acc[rows, :] = prod
            else:
                acc[rows, :] += prod

    build(0)
    mults(True)

    @pl.loop(1, n_chunk)
    def _(s):
        build(s)
        mults(False)

    for cp in copies:
        cp.wait()
    t_buf[0, :, n_grid:] = -t_buf[1, :, :n_grid]
    for q in range(2):
        e_ref[q, 0:32] = acc[1056 * q:1056 * q + 32, :]
        e_ref[q, 32:64] = acc[1056 * q + 1024:1056 * q + 1056, :]
        g_buf[:, n_grid * q:n_grid * (q + 1)] = acc[1056 * q + 16:1056 * q + 1040, :].astype(BF)
    for e in range(2):
        prod = lax.dot_general(g_buf[...], t_buf[e], NT, preferred_element_type=F32)
        for hc in range(2):
            hs[2 * e + hc] = prod[:, 128 * hc:128 * hc + 128]
    for e in range(2):
        for hc in range(2):
            for c in range(4):
                h_ref[hc, e, :, 128 * c:128 * c + 128] = hs[2 * e + hc, pl.ds(c, 256, stride=4), :].astype(BF)


def spread(pk, tab):
    vm = pl.BlockSpec(memory_space=pltpu.VMEM)
    return pl.pallas_call(
        spread_kernel,
        out_shape=(jax.ShapeDtypeStruct((2, 2, 256, 512), BF), jax.ShapeDtypeStruct((2, 64, 1024), F32)),
        in_specs=[vm, pl.BlockSpec(memory_space=pl.ANY)],
        out_specs=(vm, vm),
        scratch_shapes=[
            pltpu.VMEM((2112, 1024), F32),
            pltpu.VMEM((2112, KC), BF),
            pltpu.VMEM((1024, KC), BF),
            pltpu.VMEM((1024, 2048), BF),
            pltpu.VMEM((4, 1024, 128), F32),
            pltpu.VMEM((2, 256, 2048), BF),
            pltpu.SemaphoreType.DMA((3,)),
        ],
        compiler_params=pltpu.CompilerParams(vmem_limit_bytes=40 * 2**20),
        cost_estimate=pl.CostEstimate(flops=13 * 10**9, bytes_accessed=4 * 2**20, transcendentals=0),
        name='spread',
    )(pk, tab)


def combine_kernel(h_own, h_nb, e_own, e_nb, tab, maps, out_ref,
                   t3, rhs, sbuf, s_vm, rx, ge, hs, pt, part, rx2,
                   loc, esend, erecv, hsend, hrecv, psend, precv, ysend, yrecv):
    n_grid = 1024
    row_id = lax.axis_index('rows')
    y_id = lax.axis_index('coil')
    core = row_id % 2
    x_id = row_id // 2
    sib = {'rows': row_id + 1 - 2 * core}
    mate = {'coil': 1 - y_id}
    blocks = [row_id, (row_id + 2) % 4]
    hh = [h_own, h_nb]
    ee = [e_own, e_nb]

    n_loc = 0
    t_copies = []
    for src, dst in ((tab.at[0], t3.at[0, :, pl.ds(0, n_grid)]), (tab.at[1], t3.at[1, :, pl.ds(0, n_grid)]), (tab.at[0], t3.at[1, :, pl.ds(n_grid, n_grid)])):
        t_copies.append(pltpu.make_async_copy(src, dst, loc.at[n_loc]))
        n_loc += 1
    h_copies = []
    for o in range(2):
        for b in range(2):
            h_copies.append(pltpu.make_async_copy(hh[o].at[core, b], rhs.at[b, blocks[o]], loc.at[n_loc]))
            n_loc += 1
            for end in range(2):
                h_copies.append(pltpu.make_async_copy(hh[o].at[1 - core, b, pl.ds(240 * end, 16)], sbuf.at[o, b, end], loc.at[n_loc]))
                n_loc += 1
    s_copy = pltpu.make_async_copy(maps, s_vm, loc.at[n_loc])
    for cp in t_copies + h_copies:
        cp.start()

    barrier = pltpu.get_barrier_semaphore()
    pl.semaphore_signal(barrier, inc=1, device_id=sib, device_id_type=pl.DeviceIdType.MESH)
    pl.semaphore_signal(barrier, inc=1, device_id=mate, device_id_type=pl.DeviceIdType.MESH)
    pl.semaphore_wait(barrier, 2)

    def remote(src, dst, ssem, rsem, dev):
        return pltpu.make_async_remote_copy(src_ref=src, dst_ref=dst, send_sem=ssem, recv_sem=rsem, device_id=dev, device_id_type=pl.DeviceIdType.MESH)

    e_copies = []
    for o in range(2):
        low = o * core + (1 - o) * (1 - core)
        high = o * (1 - core) + (1 - o) * core
        for k, (slot, end, row0) in enumerate(((low, 1, 0), (high, 0, 48))):
            e_copies.append(remote(ee[o].at[:, pl.ds(row0, 16)], rx.at[slot, end], esend.at[2 * o + k], erecv.at[slot, end], sib))
    for cp in e_copies:
        cp.start()
    hr_copies = []
    for o in range(2):
        for b in range(2):
            hr_copies.append(remote(hh[o].at[1 - core, b, pl.ds(16, 224)], rhs.at[b, blocks[o], pl.ds(16, 224)], hsend.at[o, b], hrecv.at[o, b], sib))
    for cp in hr_copies:
        cp.start()
    s_copy.start()

    for cp in t_copies:
        cp.wait()
    t3[0, :, n_grid:] = -t3[1, :, :n_grid]
    for cp in e_copies:
        cp.wait_send()
    for o in range(2):
        for end in range(2):
            remote(rx.at[o, end], rx.at[o, end], esend.at[2 * o + end], erecv.at[o, end], sib).wait_recv()
            for q in range(2):
                ge[32 * o + 16 * end:32 * o + 16 * end + 16, n_grid * q:n_grid * (q + 1)] = (ee[o][q, 16 + 16 * end:32 + 16 * end, :] + rx[o, end, q]).astype(BF)
    cols = pl.ds(pl.multiple_of(x_id * 256, 256), 256)
    for e in range(2):
        prod = lax.dot_general(ge[...], t3[e, cols, :], NT, preferred_element_type=F32)
        for hc in range(2):
            hs[2 * e + hc] = prod[:, 128 * hc:128 * hc + 128]
    for cp in h_copies:
        cp.wait()
    p_copies = []
    n_p = 0
    for o in range(2):
        for end in range(2):
            for b in range(2):
                for mine in range(2):
                    hc = core if mine else 1 - core
                    rows = pl.ds(240 * end, 16)
                    if mine:
                        pt[...] = rhs[b, blocks[o], rows, :].astype(F32)
                    else:
                        pt[...] = sbuf[o, b, end].astype(F32)
                    for c in range(4):
                        pt[12 * end:12 * end + 4, 128 * c:128 * c + 128] = hs[2 * b + hc, pl.ds(32 * o + 16 * end + c, 4, stride=4), :]
                    if mine:
                        rhs[b, blocks[o], rows, :] = pt[...].astype(BF)
                    else:
                        sbuf[o, b, end] = pt[...].astype(BF)
                        cp = remote(sbuf.at[o, b, end], rhs.at[b, blocks[o], rows], psend.at[n_p], precv.at[n_p], sib)
                        cp.start()
                        p_copies.append(cp)
                        n_p += 1
    s_copy.wait()
    for cp in hr_copies + p_copies:
        cp.wait()

    def image_rows(i0, size):
        rows = pl.ds(pl.multiple_of(i0, size), size)
        w = rhs[...].reshape(2048, 512)
        im = [jnp.dot(t3[e, rows, :], w, preferred_element_type=F32) for e in range(2)]
        xr = jnp.zeros((size, 128), F32)
        xi = jnp.zeros((size, 128), F32)
        for c in range(4):
            ir = im[0][:, 128 * c:128 * c + 128]
            ii = im[1][:, 128 * c:128 * c + 128]
            sr = s_vm[0, c, rows, :]
            si = s_vm[1, c, rows, :]
            xr = xr + (sr * ir + si * ii)
            xi = xi + (sr * ii - si * ir)
        return xr, xi

    y_copies = []
    for k in range(2):
        xr, xi = image_rows((1 - y_id) * 256 + 128 * k, 128)
        part[0, 128 * k:128 * k + 128] = xr
        part[1, 128 * k:128 * k + 128] = xi
        cp = remote(part.at[:, pl.ds(128 * k, 128)], rx2.at[:, pl.ds(128 * k, 128)], ysend.at[k], yrecv.at[k], mate)
        cp.start()
        y_copies.append(cp)
    for k in range(2):
        xr, xi = image_rows(y_id * 256 + 128 * k, 128)
        out_ref[0, 128 * k:128 * k + 128] = xr
        out_ref[1, 128 * k:128 * k + 128] = xi
    for k in range(2):
        y_copies[k].wait()
        sl = slice(128 * k, 128 * k + 128)
        out_ref[:, sl] += rx2[:, sl]


def combine(h_own, h_nb, e_own, e_nb, tab, maps):
    vm = pl.BlockSpec(memory_space=pltpu.VMEM)
    anym = pl.BlockSpec(memory_space=pl.ANY)
    dma = pltpu.SemaphoreType.DMA
    return pl.pallas_call(
        combine_kernel,
        out_shape=jax.ShapeDtypeStruct((2, 256, 128), F32),
        in_specs=[anym, anym, vm, vm, anym, anym],
        out_specs=vm,
        scratch_shapes=[
            pltpu.VMEM((2, 512, 2048), BF),
            pltpu.VMEM((2, 4, 256, 512), BF),
            pltpu.VMEM((2, 2, 2, 16, 512), BF),
            pltpu.VMEM((2, 4, 512, 128), F32),
            pltpu.VMEM((2, 2, 2, 16, 1024), F32),
            pltpu.VMEM((64, 2048), BF),
            pltpu.VMEM((4, 64, 128), F32),
            pltpu.VMEM((16, 512), F32),
            pltpu.VMEM((2, 256, 128), F32),
            pltpu.VMEM((2, 256, 128), F32),
            dma((16,)), dma((4,)), dma((2, 2)), dma((2, 2)), dma((2, 2)), dma((8,)), dma((8,)), dma((2,)), dma((2,)),
        ],
        compiler_params=pltpu.CompilerParams(vmem_limit_bytes=40 * 2**20, collective_id=0, has_side_effects=True),
        cost_estimate=pl.CostEstimate(flops=3 * 10**9, bytes_accessed=12 * 2**20, transcendentals=0),
        name='combine',
    )(h_own, h_nb, e_own, e_nb, tab, maps)


def solution(mesh):
    n_rows = mesh.shape['rows']
    swap = [(i, (i + 2) % n_rows) for i in range(n_rows)]

    def local_part(kspace, weight_row, weight_col, grid_row, grid_col, valid_count, coil_maps, deapod):
        n_img = deapod.shape[0]
        samples = kspace.shape[2]
        row_id = lax.axis_index('rows')
        coil_id = lax.axis_index('coil')
        local_row = (grid_row - row_id * (2 * n_img // n_rows)).astype(F32)
        packed = jnp.concatenate([
            kspace.reshape(8, samples), weight_row, weight_col, local_row[None], grid_col.astype(F32)[None],
            jnp.broadcast_to(valid_count.astype(F32)[:, None], (2, samples))], axis=0)
        other = lax.ppermute(packed, 'rows', swap)
        tab = jnp.asarray(tables(n_img))
        h_own, e_own = spread(packed, tab)
        h_nb, e_nb = spread(other, tab)
        combined = combine(h_own, h_nb, e_own, e_nb, tab, coil_maps)
        row_scale = lax.dynamic_slice_in_dim(deapod, coil_id * combined.shape[1], combined.shape[1])
        col_scale = lax.dynamic_slice_in_dim(deapod, row_id * combined.shape[2], combined.shape[2])
        return combined * (row_scale[:, None] * col_scale[None, :])[None]

    spec_samples = P(None, 'coil', ('slab', 'rows'))
    spec_weights = P(None, ('slab', 'rows'))
    spec_index = P(('slab', 'rows'))
    return jax.shard_map(local_part, mesh=mesh, in_specs=(spec_samples, spec_weights, spec_weights, spec_index, spec_index, spec_index, P(None, 'coil', 'slab', 'rows'), P()), out_specs=P(None, ('slab', 'coil'), 'rows'), check_vma=False)
```

```python
import math
import functools
import numpy as np
import jax
import jax.numpy as jnp
from jax import lax
from jax.experimental import pallas as pl
from jax.experimental.pallas import tpu as pltpu
from jax.sharding import PartitionSpec as P

F32 = jnp.float32
BF = jnp.bfloat16
NT = (((1,), (1,)), ((), ()))
KC = 512


def tables(n_img):
    n_grid = 2 * n_img
    pix = np.arange(n_img) - n_img // 2
    freq = np.arange(n_grid) - n_img
    ang = np.mod(pix[:, None] * freq[None, :], n_grid) * (2.0 * math.pi / n_grid)
    return np.stack([np.cos(ang), np.sin(ang)]).astype(np.float32).astype(BF)


def spread_kernel(shift, y_ref, wy_ref, wx_ref, iy_ref, ix_ref, n_ref, tab, h_ref, e_ref, acc, a_buf, b_buf, g_buf, hs, t_buf, sem):
    n_grid = 1024
    row_id = lax.axis_index('rows')
    x_id = row_id // 2
    first_row = ((row_id + shift) % 4) * 256
    my_cols = pl.ds(pl.multiple_of(x_id * 256, 256), 256)
    copies = [
        pltpu.make_async_copy(tab.at[0, my_cols], t_buf.at[0, :, pl.ds(0, n_grid)], sem.at[0]),
        pltpu.make_async_copy(tab.at[1, my_cols], t_buf.at[1, :, pl.ds(0, n_grid)], sem.at[1]),
        pltpu.make_async_copy(tab.at[0, my_cols], t_buf.at[1, :, pl.ds(n_grid, n_grid)], sem.at[2]),
    ]
    for cp in copies:
        cp.start()
    valid = n_ref[0]
    n_chunk = (valid + (KC - 1)) // KC

    def build(s):
        cols = pl.ds(pl.multiple_of(s * KC, KC), KC)
        sub = lax.broadcasted_iota(jnp.int32, (16, KC), 0)
        keep = (lax.broadcasted_iota(jnp.int32, (1, KC), 1) + s * KC) < valid
        r0 = iy_ref[:, cols] - (first_row - 1)
        u = jnp.broadcast_to((r0 >> 2).astype(F32), (16, KC)).astype(BF)
        t = (sub >> 2) - (r0 & 3)
        es = []
        for q in range(2):
            y16 = jnp.zeros((16, KC), F32)
            for c in range(4):
                y16 = jnp.where((sub & 3) == c, y_ref[q, c:c + 1, cols], y16)
            coef = [jnp.where(keep, y16 * wy_ref[a:a + 1, cols], 0.0) for a in range(6)]
            row = []
            for j in range(3):
                e = jnp.zeros((16, KC), F32)
                for a in range(6):
                    if -3 <= a - 4 * j <= 3:
                        e = jnp.where(t == a - 4 * j, coef[a], e)
                row.append(e.astype(BF))
            es.append(row)
        zero = jnp.zeros((16, KC), BF)
        for g in range(66):
            m0 = u == jnp.array(g, BF)
            m1 = u == jnp.array(g - 1, BF)
            m2 = u == jnp.array(g - 2, BF)
            for q in range(2):
                a_buf[1056 * q + 16 * g:1056 * q + 16 * g + 16, :] = jnp.where(m0, es[q][0], jnp.where(m1, es[q][1], jnp.where(m2, es[q][2], zero)))
        c0 = (ix_ref[:, cols] + (n_grid - 3)) & (n_grid - 1)
        uc = jnp.broadcast_to((c0 >> 4).astype(F32), (16, KC)).astype(BF)
        tc = sub - (c0 & 15)
        eb = []
        for j in range(2):
            e = jnp.zeros((16, KC), F32)
            for b in range(6):
                e = jnp.where(tc == b - 16 * j, wx_ref[b:b + 1, cols], e)
            eb.append(e.astype(BF))
        for g in range(64):
            m0 = uc == jnp.array(g, BF)
            m1 = uc == jnp.array((g - 1) % 64, BF)
            b_buf[16 * g:16 * g + 16, :] = jnp.where(m0, eb[0], jnp.where(m1, eb[1], zero))

    def mults(first):
        @pl.loop(0, 2)
        def _(q):
            rows = pl.ds(pl.multiple_of(q * 1056, 16), 1056)
            prod = lax.dot_general(a_buf[rows, :], b_buf[...], NT, preferred_element_type=F32)
            if first:
                acc[rows, :] = prod
            else:
                acc[rows, :] += prod

    build(0)
    mults(True)

    @pl.loop(1, n_chunk)
    def _(s):
        build(s)
        mults(False)

    for cp in copies:
        cp.wait()
    t_buf[0, :, n_grid:] = -t_buf[1, :, :n_grid]
    for q in range(2):
        e_ref[q, 0:32] = acc[1056 * q:1056 * q + 32, :]
        e_ref[q, 32:64] = acc[1056 * q + 1024:1056 * q + 1056, :]
        g_buf[:, n_grid * q:n_grid * (q + 1)] = acc[1056 * q + 16:1056 * q + 1040, :].astype(BF)
    for e in range(2):
        prod = lax.dot_general(g_buf[...], t_buf[e], NT, preferred_element_type=F32)
        for hc in range(2):
            hs[2 * e + hc] = prod[:, 128 * hc:128 * hc + 128]
    for e in range(2):
        for hc in range(2):
            for c in range(4):
                h_ref[hc, e, :, 128 * c:128 * c + 128] = hs[2 * e + hc, pl.ds(c, 256, stride=4), :].astype(BF)


def spread(shift, y, wy, wx, iy, ix, n, tab):
    vm = pl.BlockSpec(memory_space=pltpu.VMEM)
    return pl.pallas_call(
        functools.partial(spread_kernel, shift),
        out_shape=(jax.ShapeDtypeStruct((2, 2, 256, 512), BF), jax.ShapeDtypeStruct((2, 64, 1024), F32)),
        in_specs=[vm, vm, vm, vm, vm, pl.BlockSpec(memory_space=pltpu.SMEM), pl.BlockSpec(memory_space=pltpu.HBM)],
        out_specs=(vm, vm),
        scratch_shapes=[
            pltpu.VMEM((2112, 1024), F32),
            pltpu.VMEM((2112, KC), BF),
            pltpu.VMEM((1024, KC), BF),
            pltpu.VMEM((1024, 2048), BF),
            pltpu.VMEM((4, 1024, 128), F32),
            pltpu.VMEM((2, 256, 2048), BF),
            pltpu.SemaphoreType.DMA((3,)),
        ],
        compiler_params=pltpu.CompilerParams(vmem_limit_bytes=40 * 2**20),
        cost_estimate=pl.CostEstimate(flops=13 * 10**9, bytes_accessed=4 * 2**20, transcendentals=0),
        name='spread',
    )(y, wy, wx, iy, ix, n, tab)


def combine_kernel(h_own, h_nb, e_own, e_nb, tab, maps, out_ref,
                   t3, rhs, sbuf, s_vm, rx, ge, hs, pt, part, rx2,
                   loc, esend, erecv, hsend, hrecv, psend, precv, ysend, yrecv):
    n_grid = 1024
    row_id = lax.axis_index('rows')
    y_id = lax.axis_index('coil')
    core = row_id % 2
    x_id = row_id // 2
    sib = {'rows': row_id + 1 - 2 * core}
    mate = {'coil': 1 - y_id}
    blocks = [row_id, (row_id + 2) % 4]
    hh = [h_own, h_nb]
    ee = [e_own, e_nb]

    n_loc = 0
    t_copies = []
    for src, dst in ((tab.at[0], t3.at[0, :, pl.ds(0, n_grid)]), (tab.at[1], t3.at[1, :, pl.ds(0, n_grid)]), (tab.at[0], t3.at[1, :, pl.ds(n_grid, n_grid)])):
        t_copies.append(pltpu.make_async_copy(src, dst, loc.at[n_loc]))
        n_loc += 1
    h_copies = []
    for o in range(2):
        for b in range(2):
            h_copies.append(pltpu.make_async_copy(hh[o].at[core, b], rhs.at[b, blocks[o]], loc.at[n_loc]))
            n_loc += 1
            for end in range(2):
                h_copies.append(pltpu.make_async_copy(hh[o].at[1 - core, b, pl.ds(240 * end, 16)], sbuf.at[o, b, end], loc.at[n_loc]))
                n_loc += 1
    s_copy = pltpu.make_async_copy(maps, s_vm, loc.at[n_loc])
    for cp in t_copies + h_copies:
        cp.start()

    barrier = pltpu.get_barrier_semaphore()
    pl.semaphore_signal(barrier, inc=1, device_id=sib, device_id_type=pl.DeviceIdType.MESH)
    pl.semaphore_signal(barrier, inc=1, device_id=mate, device_id_type=pl.DeviceIdType.MESH)
    pl.semaphore_wait(barrier, 2)

    def remote(src, dst, ssem, rsem, dev):
        return pltpu.make_async_remote_copy(src_ref=src, dst_ref=dst, send_sem=ssem, recv_sem=rsem, device_id=dev, device_id_type=pl.DeviceIdType.MESH)

    e_copies = []
    for o in range(2):
        low = o * core + (1 - o) * (1 - core)
        high = o * (1 - core) + (1 - o) * core
        for k, (slot, end, row0) in enumerate(((low, 1, 0), (high, 0, 48))):
            e_copies.append(remote(ee[o].at[:, pl.ds(row0, 16)], rx.at[slot, end], esend.at[2 * o + k], erecv.at[slot, end], sib))
    for cp in e_copies:
        cp.start()
    hr_copies = []
    for o in range(2):
        for b in range(2):
            hr_copies.append(remote(hh[o].at[1 - core, b, pl.ds(16, 224)], rhs.at[b, blocks[o], pl.ds(16, 224)], hsend.at[o, b], hrecv.at[o, b], sib))
    for cp in hr_copies:
        cp.start()
    s_copy.start()

    for cp in t_copies:
        cp.wait()
    t3[0, :, n_grid:] = -t3[1, :, :n_grid]
    for cp in e_copies:
        cp.wait_send()
    for o in range(2):
        for end in range(2):
            remote(rx.at[o, end], rx.at[o, end], esend.at[2 * o + end], erecv.at[o, end], sib).wait_recv()
            for q in range(2):
                ge[32 * o + 16 * end:32 * o + 16 * end + 16, n_grid * q:n_grid * (q + 1)] = (ee[o][q, 16 + 16 * end:32 + 16 * end, :] + rx[o, end, q]).astype(BF)
    cols = pl.ds(pl.multiple_of(x_id * 256, 256), 256)
    for e in range(2):
        prod = lax.dot_general(ge[...], t3[e, cols, :], NT, preferred_element_type=F32)
        for hc in range(2):
            hs[2 * e + hc] = prod[:, 128 * hc:128 * hc + 128]
    for cp in h_copies:
        cp.wait()
    p_copies = []
    n_p = 0
    for o in range(2):
        for end in range(2):
            for b in range(2):
                for mine in range(2):
                    hc = core if mine else 1 - core
                    rows = pl.ds(240 * end, 16)
                    if mine:
                        pt[...] = rhs[b, blocks[o], rows, :].astype(F32)
                    else:
                        pt[...] = sbuf[o, b, end].astype(F32)
                    for c in range(4):
                        pt[12 * end:12 * end + 4, 128 * c:128 * c + 128] = hs[2 * b + hc, pl.ds(32 * o + 16 * end + c, 4, stride=4), :]
                    if mine:
                        rhs[b, blocks[o], rows, :] = pt[...].astype(BF)
                    else:
                        sbuf[o, b, end] = pt[...].astype(BF)
                        cp = remote(sbuf.at[o, b, end], rhs.at[b, blocks[o], rows], psend.at[n_p], precv.at[n_p], sib)
                        cp.start()
                        p_copies.append(cp)
                        n_p += 1
    s_copy.wait()
    for cp in hr_copies + p_copies:
        cp.wait()

    def image_rows(i0, size):
        rows = pl.ds(pl.multiple_of(i0, size), size)
        w = rhs[...].reshape(2048, 512)
        im = [jnp.dot(t3[e, rows, :], w, preferred_element_type=F32) for e in range(2)]
        xr = jnp.zeros((size, 128), F32)
        xi = jnp.zeros((size, 128), F32)
        for c in range(4):
            ir = im[0][:, 128 * c:128 * c + 128]
            ii = im[1][:, 128 * c:128 * c + 128]
            sr = s_vm[0, c, rows, :]
            si = s_vm[1, c, rows, :]
            xr = xr + (sr * ir + si * ii)
            xi = xi + (sr * ii - si * ir)
        return xr, xi

    y_copies = []
    for k in range(2):
        xr, xi = image_rows((1 - y_id) * 256 + 128 * k, 128)
        part[0, 128 * k:128 * k + 128] = xr
        part[1, 128 * k:128 * k + 128] = xi
        cp = remote(part.at[:, pl.ds(128 * k, 128)], rx2.at[:, pl.ds(128 * k, 128)], ysend.at[k], yrecv.at[k], mate)
        cp.start()
        y_copies.append(cp)
    for k in range(2):
        xr, xi = image_rows(y_id * 256 + 128 * k, 128)
        out_ref[0, 128 * k:128 * k + 128] = xr
        out_ref[1, 128 * k:128 * k + 128] = xi
    for k in range(2):
        y_copies[k].wait()
        sl = slice(128 * k, 128 * k + 128)
        out_ref[:, sl] += rx2[:, sl]


def combine(h_own, h_nb, e_own, e_nb, tab, maps):
    vm = pl.BlockSpec(memory_space=pltpu.VMEM)
    anym = pl.BlockSpec(memory_space=pl.ANY)
    hbm = pl.BlockSpec(memory_space=pltpu.HBM)
    dma = pltpu.SemaphoreType.DMA
    return pl.pallas_call(
        combine_kernel,
        out_shape=jax.ShapeDtypeStruct((2, 256, 128), F32),
        in_specs=[anym, anym, vm, vm, hbm, hbm],
        out_specs=vm,
        scratch_shapes=[
            pltpu.VMEM((2, 512, 2048), BF),
            pltpu.VMEM((2, 4, 256, 512), BF),
            pltpu.VMEM((2, 2, 2, 16, 512), BF),
            pltpu.VMEM((2, 4, 512, 128), F32),
            pltpu.VMEM((2, 2, 2, 16, 1024), F32),
            pltpu.VMEM((64, 2048), BF),
            pltpu.VMEM((4, 64, 128), F32),
            pltpu.VMEM((16, 512), F32),
            pltpu.VMEM((2, 256, 128), F32),
            pltpu.VMEM((2, 256, 128), F32),
            dma((16,)), dma((4,)), dma((2, 2)), dma((2, 2)), dma((2, 2)), dma((8,)), dma((8,)), dma((2,)), dma((2,)),
        ],
        compiler_params=pltpu.CompilerParams(vmem_limit_bytes=40 * 2**20, collective_id=0, has_side_effects=True),
        cost_estimate=pl.CostEstimate(flops=3 * 10**9, bytes_accessed=12 * 2**20, transcendentals=0),
        name='combine',
    )(h_own, h_nb, e_own, e_nb, tab, maps)


def solution(mesh):
    n_rows = mesh.shape['rows']
    swap = [(i, (i + 2) % n_rows) for i in range(n_rows)]

    def local_part(kspace, weight_row, weight_col, grid_row, grid_col, valid_count, coil_maps, deapod):
        n_img = deapod.shape[0]
        row_id = lax.axis_index('rows')
        coil_id = lax.axis_index('coil')
        own = (kspace, weight_row, weight_col, grid_row[None], grid_col[None], valid_count)
        other = [lax.ppermute(v, 'rows', swap) for v in own]
        tab = jnp.asarray(tables(n_img))
        h_own, e_own = spread(0, *own, tab)
        h_nb, e_nb = spread(2, *other, tab)
        combined = combine(h_own, h_nb, e_own, e_nb, tab, coil_maps)
        row_scale = lax.dynamic_slice_in_dim(deapod, coil_id * combined.shape[1], combined.shape[1])
        col_scale = lax.dynamic_slice_in_dim(deapod, row_id * combined.shape[2], combined.shape[2])
        return combined * (row_scale[:, None] * col_scale[None, :])[None]

    spec_samples = P(None, 'coil', ('slab', 'rows'))
    spec_weights = P(None, ('slab', 'rows'))
    spec_index = P(('slab', 'rows'))
    return jax.shard_map(local_part, mesh=mesh, in_specs=(spec_samples, spec_weights, spec_weights, spec_index, spec_index, spec_index, P(None, 'coil', 'slab', 'rows'), P()), out_specs=P(None, ('slab', 'coil'), 'rows'), check_vma=False)
```

```python
import math
import functools
import numpy as np
import jax
import jax.numpy as jnp
from jax import lax
from jax.experimental import pallas as pl
from jax.experimental.pallas import tpu as pltpu
from jax.sharding import PartitionSpec as P

F32 = jnp.float32
BF = jnp.bfloat16
NT = (((1,), (1,)), ((), ()))
KC = 512


def tables(n_img):
    n_grid = 2 * n_img
    pix = np.arange(n_img) - n_img // 2
    freq = np.arange(n_grid) - n_img
    ang = np.mod(pix[:, None] * freq[None, :], n_grid) * (2.0 * math.pi / n_grid)
    return np.stack([np.cos(ang), np.sin(ang)]).astype(np.float32).astype(BF)


def exchange_kernel(y_ref, wy_ref, wx_ref, iy_ref, ix_ref, n_ref, y_out, wy_out, wx_out, iy_out, ix_out, iy_in, loc, ssem, rsem):
    row_id = lax.axis_index('rows')
    other = {'rows': (row_id + 2) % 4}
    iy_copy = pltpu.make_async_copy(iy_ref, iy_in, loc.at[4])
    iy_copy.start()
    pairs = [(y_ref, y_out), (wy_ref, wy_out), (wx_ref, wx_out), (ix_ref, ix_out)]
    locs = [pltpu.make_async_copy(a, b.at[0], loc.at[i]) for i, (a, b) in enumerate(pairs)]
    for cp in locs:
        cp.start()
    barrier = pltpu.get_barrier_semaphore()
    pl.semaphore_signal(barrier, inc=1, device_id=other, device_id_type=pl.DeviceIdType.MESH)
    iy_copy.wait()
    slot = lax.broadcasted_iota(jnp.int32, iy_in.shape, 1)
    iy_out[0] = jnp.where(slot < n_ref[0], iy_in[...] - row_id * 256, -1000)
    pl.semaphore_wait(barrier, 1)
    pairs.append((iy_out.at[0], iy_out))
    sends = [pltpu.make_async_remote_copy(src_ref=a, dst_ref=b.at[1], send_sem=ssem.at[i], recv_sem=rsem.at[i], device_id=other, device_id_type=pl.DeviceIdType.MESH) for i, (a, b) in enumerate(pairs)]
    for cp in sends:
        cp.start()
    for cp in locs:
        cp.wait()
    for cp in sends:
        cp.wait()


def exchange(y, wy, wx, iy, ix, n):
    vm = pl.BlockSpec(memory_space=pltpu.VMEM)
    anym = pl.BlockSpec(memory_space=pl.ANY)
    dma = pltpu.SemaphoreType.DMA
    return pl.pallas_call(
        exchange_kernel,
        out_shape=tuple(jax.ShapeDtypeStruct((2,) + v.shape, v.dtype) for v in (y, wy, wx, iy, ix)),
        in_specs=[anym, anym, anym, anym, anym, pl.BlockSpec(memory_space=pltpu.SMEM)],
        out_specs=(vm,) * 5,
        scratch_shapes=[pltpu.VMEM(iy.shape, jnp.int32), dma((5,)), dma((5,)), dma((5,))],
        compiler_params=pltpu.CompilerParams(vmem_limit_bytes=4 * 2**20, collective_id=1, has_side_effects=True),
        cost_estimate=pl.CostEstimate(flops=10**9, bytes_accessed=10**6, transcendentals=0),
        name='exchange',
    )(y, wy, wx, iy, ix, n)


def spread_kernel(y_ref, wy_ref, wx_ref, iy_ref, ix_ref, tab, h_ref, e_ref, acc, a_buf, b_buf, g_buf, hs, t_buf, sem):
    n_grid = 1024
    x_id = lax.axis_index('rows') // 2
    my_cols = pl.ds(pl.multiple_of(x_id * 256, 256), 256)
    copies = [
        pltpu.make_async_copy(tab.at[0, my_cols], t_buf.at[0, :, pl.ds(0, n_grid)], sem.at[0]),
        pltpu.make_async_copy(tab.at[1, my_cols], t_buf.at[1, :, pl.ds(0, n_grid)], sem.at[1]),
        pltpu.make_async_copy(tab.at[0, my_cols], t_buf.at[1, :, pl.ds(n_grid, n_grid)], sem.at[2]),
    ]
    for cp in copies:
        cp.start()
    def build(o, s):
        cols = pl.ds(pl.multiple_of(s * KC, KC), KC)
        sub = lax.broadcasted_iota(jnp.int32, (16, KC), 0)
        r0 = iy_ref[o, :, cols] + 1
        keep = r0 > 0
        u = jnp.broadcast_to((r0 >> 2).astype(F32), (16, KC)).astype(BF)
        t = (sub >> 2) - (r0 & 3)
        es = []
        for q in range(2):
            y16 = jnp.zeros((16, KC), F32)
            for c in range(4):
                y16 = jnp.where((sub & 3) == c, y_ref[o, q, c:c + 1, cols], y16)
            coef = [jnp.where(keep, y16 * wy_ref[o, a:a + 1, cols], 0.0) for a in range(6)]
            row = []
            for j in range(3):
                e = jnp.zeros((16, KC), F32)
                for a in range(6):
                    if -3 <= a - 4 * j <= 3:
                        e = jnp.where(t == a - 4 * j, coef[a], e)
                row.append(e.astype(BF))
            es.append(row)
        zero = jnp.zeros((16, KC), BF)
        for g in range(66):
            m0 = u == jnp.array(g, BF)
            m1 = u == jnp.array(g - 1, BF)
            m2 = u == jnp.array(g - 2, BF)
            for q in range(2):
                a_buf[1056 * q + 16 * g:1056 * q + 16 * g + 16, :] = jnp.where(m0, es[q][0], jnp.where(m1, es[q][1], jnp.where(m2, es[q][2], zero)))
        c0 = (ix_ref[o, :, cols] + (n_grid - 3)) & (n_grid - 1)
        uc = jnp.broadcast_to((c0 >> 4).astype(F32), (16, KC)).astype(BF)
        tc = sub - (c0 & 15)
        eb = []
        for j in range(2):
            e = jnp.zeros((16, KC), F32)
            for b in range(6):
                e = jnp.where(tc == b - 16 * j, wx_ref[o, b:b + 1, cols], e)
            eb.append(e.astype(BF))
        for g in range(64):
            m0 = uc == jnp.array(g, BF)
            m1 = uc == jnp.array((g - 1) % 64, BF)
            b_buf[16 * g:16 * g + 16, :] = jnp.where(m0, eb[0], jnp.where(m1, eb[1], zero))

    def mults(first):
        @pl.loop(0, 2)
        def _(q):
            rows = pl.ds(pl.multiple_of(q * 1056, 16), 1056)
            prod = lax.dot_general(a_buf[rows, :], b_buf[...], NT, preferred_element_type=F32)
            if first:
                acc[rows, :] = prod
            else:
                acc[rows, :] += prod

    for cp in copies:
        cp.wait()
    t_buf[0, :, n_grid:] = -t_buf[1, :, :n_grid]

    @pl.loop(0, 2)
    def _(o):
        valid = jnp.sum(jnp.where(iy_ref[o] >= 0, 1.0, 0.0)).astype(jnp.int32)
        build(o, 0)
        mults(True)

        @pl.loop(1, (valid + (KC - 1)) // KC)
        def _(s):
            build(o, s)
            mults(False)

        for q in range(2):
            e_ref[o, q, 0:32] = acc[1056 * q:1056 * q + 32, :]
            e_ref[o, q, 32:64] = acc[1056 * q + 1024:1056 * q + 1056, :]
            g_buf[:, n_grid * q:n_grid * (q + 1)] = acc[1056 * q + 16:1056 * q + 1040, :].astype(BF)
        for e in range(2):
            prod = lax.dot_general(g_buf[...], t_buf[e], NT, preferred_element_type=F32)
            for hc in range(2):
                hs[2 * e + hc] = prod[:, 128 * hc:128 * hc + 128]
        for e in range(2):
            for hc in range(2):
                for c in range(4):
                    h_ref[o, hc, e, :, 128 * c:128 * c + 128] = hs[2 * e + hc, pl.ds(c, 256, stride=4), :].astype(BF)


def spread(y, wy, wx, iy, ix, tab):
    vm = pl.BlockSpec(memory_space=pltpu.VMEM)
    return pl.pallas_call(
        spread_kernel,
        out_shape=(jax.ShapeDtypeStruct((2, 2, 2, 256, 512), BF), jax.ShapeDtypeStruct((2, 2, 64, 1024), F32)),
        in_specs=[vm, vm, vm, vm, vm, pl.BlockSpec(memory_space=pl.ANY)],
        out_specs=(vm, vm),
        scratch_shapes=[
            pltpu.VMEM((2112, 1024), F32),
            pltpu.VMEM((2112, KC), BF),
            pltpu.VMEM((1024, KC), BF),
            pltpu.VMEM((1024, 2048), BF),
            pltpu.VMEM((4, 1024, 128), F32),
            pltpu.VMEM((2, 256, 2048), BF),
            pltpu.SemaphoreType.DMA((3,)),
        ],
        compiler_params=pltpu.CompilerParams(vmem_limit_bytes=40 * 2**20),
        cost_estimate=pl.CostEstimate(flops=13 * 10**9, bytes_accessed=4 * 2**20, transcendentals=0),
        name='spread',
    )(y, wy, wx, iy, ix, tab)


def combine_kernel(hh, ee, tab, maps, dd, out_ref,
                   t3, rhs, sbuf, s_vm, rx, ge, hs, pt, part, rx2, scale,
                   loc, esend, erecv, hsend, hrecv, psend, precv, ysend, yrecv):
    n_grid = 1024
    row_id = lax.axis_index('rows')
    y_id = lax.axis_index('coil')
    core = row_id % 2
    x_id = row_id // 2
    sib = {'rows': row_id + 1 - 2 * core}
    mate = {'coil': 1 - y_id}
    blocks = [row_id, (row_id + 2) % 4]

    n_loc = 0
    t_copies = []
    for src, dst in ((tab.at[0], t3.at[0, :, pl.ds(0, n_grid)]), (tab.at[1], t3.at[1, :, pl.ds(0, n_grid)]), (tab.at[0], t3.at[1, :, pl.ds(n_grid, n_grid)])):
        t_copies.append(pltpu.make_async_copy(src, dst, loc.at[n_loc]))
        n_loc += 1
    h_copies = []
    for o in range(2):
        for b in range(2):
            h_copies.append(pltpu.make_async_copy(hh.at[o, core, b], rhs.at[b, blocks[o]], loc.at[n_loc]))
            n_loc += 1
            for end in range(2):
                h_copies.append(pltpu.make_async_copy(hh.at[o, 1 - core, b, pl.ds(240 * end, 16)], sbuf.at[o, b, end], loc.at[n_loc]))
                n_loc += 1
    s_copy = pltpu.make_async_copy(maps, s_vm, loc.at[n_loc])
    for cp in t_copies + h_copies:
        cp.start()

    barrier = pltpu.get_barrier_semaphore()
    pl.semaphore_signal(barrier, inc=1, device_id=sib, device_id_type=pl.DeviceIdType.MESH)
    pl.semaphore_signal(barrier, inc=1, device_id=mate, device_id_type=pl.DeviceIdType.MESH)
    pl.semaphore_wait(barrier, 2)

    def remote(src, dst, ssem, rsem, dev):
        return pltpu.make_async_remote_copy(src_ref=src, dst_ref=dst, send_sem=ssem, recv_sem=rsem, device_id=dev, device_id_type=pl.DeviceIdType.MESH)

    e_copies = []
    for o in range(2):
        low = o * core + (1 - o) * (1 - core)
        high = o * (1 - core) + (1 - o) * core
        for k, (slot, end, row0) in enumerate(((low, 1, 0), (high, 0, 48))):
            e_copies.append(remote(ee.at[o, :, pl.ds(row0, 16)], rx.at[slot, end], esend.at[2 * o + k], erecv.at[slot, end], sib))
    for cp in e_copies:
        cp.start()
    hr_copies = []
    for o in range(2):
        for b in range(2):
            hr_copies.append(remote(hh.at[o, 1 - core, b, pl.ds(16, 224)], rhs.at[b, blocks[o], pl.ds(16, 224)], hsend.at[o, b], hrecv.at[o, b], sib))
    for cp in hr_copies:
        cp.start()
    s_copy.start()
    row_scale = jnp.broadcast_to(dd[:, pl.ds(pl.multiple_of(y_id * 256, 256), 256)], (128, 256)).T
    scale[...] = row_scale * dd[:, pl.ds(pl.multiple_of(row_id * 128, 128), 128)]

    for cp in t_copies:
        cp.wait()
    t3[0, :, n_grid:] = -t3[1, :, :n_grid]
    for cp in e_copies:
        cp.wait_send()
    for o in range(2):
        for end in range(2):
            remote(rx.at[o, end], rx.at[o, end], esend.at[2 * o + end], erecv.at[o, end], sib).wait_recv()
            for q in range(2):
                ge[32 * o + 16 * end:32 * o + 16 * end + 16, n_grid * q:n_grid * (q + 1)] = (ee[o, q, 16 + 16 * end:32 + 16 * end, :] + rx[o, end, q]).astype(BF)
    cols = pl.ds(pl.multiple_of(x_id * 256, 256), 256)
    for e in range(2):
        prod = lax.dot_general(ge[...], t3[e, cols, :], NT, preferred_element_type=F32)
        for hc in range(2):
            hs[2 * e + hc] = prod[:, 128 * hc:128 * hc + 128]
    for cp in h_copies:
        cp.wait()
    p_copies = []
    n_p = 0
    for o in range(2):
        for end in range(2):
            for b in range(2):
                for mine in range(2):
                    hc = core if mine else 1 - core
                    rows = pl.ds(240 * end, 16)
                    if mine:
                        pt[...] = rhs[b, blocks[o], rows, :].astype(F32)
                    else:
                        pt[...] = sbuf[o, b, end].astype(F32)
                    for c in range(4):
                        pt[12 * end:12 * end + 4, 128 * c:128 * c + 128] = hs[2 * b + hc, pl.ds(32 * o + 16 * end + c, 4, stride=4), :]
                    if mine:
                        rhs[b, blocks[o], rows, :] = pt[...].astype(BF)
                    else:
                        sbuf[o, b, end] = pt[...].astype(BF)
                        cp = remote(sbuf.at[o, b, end], rhs.at[b, blocks[o], rows], psend.at[n_p], precv.at[n_p], sib)
                        cp.start()
                        p_copies.append(cp)
                        n_p += 1
    s_copy.wait()
    for cp in hr_copies + p_copies:
        cp.wait()

    def image_rows(i0, size):
        rows = pl.ds(pl.multiple_of(i0, size), size)
        w = rhs[...].reshape(2048, 512)
        im = [jnp.dot(t3[e, rows, :], w, preferred_element_type=F32) for e in range(2)]
        xr = jnp.zeros((size, 128), F32)
        xi = jnp.zeros((size, 128), F32)
        for c in range(4):
            ir = im[0][:, 128 * c:128 * c + 128]
            ii = im[1][:, 128 * c:128 * c + 128]
            sr = s_vm[0, c, rows, :]
            si = s_vm[1, c, rows, :]
            xr = xr + (sr * ir + si * ii)
            xi = xi + (sr * ii - si * ir)
        return xr, xi

    y_copies = []
    for k in range(2):
        xr, xi = image_rows((1 - y_id) * 256 + 128 * k, 128)
        part[0, 128 * k:128 * k + 128] = xr
        part[1, 128 * k:128 * k + 128] = xi
        cp = remote(part.at[:, pl.ds(128 * k, 128)], rx2.at[:, pl.ds(128 * k, 128)], ysend.at[k], yrecv.at[k], mate)
        cp.start()
        y_copies.append(cp)
    for k in range(2):
        xr, xi = image_rows(y_id * 256 + 128 * k, 128)
        out_ref[0, 128 * k:128 * k + 128] = xr
        out_ref[1, 128 * k:128 * k + 128] = xi
    for k in range(2):
        y_copies[k].wait()
        sl = slice(128 * k, 128 * k + 128)
        for e in range(2):
            out_ref[e, sl] = (out_ref[e, sl] + rx2[e, sl]) * scale[sl]


def combine(hh, ee, tab, maps, dd):
    vm = pl.BlockSpec(memory_space=pltpu.VMEM)
    anym = pl.BlockSpec(memory_space=pl.ANY)
    dma = pltpu.SemaphoreType.DMA
    return pl.pallas_call(
        combine_kernel,
        out_shape=jax.ShapeDtypeStruct((2, 256, 128), F32),
        in_specs=[anym, vm, anym, anym, vm],
        out_specs=vm,
        scratch_shapes=[
            pltpu.VMEM((2, 512, 2048), BF),
            pltpu.VMEM((2, 4, 256, 512), BF),
            pltpu.VMEM((2, 2, 2, 16, 512), BF),
            pltpu.VMEM((2, 4, 512, 128), F32),
            pltpu.VMEM((2, 2, 2, 16, 1024), F32),
            pltpu.VMEM((64, 2048), BF),
            pltpu.VMEM((4, 64, 128), F32),
            pltpu.VMEM((16, 512), F32),
            pltpu.VMEM((2, 256, 128), F32),
            pltpu.VMEM((2, 256, 128), F32),
            pltpu.VMEM((256, 128), F32),
            dma((16,)), dma((4,)), dma((2, 2)), dma((2, 2)), dma((2, 2)), dma((8,)), dma((8,)), dma((2,)), dma((2,)),
        ],
        compiler_params=pltpu.CompilerParams(vmem_limit_bytes=40 * 2**20, collective_id=0, has_side_effects=True),
        cost_estimate=pl.CostEstimate(flops=3 * 10**9, bytes_accessed=12 * 2**20, transcendentals=0),
        name='combine',
    )(hh, ee, tab, maps, dd)


def solution(mesh):
    def local_part(kspace, weight_row, weight_col, grid_row, grid_col, valid_count, coil_maps, deapod):
        n_img = deapod.shape[0]
        hbm = [pltpu.with_memory_space_constraint(v, pltpu.HBM) for v in (kspace, weight_row, weight_col, grid_row[None], grid_col[None])]
        stacked = exchange(*hbm, valid_count)
        tab = jnp.asarray(tables(n_img))
        hh, ee = spread(*stacked, tab)
        return combine(hh, ee, tab, coil_maps, deapod[None])

    spec_samples = P(None, 'coil', ('slab', 'rows'))
    spec_weights = P(None, ('slab', 'rows'))
    spec_index = P(('slab', 'rows'))
    return jax.shard_map(local_part, mesh=mesh, in_specs=(spec_samples, spec_weights, spec_weights, spec_index, spec_index, spec_index, P(None, 'coil', 'slab', 'rows'), P()), out_specs=P(None, ('slab', 'coil'), 'rows'), check_vma=False)
```

```python
import math
import functools
import numpy as np
import jax
import jax.numpy as jnp
from jax import lax
from jax.experimental import pallas as pl
from jax.experimental.pallas import tpu as pltpu
from jax.sharding import PartitionSpec as P

F32 = jnp.float32
BF = jnp.bfloat16
NT = (((1,), (1,)), ((), ()))
KC = 512
GRID = 1024
SAMPLES = 2048
RUN = 256
WIN = 12


def tables(n_img):
    n_grid = 2 * n_img
    pix = np.arange(n_img) - n_img // 2
    freq = np.arange(n_grid) - n_img
    ang = np.mod(pix[:, None] * freq[None, :], n_grid) * (2.0 * math.pi / n_grid)
    return np.stack([np.cos(ang), np.sin(ang)]).astype(np.float32).astype(BF)


def payload(y_ref, wy_ref, wx_ref, iy_ref, ix_ref, pay):
    @pl.loop(0, SAMPLES // KC)
    def _(s):
        cols = pl.ds(pl.multiple_of(s * KC, KC), KC)
        sub = lax.broadcasted_iota(jnp.int32, (16, KC), 0)
        r0 = iy_ref[:, cols] + 1
        counted = r0 > 0
        t = jnp.where(counted, (sub >> 2) - (r0 & 3), 100)
        for q in range(2):
            y16 = jnp.zeros((16, KC), F32)
            for c in range(4):
                y16 = jnp.where((sub & 3) == c, y_ref[q, c:c + 1, cols], y16)
            coef = [y16 * wy_ref[a:a + 1, cols] for a in range(6)]
            for j in range(3):
                e = jnp.zeros((16, KC), F32)
                for a in range(6):
                    if -3 <= a - 4 * j <= 3:
                        e = jnp.where(t == a - 4 * j, coef[a], e)
                pay[48 * q + 16 * j:48 * q + 16 * j + 16, cols] = e.astype(BF)
        c0 = (ix_ref[:, cols] + (GRID - 3)) & (GRID - 1)
        tc = jnp.where(counted, sub - (c0 & 15), 100)
        for j in range(2):
            e = jnp.zeros((16, KC), F32)
            for b in range(6):
                e = jnp.where(tc == b - 16 * j, wx_ref[b:b + 1, cols], e)
            pay[96 + 16 * j:112 + 16 * j, cols] = e.astype(BF)
        pay[128:144, cols] = jnp.broadcast_to(((r0 >> 2) + 1).astype(F32), (16, KC)).astype(BF)
        pay[144:160, cols] = jnp.broadcast_to((c0 >> 4).astype(F32), (16, KC)).astype(BF)


def iota16():
    return lax.broadcasted_iota(jnp.int32, (16, 1), 0).astype(F32)


def ranks(iy_ref, oh, rank):
    n_run = SAMPLES // RUN
    for ch in range(n_run):
        lanes = slice(RUN * ch, RUN * ch + RUN)
        bucket = jnp.broadcast_to(((iy_ref[:, lanes] + 1) >> 2).astype(F32), (16, RUN)).astype(BF)
        for g in range(5):
            oh[80 * ch + 16 * g:80 * ch + 16 * g + 16, :] = jnp.where(bucket == (iota16() + 16 * g).astype(BF), jnp.ones((), BF), jnp.zeros((), BF))
    lower = lax.broadcasted_iota(jnp.int32, (RUN, RUN + 128), 0)
    upper = lax.broadcasted_iota(jnp.int32, (RUN, RUN + 128), 1)
    tri = jnp.where((lower < upper) | (upper >= RUN), 1.0, 0.0).astype(BF)
    pre = jnp.dot(oh[...], tri, preferred_element_type=F32)
    counts = [pre[80 * ch:80 * ch + 80, RUN:] for ch in range(n_run)]
    total = counts[0]
    for ch in range(1, n_run):
        total = total + counts[ch]
    high = jnp.floor(total * (1.0 / 256.0))
    low = total - 256.0 * high
    strict = jnp.where(lax.broadcasted_iota(jnp.int32, (80, 80), 1) < lax.broadcasted_iota(jnp.int32, (80, 80), 0), 1.0, 0.0).astype(BF)
    base = 256.0 * jnp.dot(strict, high.astype(BF), preferred_element_type=F32) + jnp.dot(strict, low.astype(BF), preferred_element_type=F32)
    for ch in range(n_run):
        lanes = slice(RUN * ch, RUN * ch + RUN)
        place = pre[80 * ch:80 * ch + 80, :RUN] + jnp.concatenate([base] * (RUN // 128), axis=1)
        place = jnp.sum(oh[80 * ch:80 * ch + 80, :].astype(F32) * place, axis=0, keepdims=True)
        rank[:, lanes] = jnp.where(iy_ref[:, lanes] >= 0, place, -1.0)
        base = base + counts[ch]


def reorder(s, pay, rank, pt):
    place = jnp.broadcast_to(rank[...] - (s * RUN).astype(F32), (16, SAMPLES)).astype(BF)
    for g in range(RUN // 16):
        pt[16 * g:16 * g + 16, :] = jnp.where(place == (iota16() + 16 * g).astype(BF), jnp.ones((), BF), jnp.zeros((), BF))
    return lax.dot_general(pay[...], pt[...], NT, preferred_element_type=F32).astype(BF)


def exchange_kernel(y_ref, wy_ref, wx_ref, iy_ref, ix_ref, n_ref, y_out, wy_out, wx_out, iy_out, ix_out, d_out,
                    y_in, wy_in, wx_in, iy_in, ix_in, iy_raw, pay, oh, rank, pt, loc, ssem, rsem):
    row_id = lax.axis_index('rows')
    other = {'rows': (row_id + 2) % 4}
    iy_copy = pltpu.make_async_copy(iy_ref, iy_raw, loc.at[4])
    iy_copy.start()
    trips = [(y_ref, y_in, y_out), (wy_ref, wy_in, wy_out), (wx_ref, wx_in, wx_out), (ix_ref, ix_in, ix_out)]
    locs = [pltpu.make_async_copy(a, b, loc.at[i]) for i, (a, b, _) in enumerate(trips)]
    for cp in locs:
        cp.start()
    barrier = pltpu.get_barrier_semaphore()
    pl.semaphore_signal(barrier, inc=1, device_id=other, device_id_type=pl.DeviceIdType.MESH)
    iy_copy.wait()
    slot = lax.broadcasted_iota(jnp.int32, iy_in.shape, 1)
    iy_in[...] = jnp.where(slot < n_ref[0], iy_raw[...] - row_id * 256, -1000)
    pl.semaphore_wait(barrier, 1)
    trips.append((iy_in, None, iy_out))
    sends = [pltpu.make_async_remote_copy(src_ref=a, dst_ref=b, send_sem=ssem.at[i], recv_sem=rsem.at[i], device_id=other, device_id_type=pl.DeviceIdType.MESH) for i, (a, _, b) in enumerate(trips)]
    for cp in sends:
        cp.start()
    for cp in locs:
        cp.wait()
    payload(y_in, wy_in, wx_in, iy_in, ix_in, pay)
    ranks(iy_in, oh, rank)

    @pl.loop(0, SAMPLES // RUN)
    def _(s):
        d_out[s] = reorder(s, pay, rank, pt)

    for cp in sends:
        cp.wait()


def sort_scratch():
    return [pltpu.VMEM((160, SAMPLES), BF), pltpu.VMEM((80 * (SAMPLES // RUN), RUN), BF), pltpu.VMEM((1, SAMPLES), F32), pltpu.VMEM((RUN, SAMPLES), BF)]


def exchange(y, wy, wx, iy, ix, n):
    vm = pl.BlockSpec(memory_space=pltpu.VMEM)
    anym = pl.BlockSpec(memory_space=pl.ANY)
    dma = pltpu.SemaphoreType.DMA
    raw = (y, wy, wx, iy, ix)
    return pl.pallas_call(
        exchange_kernel,
        out_shape=tuple(jax.ShapeDtypeStruct(v.shape, v.dtype) for v in raw) + (jax.ShapeDtypeStruct((SAMPLES // RUN, 160, RUN), BF),),
        in_specs=[anym, anym, anym, anym, anym, pl.BlockSpec(memory_space=pltpu.SMEM)],
        out_specs=(vm,) * 6,
        scratch_shapes=[pltpu.VMEM(v.shape, v.dtype) for v in raw + (iy,)] + sort_scratch() + [dma((5,)), dma((5,)), dma((5,))],
        compiler_params=pltpu.CompilerParams(vmem_limit_bytes=12 * 2**20, collective_id=1, has_side_effects=True),
        cost_estimate=pl.CostEstimate(flops=10**9, bytes_accessed=10**6, transcendentals=0),
        name='exchange',
    )(y, wy, wx, iy, ix, n)


def spread_kernel(y_ref, wy_ref, wx_ref, iy_ref, ix_ref, d_own, tab, h_ref, e_ref,
                  n_buf, d_nb, pay, oh, rank, pt, acc, a_buf, b_buf, g_buf, hs, t_buf, sem):
    x_id = lax.axis_index('rows') // 2
    my_cols = pl.ds(pl.multiple_of(x_id * 256, 256), 256)
    copies = [
        pltpu.make_async_copy(tab.at[0, my_cols], t_buf.at[0, :, pl.ds(0, GRID)], sem.at[0]),
        pltpu.make_async_copy(tab.at[1, my_cols], t_buf.at[1, :, pl.ds(0, GRID)], sem.at[1]),
        pltpu.make_async_copy(tab.at[0, my_cols], t_buf.at[1, :, pl.ds(GRID, GRID)], sem.at[2]),
    ]
    for cp in copies:
        cp.start()
    zero = jnp.zeros((16, RUN), BF)

    def run(d_ref, s):
        first = jnp.sum(jnp.where(lax.broadcasted_iota(jnp.int32, (1, RUN), 1) == 0, d_ref[s, 128:129, :].astype(F32), 0.0)).astype(jnp.int32) - 1
        last = jnp.max(d_ref[s, 128:129, :].astype(F32)).astype(jnp.int32) + 1
        uc = d_ref[s, 144:160, :]
        eb = [d_ref[s, 96 + 16 * j:112 + 16 * j, :] for j in range(2)]
        for g in range(64):
            b_buf[16 * g:16 * g + 16, :] = jnp.where(uc == jnp.array(g, BF), eb[0], jnp.where(uc == jnp.array((g - 1) % 64, BF), eb[1], zero))

        @pl.loop(0, (last - first + WIN) // WIN)
        def _(w):
            g0 = first + WIN * w
            rel = (d_ref[s, 128:144, :].astype(F32) - (g0 + 1).astype(F32)).astype(BF)
            for gi in range(WIN):
                m = [rel == jnp.array(gi - j, BF) for j in range(3)]
                for q in range(2):
                    e = [d_ref[s, 48 * q + 16 * j:48 * q + 16 * j + 16, :] for j in range(3)]
                    a_buf[16 * (WIN * q + gi):16 * (WIN * q + gi) + 16, :] = jnp.where(m[0], e[0], jnp.where(m[1], e[1], jnp.where(m[2], e[2], zero)))
            prod = lax.dot_general(a_buf[...], b_buf[...], NT, preferred_element_type=F32)
            rows = pl.ds(pl.multiple_of(g0 * 16, 16), 16 * WIN)
            for q in range(2):
                acc[q, rows, :] += prod[16 * WIN * q:16 * WIN * (q + 1)]

    def block(o, d_ref, n_runs):
        acc[...] = jnp.zeros_like(acc)

        @pl.loop(0, n_runs)
        def _(s):
            run(d_ref, s)

        for q in range(2):
            e_ref[o, q, 0:32] = acc[q, 0:32, :]
            e_ref[o, q, 32:64] = acc[q, 1024:1056, :]
            g_buf[:, GRID * q:GRID * (q + 1)] = acc[q, 16:1040, :].astype(BF)
        for e in range(2):
            prod = lax.dot_general(g_buf[...], t_buf[e], NT, preferred_element_type=F32)
            for hc in range(2):
                hs[2 * e + hc] = prod[:, 128 * hc:128 * hc + 128]
        for e in range(2):
            for hc in range(2):
                for c in range(4):
                    h_ref[o, hc, e, :, 128 * c:128 * c + 128] = hs[2 * e + hc, pl.ds(c, 256, stride=4), :].astype(BF)

    n_own = (n_buf[0] + (RUN - 1)) // RUN
    n_nb = (jnp.sum(jnp.where(iy_ref[...] >= 0, 1.0, 0.0)).astype(jnp.int32) + (RUN - 1)) // RUN
    for cp in copies:
        cp.wait()
    t_buf[0, :, GRID:] = -t_buf[1, :, :GRID]
    payload(y_ref, wy_ref, wx_ref, iy_ref, ix_ref, pay)
    ranks(iy_ref, oh, rank)

    @pl.loop(0, n_nb)
    def _(s):
        d_nb[s] = reorder(s, pay, rank, pt)

    block(0, d_own, n_own)
    block(1, d_nb, n_nb)


def spread(y, wy, wx, iy, ix, d_own, tab, n):
    vm = pl.BlockSpec(memory_space=pltpu.VMEM)
    return pl.pallas_call(
        lambda *refs: spread_kernel(*refs[:7], *refs[8:10], refs[7], *refs[10:]),
        out_shape=(jax.ShapeDtypeStruct((2, 2, 2, 256, 512), BF), jax.ShapeDtypeStruct((2, 2, 64, 1024), F32)),
        in_specs=[vm, vm, vm, vm, vm, vm, pl.BlockSpec(memory_space=pl.ANY), pl.BlockSpec(memory_space=pltpu.SMEM)],
        out_specs=(vm, vm),
        scratch_shapes=[pltpu.VMEM((SAMPLES // RUN, 160, RUN), BF)] + sort_scratch() + [
            pltpu.VMEM((2, 16 * (66 + WIN), GRID), F32),
            pltpu.VMEM((32 * WIN, RUN), BF),
            pltpu.VMEM((GRID, RUN), BF),
            pltpu.VMEM((1024, 2 * GRID), BF),
            pltpu.VMEM((4, 1024, 128), F32),
            pltpu.VMEM((2, 256, 2 * GRID), BF),
            pltpu.SemaphoreType.DMA((3,)),
        ],
        compiler_params=pltpu.CompilerParams(vmem_limit_bytes=40 * 2**20),
        cost_estimate=pl.CostEstimate(flops=13 * 10**9, bytes_accessed=4 * 2**20, transcendentals=0),
        name='spread',
    )(y, wy, wx, iy, ix, d_own, tab, n)


def combine_kernel(hh, ee, tab, maps, dd, out_ref,
                   t3, rhs, sbuf, s_vm, rx, ge, hs, pt, part, rx2, scale,
                   loc, esend, erecv, hsend, hrecv, psend, precv, ysend, yrecv):
    n_grid = 1024
    row_id = lax.axis_index('rows')
    y_id = lax.axis_index('coil')
    core = row_id % 2
    x_id = row_id // 2
    sib = {'rows': row_id + 1 - 2 * core}
    mate = {'coil': 1 - y_id}
    blocks = [row_id, (row_id + 2) % 4]

    n_loc = 0
    t_copies = []
    for src, dst in ((tab.at[0], t3.at[0, :, pl.ds(0, n_grid)]), (tab.at[1], t3.at[1, :, pl.ds(0, n_grid)]), (tab.at[0], t3.at[1, :, pl.ds(n_grid, n_grid)])):
        t_copies.append(pltpu.make_async_copy(src, dst, loc.at[n_loc]))
        n_loc += 1
    h_copies = []
    for o in range(2):
        for b in range(2):
            h_copies.append(pltpu.make_async_copy(hh.at[o, core, b], rhs.at[b, blocks[o]], loc.at[n_loc]))
            n_loc += 1
            for end in range(2):
                h_copies.append(pltpu.make_async_copy(hh.at[o, 1 - core, b, pl.ds(240 * end, 16)], sbuf.at[o, b, end], loc.at[n_loc]))
                n_loc += 1
    s_copy = pltpu.make_async_copy(maps, s_vm, loc.at[n_loc])
    for cp in t_copies + h_copies:
        cp.start()

    barrier = pltpu.get_barrier_semaphore()
    pl.semaphore_signal(barrier, inc=1, device_id=sib, device_id_type=pl.DeviceIdType.MESH)
    pl.semaphore_signal(barrier, inc=1, device_id=mate, device_id_type=pl.DeviceIdType.MESH)
    pl.semaphore_wait(barrier, 2)

    def remote(src, dst, ssem, rsem, dev):
        return pltpu.make_async_remote_copy(src_ref=src, dst_ref=dst, send_sem=ssem, recv_sem=rsem, device_id=dev, device_id_type=pl.DeviceIdType.MESH)

    e_copies = []
    for o in range(2):
        low = o * core + (1 - o) * (1 - core)
        high = o * (1 - core) + (1 - o) * core
        for k, (slot, end, row0) in enumerate(((low, 1, 0), (high, 0, 48))):
            e_copies.append(remote(ee.at[o, :, pl.ds(row0, 16)], rx.at[slot, end], esend.at[2 * o + k], erecv.at[slot, end], sib))
    for cp in e_copies:
        cp.start()
    hr_copies = []
    for o in range(2):
        for b in range(2):
            hr_copies.append(remote(hh.at[o, 1 - core, b, pl.ds(16, 224)], rhs.at[b, blocks[o], pl.ds(16, 224)], hsend.at[o, b], hrecv.at[o, b], sib))
    for cp in hr_copies:
        cp.start()
    s_copy.start()
    row_scale = jnp.broadcast_to(dd[:, pl.ds(pl.multiple_of(y_id * 256, 256), 256)], (128, 256)).T
    scale[...] = row_scale * dd[:, pl.ds(pl.multiple_of(row_id * 128, 128), 128)]

    for cp in t_copies:
        cp.wait()
    t3[0, :, n_grid:] = -t3[1, :, :n_grid]
    for cp in e_copies:
        cp.wait_send()
    for o in range(2):
        for end in range(2):
            remote(rx.at[o, end], rx.at[o, end], esend.at[2 * o + end], erecv.at[o, end], sib).wait_recv()
            for q in range(2):
                ge[32 * o + 16 * end:32 * o + 16 * end + 16, n_grid * q:n_grid * (q + 1)] = (ee[o, q, 16 + 16 * end:32 + 16 * end, :] + rx[o, end, q]).astype(BF)
    cols = pl.ds(pl.multiple_of(x_id * 256, 256), 256)
    for e in range(2):
        prod = lax.dot_general(ge[...], t3[e, cols, :], NT, preferred_element_type=F32)
        for hc in range(2):
            hs[2 * e + hc] = prod[:, 128 * hc:128 * hc + 128]
    for cp in h_copies:
        cp.wait()
    p_copies = []
    n_p = 0
    for o in range(2):
        for end in range(2):
            for b in range(2):
                for mine in range(2):
                    hc = core if mine else 1 - core
                    rows = pl.ds(240 * end, 16)
                    if mine:
                        pt[...] = rhs[b, blocks[o], rows, :].astype(F32)
                    else:
                        pt[...] = sbuf[o, b, end].astype(F32)
                    for c in range(4):
                        pt[12 * end:12 * end + 4, 128 * c:128 * c + 128] = hs[2 * b + hc, pl.ds(32 * o + 16 * end + c, 4, stride=4), :]
                    if mine:
                        rhs[b, blocks[o], rows, :] = pt[...].astype(BF)
                    else:
                        sbuf[o, b, end] = pt[...].astype(BF)
                        cp = remote(sbuf.at[o, b, end], rhs.at[b, blocks[o], rows], psend.at[n_p], precv.at[n_p], sib)
                        cp.start()
                        p_copies.append(cp)
                        n_p += 1
    s_copy.wait()
    for cp in hr_copies + p_copies:
        cp.wait()

    def image_rows(i0, size):
        rows = pl.ds(pl.multiple_of(i0, size), size)
        w = rhs[...].reshape(2048, 512)
        im = [jnp.dot(t3[e, rows, :], w, preferred_element_type=F32) for e in range(2)]
        xr = jnp.zeros((size, 128), F32)
        xi = jnp.zeros((size, 128), F32)
        for c in range(4):
            ir = im[0][:, 128 * c:128 * c + 128]
            ii = im[1][:, 128 * c:128 * c + 128]
            sr = s_vm[0, c, rows, :]
            si = s_vm[1, c, rows, :]
            xr = xr + (sr * ir + si * ii)
            xi = xi + (sr * ii - si * ir)
        return xr, xi

    y_copies = []
    for k in range(2):
        xr, xi = image_rows((1 - y_id) * 256 + 128 * k, 128)
        part[0, 128 * k:128 * k + 128] = xr
        part[1, 128 * k:128 * k + 128] = xi
        cp = remote(part.at[:, pl.ds(128 * k, 128)], rx2.at[:, pl.ds(128 * k, 128)], ysend.at[k], yrecv.at[k], mate)
        cp.start()
        y_copies.append(cp)
    for k in range(2):
        xr, xi = image_rows(y_id * 256 + 128 * k, 128)
        out_ref[0, 128 * k:128 * k + 128] = xr
        out_ref[1, 128 * k:128 * k + 128] = xi
    for k in range(2):
        y_copies[k].wait()
        sl = slice(128 * k, 128 * k + 128)
        for e in range(2):
            out_ref[e, sl] = (out_ref[e, sl] + rx2[e, sl]) * scale[sl]


def combine(hh, ee, tab, maps, dd):
    vm = pl.BlockSpec(memory_space=pltpu.VMEM)
    anym = pl.BlockSpec(memory_space=pl.ANY)
    dma = pltpu.SemaphoreType.DMA
    return pl.pallas_call(
        combine_kernel,
        out_shape=jax.ShapeDtypeStruct((2, 256, 128), F32),
        in_specs=[anym, vm, anym, anym, vm],
        out_specs=vm,
        scratch_shapes=[
            pltpu.VMEM((2, 512, 2048), BF),
            pltpu.VMEM((2, 4, 256, 512), BF),
            pltpu.VMEM((2, 2, 2, 16, 512), BF),
            pltpu.VMEM((2, 4, 512, 128), F32),
            pltpu.VMEM((2, 2, 2, 16, 1024), F32),
            pltpu.VMEM((64, 2048), BF),
            pltpu.VMEM((4, 64, 128), F32),
            pltpu.VMEM((16, 512), F32),
            pltpu.VMEM((2, 256, 128), F32),
            pltpu.VMEM((2, 256, 128), F32),
            pltpu.VMEM((256, 128), F32),
            dma((16,)), dma((4,)), dma((2, 2)), dma((2, 2)), dma((2, 2)), dma((8,)), dma((8,)), dma((2,)), dma((2,)),
        ],
        compiler_params=pltpu.CompilerParams(vmem_limit_bytes=40 * 2**20, collective_id=0, has_side_effects=True),
        cost_estimate=pl.CostEstimate(flops=3 * 10**9, bytes_accessed=12 * 2**20, transcendentals=0),
        name='combine',
    )(hh, ee, tab, maps, dd)


def solution(mesh):
    def local_part(kspace, weight_row, weight_col, grid_row, grid_col, valid_count, coil_maps, deapod):
        n_img = deapod.shape[0]
        hbm = [pltpu.with_memory_space_constraint(v, pltpu.HBM) for v in (kspace, weight_row, weight_col, grid_row[None], grid_col[None])]
        stacked = exchange(*hbm, valid_count)
        tab = jnp.asarray(tables(n_img))
        hh, ee = spread(*stacked, tab, valid_count)
        return combine(hh, ee, tab, coil_maps, deapod[None])

    spec_samples = P(None, 'coil', ('slab', 'rows'))
    spec_weights = P(None, ('slab', 'rows'))
    spec_index = P(('slab', 'rows'))
    return jax.shard_map(local_part, mesh=mesh, in_specs=(spec_samples, spec_weights, spec_weights, spec_index, spec_index, spec_index, P(None, 'coil', 'slab', 'rows'), P()), out_specs=P(None, ('slab', 'coil'), 'rows'), check_vma=False)
```

```python
import math
import functools
import numpy as np
import jax
import jax.numpy as jnp
from jax import lax
from jax.experimental import pallas as pl
from jax.experimental.pallas import tpu as pltpu
from jax.sharding import PartitionSpec as P

F32 = jnp.float32
BF = jnp.bfloat16
NT = (((1,), (1,)), ((), ()))
KC = 512
GRID = 1024
SAMPLES = 2048
RUN = 256
WIN = 12


def tables(n_img):
    n_grid = 2 * n_img
    pix = np.arange(n_img) - n_img // 2
    freq = np.arange(n_grid) - n_img
    ang = np.mod(pix[:, None] * freq[None, :], n_grid) * (2.0 * math.pi / n_grid)
    return np.stack([np.cos(ang), np.sin(ang)]).astype(np.float32).astype(BF)


def payload(y_ref, wy_ref, wx_ref, iy_ref, ix_ref, pay):
    @pl.loop(0, SAMPLES // KC)
    def _(s):
        cols = pl.ds(pl.multiple_of(s * KC, KC), KC)
        sub = lax.broadcasted_iota(jnp.int32, (16, KC), 0)
        r0 = iy_ref[:, cols] + 1
        counted = r0 > 0
        t = jnp.where(counted, (sub >> 2) - (r0 & 3), 100)
        for q in range(2):
            y16 = jnp.zeros((16, KC), F32)
            for c in range(4):
                y16 = jnp.where((sub & 3) == c, y_ref[q, c:c + 1, cols], y16)
            coef = [y16 * wy_ref[a:a + 1, cols] for a in range(6)]
            for j in range(3):
                e = jnp.zeros((16, KC), F32)
                for a in range(6):
                    if -3 <= a - 4 * j <= 3:
                        e = jnp.where(t == a - 4 * j, coef[a], e)
                pay[48 * q + 16 * j:48 * q + 16 * j + 16, cols] = e.astype(BF)
        c0 = (ix_ref[:, cols] + (GRID - 3)) & (GRID - 1)
        tc = jnp.where(counted, sub - (c0 & 15), 100)
        for j in range(2):
            e = jnp.zeros((16, KC), F32)
            for b in range(6):
                e = jnp.where(tc == b - 16 * j, wx_ref[b:b + 1, cols], e)
            pay[96 + 16 * j:112 + 16 * j, cols] = e.astype(BF)
        pay[128:144, cols] = jnp.broadcast_to(((r0 >> 2) + 1).astype(F32), (16, KC)).astype(BF)
        pay[144:160, cols] = jnp.broadcast_to((c0 >> 4).astype(F32), (16, KC)).astype(BF)


def iota16():
    return lax.broadcasted_iota(jnp.int32, (16, 1), 0).astype(F32)


def ranks(iy_ref, oh, rank):
    n_run = SAMPLES // RUN
    for ch in range(n_run):
        lanes = slice(RUN * ch, RUN * ch + RUN)
        bucket = jnp.broadcast_to(((iy_ref[:, lanes] + 1) >> 2).astype(F32), (16, RUN)).astype(BF)
        for g in range(5):
            oh[80 * ch + 16 * g:80 * ch + 16 * g + 16, :] = jnp.where(bucket == (iota16() + 16 * g).astype(BF), jnp.ones((), BF), jnp.zeros((), BF))
    lower = lax.broadcasted_iota(jnp.int32, (RUN, RUN + 128), 0)
    upper = lax.broadcasted_iota(jnp.int32, (RUN, RUN + 128), 1)
    tri = jnp.where((lower < upper) | (upper >= RUN), 1.0, 0.0).astype(BF)
    pre = jnp.dot(oh[...], tri, preferred_element_type=F32)
    counts = [pre[80 * ch:80 * ch + 80, RUN:] for ch in range(n_run)]
    total = counts[0]
    for ch in range(1, n_run):
        total = total + counts[ch]
    high = jnp.floor(total * (1.0 / 256.0))
    low = total - 256.0 * high
    strict = jnp.where(lax.broadcasted_iota(jnp.int32, (80, 80), 1) < lax.broadcasted_iota(jnp.int32, (80, 80), 0), 1.0, 0.0).astype(BF)
    base = 256.0 * jnp.dot(strict, high.astype(BF), preferred_element_type=F32) + jnp.dot(strict, low.astype(BF), preferred_element_type=F32)
    for ch in range(n_run):
        lanes = slice(RUN * ch, RUN * ch + RUN)
        place = pre[80 * ch:80 * ch + 80, :RUN] + jnp.concatenate([base] * (RUN // 128), axis=1)
        place = jnp.sum(oh[80 * ch:80 * ch + 80, :].astype(F32) * place, axis=0, keepdims=True)
        rank[:, lanes] = jnp.where(iy_ref[:, lanes] >= 0, place, -1.0)
        base = base + counts[ch]


def reorder(s, pay, rank, pt):
    place = jnp.broadcast_to(rank[...] - (s * RUN).astype(F32), (16, SAMPLES)).astype(BF)
    for g in range(RUN // 16):
        pt[16 * g:16 * g + 16, :] = jnp.where(place == (iota16() + 16 * g).astype(BF), jnp.ones((), BF), jnp.zeros((), BF))
    return lax.dot_general(pay[...], pt[...], NT, preferred_element_type=F32).astype(BF)


def exchange_kernel(y_ref, wy_ref, wx_ref, iy_ref, ix_ref, n_ref, y_out, wy_out, wx_out, iy_out, ix_out, d_out,
                    y_in, wy_in, wx_in, iy_in, ix_in, iy_raw, pay, oh, rank, pt, loc, ssem, rsem):
    row_id = lax.axis_index('rows')
    other = {'rows': (row_id + 2) % 4}
    iy_copy = pltpu.make_async_copy(iy_ref, iy_raw, loc.at[4])
    iy_copy.start()
    trips = [(y_ref, y_in, y_out), (wy_ref, wy_in, wy_out), (wx_ref, wx_in, wx_out), (ix_ref, ix_in, ix_out)]
    locs = [pltpu.make_async_copy(a, b, loc.at[i]) for i, (a, b, _) in enumerate(trips)]
    for cp in locs:
        cp.start()
    barrier = pltpu.get_barrier_semaphore()
    pl.semaphore_signal(barrier, inc=1, device_id=other, device_id_type=pl.DeviceIdType.MESH)
    iy_copy.wait()
    slot = lax.broadcasted_iota(jnp.int32, iy_in.shape, 1)
    iy_in[...] = jnp.where(slot < n_ref[0], iy_raw[...] - row_id * 256, -1000)
    pl.semaphore_wait(barrier, 1)
    trips.append((iy_in, None, iy_out))
    sends = [pltpu.make_async_remote_copy(src_ref=a, dst_ref=b, send_sem=ssem.at[i], recv_sem=rsem.at[i], device_id=other, device_id_type=pl.DeviceIdType.MESH) for i, (a, _, b) in enumerate(trips)]
    for cp in sends:
        cp.start()
    for cp in locs:
        cp.wait()
    payload(y_in, wy_in, wx_in, iy_in, ix_in, pay)
    ranks(iy_in, oh, rank)

    @pl.loop(0, SAMPLES // RUN)
    def _(s):
        d_out[s] = reorder(s, pay, rank, pt)

    for cp in sends:
        cp.wait()


def sort_scratch():
    return [pltpu.VMEM((160, SAMPLES), BF), pltpu.VMEM((80 * (SAMPLES // RUN), RUN), BF), pltpu.VMEM((1, SAMPLES), F32), pltpu.VMEM((RUN, SAMPLES), BF)]


def exchange(y, wy, wx, iy, ix, n):
    vm = pl.BlockSpec(memory_space=pltpu.VMEM)
    anym = pl.BlockSpec(memory_space=pl.ANY)
    dma = pltpu.SemaphoreType.DMA
    raw = (y, wy, wx, iy, ix)
    return pl.pallas_call(
        exchange_kernel,
        out_shape=tuple(jax.ShapeDtypeStruct(v.shape, v.dtype) for v in raw) + (jax.ShapeDtypeStruct((SAMPLES // RUN, 160, RUN), BF),),
        in_specs=[anym, anym, anym, anym, anym, pl.BlockSpec(memory_space=pltpu.SMEM)],
        out_specs=(vm,) * 6,
        scratch_shapes=[pltpu.VMEM(v.shape, v.dtype) for v in raw + (iy,)] + sort_scratch() + [dma((5,)), dma((5,)), dma((5,))],
        compiler_params=pltpu.CompilerParams(vmem_limit_bytes=12 * 2**20, collective_id=1, has_side_effects=True),
        cost_estimate=pl.CostEstimate(flops=10**9, bytes_accessed=10**6, transcendentals=0),
        name='exchange',
    )(y, wy, wx, iy, ix, n)


def spread_kernel(y_ref, wy_ref, wx_ref, iy_ref, ix_ref, d_own, n_ref, g_ref, e_ref, d_nb, pay, oh, rank, pt, acc, a_buf, b_buf):
    zero = jnp.zeros((16, RUN), BF)

    def run(d_ref, s):
        first = jnp.sum(jnp.where(lax.broadcasted_iota(jnp.int32, (1, RUN), 1) == 0, d_ref[s, 128:129, :].astype(F32), 0.0)).astype(jnp.int32) - 1
        last = jnp.max(d_ref[s, 128:129, :].astype(F32)).astype(jnp.int32) + 1
        uc = d_ref[s, 144:160, :]
        eb = [d_ref[s, 96 + 16 * j:112 + 16 * j, :] for j in range(2)]
        for g in range(64):
            b_buf[16 * g:16 * g + 16, :] = jnp.where(uc == jnp.array(g, BF), eb[0], jnp.where(uc == jnp.array((g - 1) % 64, BF), eb[1], zero))

        @pl.loop(0, (last - first + WIN) // WIN)
        def _(w):
            g0 = first + WIN * w
            rel = (d_ref[s, 128:144, :].astype(F32) - (g0 + 1).astype(F32)).astype(BF)
            for gi in range(WIN):
                m = [rel == jnp.array(gi - j, BF) for j in range(3)]
                for q in range(2):
                    e = [d_ref[s, 48 * q + 16 * j:48 * q + 16 * j + 16, :] for j in range(3)]
                    a_buf[16 * (WIN * q + gi):16 * (WIN * q + gi) + 16, :] = jnp.where(m[0], e[0], jnp.where(m[1], e[1], jnp.where(m[2], e[2], zero)))
            prod = lax.dot_general(a_buf[...], b_buf[...], NT, preferred_element_type=F32)
            rows = pl.ds(pl.multiple_of(g0 * 16, 16), 16 * WIN)
            for q in range(2):
                acc[q, rows, :] += prod[16 * WIN * q:16 * WIN * (q + 1)]

    def block(o, d_ref, n_runs):
        acc[...] = jnp.zeros_like(acc)

        @pl.loop(0, n_runs)
        def _(s):
            run(d_ref, s)

        for q in range(2):
            e_ref[o, q, 0:32] = acc[q, 0:32, :]
            e_ref[o, q, 32:64] = acc[q, 1024:1056, :]
            g_ref[o, :, GRID * q:GRID * (q + 1)] = acc[q, 16:1040, :].astype(BF)

    n_own = (n_ref[0] + (RUN - 1)) // RUN
    n_nb = (jnp.sum(jnp.where(iy_ref[...] >= 0, 1.0, 0.0)).astype(jnp.int32) + (RUN - 1)) // RUN
    payload(y_ref, wy_ref, wx_ref, iy_ref, ix_ref, pay)
    ranks(iy_ref, oh, rank)

    @pl.loop(0, n_nb)
    def _(s):
        d_nb[s] = reorder(s, pay, rank, pt)

    block(0, d_own, n_own)
    block(1, d_nb, n_nb)


def spread(y, wy, wx, iy, ix, d_own, n):
    vm = pl.BlockSpec(memory_space=pltpu.VMEM)
    return pl.pallas_call(
        spread_kernel,
        out_shape=(jax.ShapeDtypeStruct((2, 1024, 2 * GRID), BF), jax.ShapeDtypeStruct((2, 2, 64, GRID), F32)),
        in_specs=[vm, vm, vm, vm, vm, vm, pl.BlockSpec(memory_space=pltpu.SMEM)],
        out_specs=(vm, vm),
        scratch_shapes=[pltpu.VMEM((SAMPLES // RUN, 160, RUN), BF)] + sort_scratch() + [
            pltpu.VMEM((2, 16 * (66 + WIN), GRID), F32),
            pltpu.VMEM((32 * WIN, RUN), BF),
            pltpu.VMEM((GRID, RUN), BF),
        ],
        compiler_params=pltpu.CompilerParams(vmem_limit_bytes=28 * 2**20),
        cost_estimate=pl.CostEstimate(flops=13 * 10**9, bytes_accessed=4 * 2**20, transcendentals=0),
        name='spread',
    )(y, wy, wx, iy, ix, d_own, n)


def combine_kernel(gg, ee, tab, maps, dd, out_ref, hbuf, hs, ge, rx, s_all, part, rx2, scale,
                   esend, erecv, ssem, hsend, hrecv, ysend, yrecv):
    row_id = lax.axis_index('rows')
    y_id = lax.axis_index('coil')
    core = row_id % 2
    x_id = row_id // 2
    sib_row = row_id + 1 - 2 * core
    sib = {'rows': sib_row}
    mate = {'coil': 1 - y_id, 'rows': sib_row}
    blocks = [row_id, (row_id + 2) % 4]

    barrier = pltpu.get_barrier_semaphore()
    pl.semaphore_signal(barrier, inc=1, device_id=sib, device_id_type=pl.DeviceIdType.MESH)
    pl.semaphore_signal(barrier, inc=1, device_id=mate, device_id_type=pl.DeviceIdType.MESH)
    half = lambda y: pl.ds(pl.multiple_of(y * 256, 256), 256)
    s_copy = pltpu.make_async_copy(maps.at[:, :, half(y_id)], s_all.at[core], ssem.at[0])
    s_copy.start()
    row_scale = jnp.broadcast_to(dd[:, half(y_id)], (128, 256)).T
    scale[...] = row_scale * dd[:, pl.ds(pl.multiple_of(row_id * 128, 128), 128)]
    pl.semaphore_wait(barrier, 2)

    def remote(src, dst, send, recv, dev):
        return pltpu.make_async_remote_copy(src_ref=src, dst_ref=dst, send_sem=send, recv_sem=recv, device_id=dev, device_id_type=pl.DeviceIdType.MESH)

    e_copies = []
    for o in range(2):
        low = o * core + (1 - o) * (1 - core)
        high = o * (1 - core) + (1 - o) * core
        for k, (slot, end, row0) in enumerate(((low, 1, 0), (high, 0, 48))):
            e_copies.append(remote(ee.at[o, :, pl.ds(row0, 16)], rx.at[slot, end], esend.at[2 * o + k], erecv.at[slot, end], sib))
    for cp in e_copies:
        cp.start()
    s_send = remote(maps.at[:, :, half(1 - y_id)], s_all.at[core], ssem.at[1], ssem.at[2], sib)
    s_send.start()
    s_recv = remote(maps.at[:, :, half(1 - y_id)], s_all.at[1 - core], ssem.at[1], ssem.at[2], sib)

    def columns(hc, lhs):
        cols = pl.ds(pl.multiple_of(x_id * 256 + hc * 128, 128), 128)
        t2 = jnp.concatenate([tab[0, cols, :], tab[1, cols, :]], axis=0)
        pr = lax.dot_general(lhs(0), t2, NT, preferred_element_type=F32)
        pi = lax.dot_general(lhs(1), t2, NT, preferred_element_type=F32)
        return pr[:, :128] - pi[:, 128:], pr[:, 128:] + pi[:, :128]

    def transform(hc, o):
        for k in range(2):
            rows = slice(512 * k, 512 * k + 512)
            pair = columns(hc, lambda q: gg[o, rows, GRID * q:GRID * (q + 1)])
            for e in range(2):
                hs[o, e, rows] = pair[e]

    def take_halos():
        for cp in e_copies:
            cp.wait_send()
        for o in range(2):
            for end in range(2):
                remote(rx.at[o, end], rx.at[o, end], esend.at[2 * o + end], erecv.at[o, end], sib).wait_recv()
                for q in range(2):
                    ge[32 * o + 16 * end:32 * o + 16 * end + 16, GRID * q:GRID * (q + 1)] = (ee[o, q, 16 + 16 * end:32 + 16 * end, :] + rx[o, end, q]).astype(BF)

    def patch(hc):
        pair = columns(hc, lambda q: ge[:, GRID * q:GRID * (q + 1)])
        return pair

    h_copies = [[remote(hbuf.at[hc, blocks[o]], hbuf.at[hc, blocks[o]], hsend.at[hc, o], hrecv.at[hc, o], sib) for o in range(2)] for hc in range(2)]

    def send(hc, o, pair):
        for e in range(2):
            for end in range(2):
                hs[o, e, 1008 * end:1008 * end + 16] = pair[e][32 * o + 16 * end:32 * o + 16 * end + 16]
            for c in range(4):
                hbuf[hc, blocks[o], e, :, 128 * c:128 * c + 128] = hs[o, e, pl.ds(c, 256, stride=4), :].astype(BF)
        h_copies[hc][o].start()

    def image(hc):
        first = 256 * (y_id + (1 - 2 * y_id) * (core + hc - 2 * core * hc))
        for k in range(2):
            rows = pl.ds(pl.multiple_of(first + 128 * k, 128), 128)
            lhs = jnp.concatenate([tab[0, rows, :], tab[1, rows, :]], axis=0)
            mr = jnp.dot(lhs, hbuf[hc, :, 0].reshape(1024, 512), preferred_element_type=F32)
            mi = jnp.dot(lhs, hbuf[hc, :, 1].reshape(1024, 512), preferred_element_type=F32)
            re = mr[:128] - mi[128:]
            im = mr[128:] + mi[:128]
            xr = jnp.zeros((128, 128), F32)
            xi = jnp.zeros((128, 128), F32)
            sl = slice(128 * k, 128 * k + 128)
            for c in range(4):
                ir = re[:, 128 * c:128 * c + 128]
                ii = im[:, 128 * c:128 * c + 128]
                sr = s_all[hc, 0, c, sl, :]
                si = s_all[hc, 1, c, sl, :]
                xr = xr + (sr * ir + si * ii)
                xi = xi + (sr * ii - si * ir)
            part[hc, 0, sl] = xr
            part[hc, 1, sl] = xi

            @pl.when(core != hc)
            def _():
                y_copies[k].start()

    y_copies = [remote(part.at[1 - core, :, pl.ds(128 * k, 128)], rx2.at[:, pl.ds(128 * k, 128)], ysend.at[k], yrecv.at[k], mate) for k in range(2)]

    transform(0, 0)
    take_halos()
    pair = patch(0)
    send(0, 0, pair)
    transform(0, 1)
    send(0, 1, pair)
    transform(1, 0)
    pair = patch(1)
    send(1, 0, pair)
    s_copy.wait()
    s_send.wait_send()
    s_recv.wait_recv()
    for o in range(2):
        h_copies[0][o].wait()
    image(0)
    transform(1, 1)
    send(1, 1, pair)
    for o in range(2):
        h_copies[1][o].wait()
    image(1)
    for k in range(2):
        y_copies[k].wait()
        sl = slice(128 * k, 128 * k + 128)
        for e in range(2):
            out_ref[e, sl] = (part[core, e, sl] + rx2[e, sl]) * scale[sl]


def combine(gg, ee, tab, maps, dd):
    vm = pl.BlockSpec(memory_space=pltpu.VMEM)
    dma = pltpu.SemaphoreType.DMA
    return pl.pallas_call(
        combine_kernel,
        out_shape=jax.ShapeDtypeStruct((2, 256, 128), F32),
        in_specs=[vm] * 5,
        out_specs=vm,
        scratch_shapes=[
            pltpu.VMEM((2, 4, 2, 256, 512), BF),
            pltpu.VMEM((2, 2, 1024, 128), F32),
            pltpu.VMEM((64, 2 * GRID), BF),
            pltpu.VMEM((2, 2, 2, 16, GRID), F32),
            pltpu.VMEM((2, 2, 4, 256, 128), F32),
            pltpu.VMEM((2, 2, 256, 128), F32),
            pltpu.VMEM((2, 256, 128), F32),
            pltpu.VMEM((256, 128), F32),
            dma((4,)), dma((2, 2)), dma((3,)), dma((2, 2)), dma((2, 2)), dma((2,)), dma((2,)),
        ],
        compiler_params=pltpu.CompilerParams(vmem_limit_bytes=24 * 2**20, collective_id=0, has_side_effects=True),
        cost_estimate=pl.CostEstimate(flops=7 * 10**9, bytes_accessed=12 * 2**20, transcendentals=0),
        name='combine',
    )(gg, ee, tab, maps, dd)


def solution(mesh):
    def local_part(kspace, weight_row, weight_col, grid_row, grid_col, valid_count, coil_maps, deapod):
        n_img = deapod.shape[0]
        hbm = [pltpu.with_memory_space_constraint(v, pltpu.HBM) for v in (kspace, weight_row, weight_col, grid_row[None], grid_col[None])]
        stacked = exchange(*hbm, valid_count)
        tab = jnp.asarray(tables(n_img))
        gg, ee = spread(*stacked, valid_count)
        return combine(gg, ee, tab, coil_maps, deapod[None])

    spec_samples = P(None, 'coil', ('slab', 'rows'))
    spec_weights = P(None, ('slab', 'rows'))
    spec_index = P(('slab', 'rows'))
    return jax.shard_map(local_part, mesh=mesh, in_specs=(spec_samples, spec_weights, spec_weights, spec_index, spec_index, spec_index, P(None, 'coil', 'slab', 'rows'), P()), out_specs=P(None, ('slab', 'coil'), 'rows'), check_vma=False)
```

```python
import math
import functools
import numpy as np
import jax
import jax.numpy as jnp
from jax import lax
from jax.experimental import pallas as pl
from jax.experimental.pallas import tpu as pltpu
from jax.sharding import PartitionSpec as P

F32 = jnp.float32
BF = jnp.bfloat16
NT = (((1,), (1,)), ((), ()))
KC = 512
GRID = 1024
SAMPLES = 2048
RUN = 256
WIN = 16


def tables(n_img):
    n_grid = 2 * n_img
    pix = np.arange(n_img) - n_img // 2
    freq = np.arange(n_grid) - n_img
    ang = np.mod(pix[:, None] * freq[None, :], n_grid) * (2.0 * math.pi / n_grid)
    return np.stack([np.cos(ang), np.sin(ang)]).astype(np.float32).astype(BF)


def payload(y_ref, wy_ref, wx_ref, key_ref, pay):
    @pl.loop(0, SAMPLES // KC)
    def _(s):
        cols = pl.ds(pl.multiple_of(s * KC, KC), KC)
        sub = lax.broadcasted_iota(jnp.int32, (16, KC), 0)
        key = key_ref[:, cols]
        r0 = (key >> 10) + 1
        counted = r0 > 0
        t = jnp.where(counted, (sub >> 2) - (r0 & 3), 100)
        for q in range(2):
            y16 = jnp.zeros((16, KC), F32)
            for c in range(4):
                y16 = jnp.where((sub & 3) == c, y_ref[q, c:c + 1, cols], y16)
            coef = [y16 * wy_ref[a:a + 1, cols] for a in range(6)]
            for j in range(3):
                e = jnp.zeros((16, KC), F32)
                for a in range(6):
                    if -3 <= a - 4 * j <= 3:
                        e = jnp.where(t == a - 4 * j, coef[a], e)
                pay[48 * q + 16 * j:48 * q + 16 * j + 16, cols] = e.astype(BF)
        c0 = ((key & (GRID - 1)) + (GRID - 3)) & (GRID - 1)
        wx = wx_ref[:, cols].astype(F32)
        tc = jnp.where(counted, sub - (c0 & 15), 100)
        for j in range(2):
            e = jnp.zeros((16, KC), F32)
            for b in range(6):
                e = jnp.where(tc == b - 16 * j, wx[b:b + 1], e)
            pay[96 + 16 * j:112 + 16 * j, cols] = e.astype(BF)
        pay[128:144, cols] = jnp.broadcast_to(((r0 >> 2) + 1).astype(F32), (16, KC)).astype(BF)
        pay[144:160, cols] = jnp.broadcast_to((c0 >> 4).astype(F32), (16, KC)).astype(BF)


def iota16():
    return lax.broadcasted_iota(jnp.int32, (16, 1), 0).astype(F32)


def ranks(key_ref, oh, rank):
    n_run = SAMPLES // RUN
    for ch in range(n_run):
        lanes = slice(RUN * ch, RUN * ch + RUN)
        bucket = jnp.broadcast_to((((key_ref[:, lanes] >> 10) + 1) >> 2).astype(F32), (16, RUN)).astype(BF)
        for g in range(5):
            oh[80 * ch + 16 * g:80 * ch + 16 * g + 16, :] = jnp.where(bucket == (iota16() + 16 * g).astype(BF), jnp.ones((), BF), jnp.zeros((), BF))
    lower = lax.broadcasted_iota(jnp.int32, (RUN, RUN + 128), 0)
    upper = lax.broadcasted_iota(jnp.int32, (RUN, RUN + 128), 1)
    tri = jnp.where((lower < upper) | (upper >= RUN), 1.0, 0.0).astype(BF)
    pre = jnp.dot(oh[...], tri, preferred_element_type=F32)
    counts = [pre[80 * ch:80 * ch + 80, RUN:] for ch in range(n_run)]
    total = counts[0]
    for ch in range(1, n_run):
        total = total + counts[ch]
    high = jnp.floor(total * (1.0 / 256.0))
    low = total - 256.0 * high
    strict = jnp.where(lax.broadcasted_iota(jnp.int32, (80, 80), 1) < lax.broadcasted_iota(jnp.int32, (80, 80), 0), 1.0, 0.0).astype(BF)
    base = 256.0 * jnp.dot(strict, high.astype(BF), preferred_element_type=F32) + jnp.dot(strict, low.astype(BF), preferred_element_type=F32)
    for ch in range(n_run):
        lanes = slice(RUN * ch, RUN * ch + RUN)
        place = pre[80 * ch:80 * ch + 80, :RUN] + jnp.concatenate([base] * (RUN // 128), axis=1)
        place = jnp.sum(oh[80 * ch:80 * ch + 80, :].astype(F32) * place, axis=0, keepdims=True)
        place = jnp.where(key_ref[:, lanes] >= 0, place, -1.0)
        for k in range(RUN // 128):
            rank[RUN * ch + 128 * k:RUN * ch + 128 * k + 128, :] = jnp.broadcast_to(place[:, 128 * k:128 * k + 128], (128, 128)).T
        base = base + counts[ch]


def reorder(s, pay, rank, pt):
    lane = lax.broadcasted_iota(jnp.int32, (1, 128), 1).astype(F32)
    one, zero = jnp.ones((), BF), jnp.zeros((), BF)
    for t in range(SAMPLES // 128):
        rows = slice(128 * t, 128 * t + 128)
        place = (rank[rows, :] - (s * RUN).astype(F32)).astype(BF)
        for k in range(RUN // 128):
            pt[rows, 128 * k:128 * k + 128] = jnp.where(place == (lane + 128 * k).astype(BF), one, zero)
    return jnp.dot(pay[...], pt[...], preferred_element_type=F32).astype(BF)


def exchange_kernel(y_ref, wy_ref, wx_ref, iy_ref, ix_ref, n_ref, y_out, wy_out, wx_out, key_out, key_own, d_out,
                    y_in, wy_in, wx_in, iy_in, ix_in, wx_bf, pay, oh, rank, pt, loc, ssem, rsem):
    row_id = lax.axis_index('rows')
    other = {'rows': (row_id + 2) % 4}
    barrier = pltpu.get_barrier_semaphore()
    pl.semaphore_signal(barrier, inc=1, device_id=other, device_id_type=pl.DeviceIdType.MESH)
    pairs = [(iy_ref, iy_in), (ix_ref, ix_in), (wx_ref, wx_in), (wy_ref, wy_in), (y_ref, y_in)]
    locs = [pltpu.make_async_copy(a, b, loc.at[i]) for i, (a, b) in enumerate(pairs)]
    for cp in locs:
        cp.start()
    moves = [(y_ref, y_out), (wy_ref, wy_out), (key_own, key_out), (wx_bf, wx_out)]
    sends = [pltpu.make_async_remote_copy(src_ref=a, dst_ref=b, send_sem=ssem.at[i], recv_sem=rsem.at[i], device_id=other, device_id_type=pl.DeviceIdType.MESH) for i, (a, b) in enumerate(moves)]
    pl.semaphore_wait(barrier, 1)
    sends[0].start()
    sends[1].start()
    for cp in locs[:3]:
        cp.wait()
    slot = lax.broadcasted_iota(jnp.int32, iy_in.shape, 1)
    key_own[...] = jnp.where(slot < n_ref[0], (iy_in[...] - row_id * 256) * GRID + ix_in[...], -1000 * GRID)
    wx_bf[...] = wx_in[...].astype(BF)
    sends[2].start()
    sends[3].start()
    for cp in locs[3:]:
        cp.wait()
    payload(y_in, wy_in, wx_bf, key_own, pay)
    ranks(key_own, oh, rank)

    @pl.loop(0, SAMPLES // RUN)
    def _(s):
        d_out[s] = reorder(s, pay, rank, pt)

    for cp in sends:
        cp.wait()


def sort_scratch():
    return [pltpu.VMEM((160, SAMPLES), BF), pltpu.VMEM((80 * (SAMPLES // RUN), RUN), BF), pltpu.VMEM((SAMPLES, 128), F32), pltpu.VMEM((SAMPLES, RUN), BF)]


def exchange(y, wy, wx, iy, ix, n):
    vm = pl.BlockSpec(memory_space=pltpu.VMEM)
    anym = pl.BlockSpec(memory_space=pl.ANY)
    dma = pltpu.SemaphoreType.DMA
    shape = jax.ShapeDtypeStruct
    return pl.pallas_call(
        exchange_kernel,
        out_shape=(shape(y.shape, F32), shape(wy.shape, F32), shape(wx.shape, BF), shape(iy.shape, jnp.int32), shape(iy.shape, jnp.int32), shape((SAMPLES // RUN, 160, RUN), BF)),
        in_specs=[anym] * 5 + [pl.BlockSpec(memory_space=pltpu.SMEM)],
        out_specs=(vm,) * 6,
        scratch_shapes=[pltpu.VMEM(v.shape, v.dtype) for v in (y, wy, wx, iy, ix)] + [pltpu.VMEM(wx.shape, BF)] + sort_scratch() + [dma((5,)), dma((4,)), dma((4,))],
        compiler_params=pltpu.CompilerParams(vmem_limit_bytes=12 * 2**20, collective_id=1, has_side_effects=True),
        cost_estimate=pl.CostEstimate(flops=10**9, bytes_accessed=10**6, transcendentals=0),
        name='exchange',
    )(y, wy, wx, iy, ix, n)


def spread_kernel(y_ref, wy_ref, wx_ref, key_ref, key_own, d_own, g_ref, e_ref, d_nb, pay, oh, rank, pt, acc, a_buf, b_buf):
    zero = jnp.zeros((16, RUN), BF)

    def run(d_ref, s):
        first = jnp.sum(jnp.where(lax.broadcasted_iota(jnp.int32, (1, RUN), 1) == 0, d_ref[s, 128:129, :].astype(F32), 0.0)).astype(jnp.int32) - 1
        last = jnp.max(d_ref[s, 128:129, :].astype(F32)).astype(jnp.int32) + 1
        uc = d_ref[s, 144:160, :]
        eb = [d_ref[s, 96 + 16 * j:112 + 16 * j, :] for j in range(2)]
        for g in range(64):
            b_buf[16 * g:16 * g + 16, :] = jnp.where(uc == jnp.array(g, BF), eb[0], jnp.where(uc == jnp.array((g - 1) % 64, BF), eb[1], zero))

        @pl.loop(0, (last - first + WIN) // WIN)
        def _(w):
            g0 = first + WIN * w
            rel = (d_ref[s, 128:144, :].astype(F32) - (g0 + 1).astype(F32)).astype(BF)
            for gi in range(WIN):
                m = [rel == jnp.array(gi - j, BF) for j in range(3)]
                for q in range(2):
                    e = [d_ref[s, 48 * q + 16 * j:48 * q + 16 * j + 16, :] for j in range(3)]
                    a_buf[16 * (WIN * q + gi):16 * (WIN * q + gi) + 16, :] = jnp.where(m[0], e[0], jnp.where(m[1], e[1], jnp.where(m[2], e[2], zero)))
            prod = lax.dot_general(a_buf[...], b_buf[...], NT, preferred_element_type=F32)
            rows = pl.ds(pl.multiple_of(g0 * 16, 16), 16 * WIN)
            for q in range(2):
                acc[q, rows, :] += prod[16 * WIN * q:16 * WIN * (q + 1)]

    def block(o, d_ref, n_runs):
        acc[:, :1056] = jnp.zeros((2, 1056, GRID), F32)

        @pl.loop(0, n_runs)
        def _(s):
            run(d_ref, s)

        for q in range(2):
            e_ref[o, q, 0:32] = acc[q, 0:32, :]
            e_ref[o, q, 32:64] = acc[q, 1024:1056, :]
            g_ref[o, :, GRID * q:GRID * (q + 1)] = acc[q, 16:1040, :].astype(BF)

    n_own, n_nb = [(jnp.sum(jnp.where(k[...] >= 0, 1.0, 0.0)).astype(jnp.int32) + (RUN - 1)) // RUN for k in (key_own, key_ref)]
    payload(y_ref, wy_ref, wx_ref, key_ref, pay)
    ranks(key_ref, oh, rank)

    @pl.loop(0, n_nb)
    def _(s):
        d_nb[s] = reorder(s, pay, rank, pt)

    block(0, d_own, n_own)
    block(1, d_nb, n_nb)


def spread(y, wy, wx, key, key_own, d_own):
    vm = pl.BlockSpec(memory_space=pltpu.VMEM)
    return pl.pallas_call(
        spread_kernel,
        out_shape=(jax.ShapeDtypeStruct((2, 1024, 2 * GRID), BF), jax.ShapeDtypeStruct((2, 2, 64, GRID), F32)),
        in_specs=[vm] * 6,
        out_specs=(vm, vm),
        scratch_shapes=[pltpu.VMEM((SAMPLES // RUN, 160, RUN), BF)] + sort_scratch() + [
            pltpu.VMEM((2, 16 * (66 + WIN), GRID), F32),
            pltpu.VMEM((32 * WIN, RUN), BF),
            pltpu.VMEM((GRID, RUN), BF),
        ],
        compiler_params=pltpu.CompilerParams(vmem_limit_bytes=28 * 2**20),
        cost_estimate=pl.CostEstimate(flops=13 * 10**9, bytes_accessed=4 * 2**20, transcendentals=0),
        name='spread',
    )(y, wy, wx, key, key_own, d_own)


def combine_kernel(gg, ee, tab, maps, dd, out_ref, hbuf, hs, ge, rx, s_all, part, rx2, scale,
                   esend, erecv, ssem, hsend, hrecv, ysend, yrecv):
    row_id = lax.axis_index('rows')
    y_id = lax.axis_index('coil')
    core = row_id % 2
    x_id = row_id // 2
    sib_row = row_id + 1 - 2 * core
    sib = {'rows': sib_row}
    mate = {'coil': 1 - y_id, 'rows': sib_row}
    blocks = [row_id, (row_id + 2) % 4]

    barrier = pltpu.get_barrier_semaphore()
    pl.semaphore_signal(barrier, inc=1, device_id=sib, device_id_type=pl.DeviceIdType.MESH)
    pl.semaphore_signal(barrier, inc=1, device_id=mate, device_id_type=pl.DeviceIdType.MESH)
    half = lambda y: pl.ds(pl.multiple_of(y * 256, 256), 256)
    s_copy = pltpu.make_async_copy(maps.at[:, :, half(y_id)], s_all.at[core], ssem.at[0])
    s_copy.start()
    row_scale = jnp.broadcast_to(dd[:, half(y_id)], (128, 256)).T
    scale[...] = row_scale * dd[:, pl.ds(pl.multiple_of(row_id * 128, 128), 128)]
    pl.semaphore_wait(barrier, 2)

    def remote(src, dst, send, recv, dev):
        return pltpu.make_async_remote_copy(src_ref=src, dst_ref=dst, send_sem=send, recv_sem=recv, device_id=dev, device_id_type=pl.DeviceIdType.MESH)

    e_copies = []
    for o in range(2):
        low = o * core + (1 - o) * (1 - core)
        high = o * (1 - core) + (1 - o) * core
        for k, (slot, end, row0) in enumerate(((low, 1, 0), (high, 0, 48))):
            e_copies.append(remote(ee.at[o, :, pl.ds(row0, 16)], rx.at[slot, end], esend.at[2 * o + k], erecv.at[slot, end], sib))
    for cp in e_copies:
        cp.start()
    s_send = remote(maps.at[:, :, half(1 - y_id)], s_all.at[core], ssem.at[1], ssem.at[2], sib)
    s_send.start()
    s_recv = remote(maps.at[:, :, half(1 - y_id)], s_all.at[1 - core], ssem.at[1], ssem.at[2], sib)

    def columns(hc, lhs):
        cols = pl.ds(pl.multiple_of(x_id * 256 + hc * 128, 128), 128)
        t2 = jnp.concatenate([tab[0, cols, :], tab[1, cols, :]], axis=0)
        pr = lax.dot_general(lhs(0), t2, NT, preferred_element_type=F32)
        pi = lax.dot_general(lhs(1), t2, NT, preferred_element_type=F32)
        return pr[:, :128] - pi[:, 128:], pr[:, 128:] + pi[:, :128]

    def transform(hc, o, k):
        rows = slice(512 * k, 512 * k + 512)
        pair = columns(hc, lambda q: gg[o, rows, GRID * q:GRID * (q + 1)])
        for e in range(2):
            hs[o, e, rows] = pair[e]

    def take_halos():
        for cp in e_copies:
            cp.wait_send()
        for o in range(2):
            for end in range(2):
                remote(rx.at[o, end], rx.at[o, end], esend.at[2 * o + end], erecv.at[o, end], sib).wait_recv()
                for q in range(2):
                    ge[32 * o + 16 * end:32 * o + 16 * end + 16, GRID * q:GRID * (q + 1)] = (ee[o, q, 16 + 16 * end:32 + 16 * end, :] + rx[o, end, q]).astype(BF)

    def patch(hc):
        pair = columns(hc, lambda q: ge[:, GRID * q:GRID * (q + 1)])
        return pair

    def piece(hc, o, k):
        return remote(hbuf.at[hc, blocks[o], :, pl.ds(128 * k, 128)], hbuf.at[hc, blocks[o], :, pl.ds(128 * k, 128)], hsend.at[hc, o, k], hrecv.at[hc, o, k], sib)

    h_copies = [[piece(hc, o, k) for o in range(2) for k in range(2)] for hc in range(2)]

    def send(hc, o, k, pair):
        for e in range(2):
            hs[o, e, 1008 * k:1008 * k + 16] = pair[e][32 * o + 16 * k:32 * o + 16 * k + 16]
            for c in range(4):
                hbuf[hc, blocks[o], e, 128 * k:128 * k + 128, 128 * c:128 * c + 128] = hs[o, e, pl.ds(512 * k + c, 128, stride=4), :].astype(BF)
        h_copies[hc][2 * o + k].start()

    def image(hc):
        first = 256 * (y_id + (1 - 2 * y_id) * (core + hc - 2 * core * hc))
        for k in range(2):
            rows = pl.ds(pl.multiple_of(first + 128 * k, 128), 128)
            lhs = jnp.concatenate([tab[0, rows, :], tab[1, rows, :]], axis=0)
            mr = jnp.dot(lhs, hbuf[hc, :, 0].reshape(1024, 512), preferred_element_type=F32)
            mi = jnp.dot(lhs, hbuf[hc, :, 1].reshape(1024, 512), preferred_element_type=F32)
            re = mr[:128] - mi[128:]
            im = mr[128:] + mi[:128]
            xr = jnp.zeros((128, 128), F32)
            xi = jnp.zeros((128, 128), F32)
            sl = slice(128 * k, 128 * k + 128)
            for c in range(4):
                ir = re[:, 128 * c:128 * c + 128]
                ii = im[:, 128 * c:128 * c + 128]
                sr = s_all[hc, 0, c, sl, :]
                si = s_all[hc, 1, c, sl, :]
                xr = xr + (sr * ir + si * ii)
                xi = xi + (sr * ii - si * ir)
            part[hc, 0, sl] = xr
            part[hc, 1, sl] = xi

            @pl.when(core != hc)
            def _():
                y_copies[k].start()

    y_copies = [remote(part.at[1 - core, :, pl.ds(128 * k, 128)], rx2.at[:, pl.ds(128 * k, 128)], ysend.at[k], yrecv.at[k], mate) for k in range(2)]

    transform(0, 0, 0)
    transform(0, 0, 1)
    take_halos()
    pair = patch(0)
    send(0, 0, 0, pair)
    send(0, 0, 1, pair)
    for k in range(2):
        transform(0, 1, k)
        send(0, 1, k, pair)
    pair = patch(1)
    for k in range(2):
        transform(1, 0, k)
        send(1, 0, k, pair)
    s_copy.wait()
    s_send.wait_send()
    s_recv.wait_recv()
    for cp in h_copies[0]:
        cp.wait()
    image(0)
    for k in range(2):
        transform(1, 1, k)
        send(1, 1, k, pair)
    for cp in h_copies[1]:
        cp.wait()
    image(1)
    for k in range(2):
        y_copies[k].wait()
        sl = slice(128 * k, 128 * k + 128)
        for e in range(2):
            out_ref[e, sl] = (part[core, e, sl] + rx2[e, sl]) * scale[sl]


def combine(gg, ee, tab, maps, dd):
    vm = pl.BlockSpec(memory_space=pltpu.VMEM)
    dma = pltpu.SemaphoreType.DMA
    return pl.pallas_call(
        combine_kernel,
        out_shape=jax.ShapeDtypeStruct((2, 256, 128), F32),
        in_specs=[vm] * 5,
        out_specs=vm,
        scratch_shapes=[
            pltpu.VMEM((2, 4, 2, 256, 512), BF),
            pltpu.VMEM((2, 2, 1024, 128), F32),
            pltpu.VMEM((64, 2 * GRID), BF),
            pltpu.VMEM((2, 2, 2, 16, GRID), F32),
            pltpu.VMEM((2, 2, 4, 256, 128), F32),
            pltpu.VMEM((2, 2, 256, 128), F32),
            pltpu.VMEM((2, 256, 128), F32),
            pltpu.VMEM((256, 128), F32),
            dma((4,)), dma((2, 2)), dma((3,)), dma((2, 2, 2)), dma((2, 2, 2)), dma((2,)), dma((2,)),
        ],
        compiler_params=pltpu.CompilerParams(vmem_limit_bytes=24 * 2**20, collective_id=0, has_side_effects=True),
        cost_estimate=pl.CostEstimate(flops=7 * 10**9, bytes_accessed=12 * 2**20, transcendentals=0),
        name='combine',
    )(gg, ee, tab, maps, dd)


def solution(mesh):
    def local_part(kspace, weight_row, weight_col, grid_row, grid_col, valid_count, coil_maps, deapod):
        n_img = deapod.shape[0]
        hbm = [pltpu.with_memory_space_constraint(v, pltpu.HBM) for v in (kspace, weight_row, weight_col, grid_row[None], grid_col[None])]
        stacked = exchange(*hbm, valid_count)
        tab = jnp.asarray(tables(n_img))
        gg, ee = spread(*stacked)
        return combine(gg, ee, tab, coil_maps, deapod[None])

    spec_samples = P(None, 'coil', ('slab', 'rows'))
    spec_weights = P(None, ('slab', 'rows'))
    spec_index = P(('slab', 'rows'))
    return jax.shard_map(local_part, mesh=mesh, in_specs=(spec_samples, spec_weights, spec_weights, spec_index, spec_index, spec_index, P(None, 'coil', 'slab', 'rows'), P()), out_specs=P(None, ('slab', 'coil'), 'rows'), check_vma=False)
```

```python
import math
import functools
import numpy as np
import jax
import jax.numpy as jnp
from jax import lax
from jax.experimental import pallas as pl
from jax.experimental.pallas import tpu as pltpu
from jax.sharding import PartitionSpec as P

F32 = jnp.float32
BF = jnp.bfloat16
NT = (((1,), (1,)), ((), ()))
KC = 512
GRID = 1024
SAMPLES = 2048
RUN = 256
WIN = 16


def tables(n_img):
    n_grid = 2 * n_img
    pix = np.arange(n_img) - n_img // 2
    freq = np.arange(n_grid) - n_img
    ang = np.mod(pix[:, None] * freq[None, :], n_grid) * (2.0 * math.pi / n_grid)
    return np.stack([np.cos(ang), np.sin(ang)]).astype(np.float32).astype(BF)


def payload(y_ref, wy_ref, wx_ref, key_ref, pay):
    @pl.loop(0, SAMPLES // KC)
    def _(s):
        cols = pl.ds(pl.multiple_of(s * KC, KC), KC)
        sub = lax.broadcasted_iota(jnp.int32, (16, KC), 0)
        key = key_ref[:, cols]
        r0 = (key >> 10) + 1
        counted = r0 > 0
        t = jnp.where(counted, (sub >> 2) - (r0 & 3), 100)
        for q in range(2):
            y16 = jnp.zeros((16, KC), F32)
            for c in range(4):
                y16 = jnp.where((sub & 3) == c, y_ref[q, c:c + 1, cols], y16)
            coef = [y16 * wy_ref[a:a + 1, cols] for a in range(6)]
            for j in range(3):
                e = jnp.zeros((16, KC), F32)
                for a in range(6):
                    if -3 <= a - 4 * j <= 3:
                        e = jnp.where(t == a - 4 * j, coef[a], e)
                pay[48 * q + 16 * j:48 * q + 16 * j + 16, cols] = e.astype(BF)
        c0 = ((key & (GRID - 1)) + (GRID - 3)) & (GRID - 1)
        wx = wx_ref[:, cols].astype(F32)
        tc = jnp.where(counted, sub - (c0 & 15), 100)
        for j in range(2):
            e = jnp.zeros((16, KC), F32)
            for b in range(6):
                e = jnp.where(tc == b - 16 * j, wx[b:b + 1], e)
            pay[96 + 16 * j:112 + 16 * j, cols] = e.astype(BF)
        pay[128:144, cols] = jnp.broadcast_to(((r0 >> 2) + 1).astype(F32), (16, KC)).astype(BF)
        pay[144:160, cols] = jnp.broadcast_to((c0 >> 4).astype(F32), (16, KC)).astype(BF)


def iota16():
    return lax.broadcasted_iota(jnp.int32, (16, 1), 0).astype(F32)


def tiles(ch):
    first = 4 * (ch // 2) + ch % 2
    return first, first + 2


def ranks(key_ref, oh, rank):
    n_chunk = SAMPLES // RUN
    one, zero = jnp.ones((), BF), jnp.zeros((), BF)
    for ch in range(n_chunk):
        for k, t in enumerate(tiles(ch)):
            bucket = jnp.broadcast_to((((key_ref[:, 128 * t:128 * t + 128] >> 10) + 1) >> 2).astype(F32), (16, 128)).astype(BF)
            for g in range(5):
                oh[80 * ch + 16 * g:80 * ch + 16 * g + 16, 128 * k:128 * k + 128] = jnp.where(bucket == (iota16() + 16 * g).astype(BF), one, zero)
    lower = lax.broadcasted_iota(jnp.int32, (RUN, RUN + 128), 0)
    upper = lax.broadcasted_iota(jnp.int32, (RUN, RUN + 128), 1)
    tri = jnp.where((lower < upper) | (upper >= RUN), 1.0, 0.0).astype(BF)
    pre = jnp.dot(oh[...], tri, preferred_element_type=F32)
    counts = [pre[80 * ch:80 * ch + 80, RUN:] for ch in range(n_chunk)]
    strict = jnp.where(lax.broadcasted_iota(jnp.int32, (80, 80), 1) < lax.broadcasted_iota(jnp.int32, (80, 80), 0), 1.0, 0.0).astype(BF)
    for h in range(2):
        total = counts[h]
        for ch in range(h + 2, n_chunk, 2):
            total = total + counts[ch]
        high = jnp.floor(total * (1.0 / 256.0))
        low = total - 256.0 * high
        base = 256.0 * jnp.dot(strict, high.astype(BF), preferred_element_type=F32) + jnp.dot(strict, low.astype(BF), preferred_element_type=F32)
        for ch in range(h, n_chunk, 2):
            for k, t in enumerate(tiles(ch)):
                place = pre[80 * ch:80 * ch + 80, 128 * k:128 * k + 128] + base
                place = jnp.sum(oh[80 * ch:80 * ch + 80, 128 * k:128 * k + 128].astype(F32) * place, axis=0, keepdims=True)
                place = jnp.where(key_ref[:, 128 * t:128 * t + 128] >= 0, place, -1.0)
                rank[128 * t:128 * t + 128, :] = jnp.broadcast_to(place, (128, 128)).T
            base = base + counts[ch]


def reorder(sp, pay, rank, d_ref):
    lane = lax.broadcasted_iota(jnp.int32, (1, 128), 1).astype(F32)
    one, zero = jnp.ones((), BF), jnp.zeros((), BF)
    for h in range(2):
        total = None
        for ch in range(h, SAMPLES // RUN, 2):
            rows = []
            for t in tiles(ch):
                place = (rank[128 * t:128 * t + 128, :] - (sp * 256).astype(F32)).astype(BF)
                rows.append(jnp.concatenate([jnp.where(place == (lane + 128 * k).astype(BF), one, zero) for k in range(2)], axis=1))
            block = jnp.concatenate(rows, axis=0)
            values = jnp.concatenate([pay[:, 128 * t:128 * t + 128] for t in tiles(ch)], axis=1)
            part = jnp.dot(values, block, preferred_element_type=F32)
            total = part if total is None else total + part
        total = total.astype(BF)
        for k in range(2):
            d_ref[2 * sp + k, :, 128 * h:128 * h + 128] = total[:, 128 * k:128 * k + 128]


def exchange_kernel(y_ref, wy_ref, wx_ref, iy_ref, ix_ref, n_ref, y_out, wy_out, wx_out, key_out, key_own, d_out,
                    y_in, wy_in, wx_in, iy_in, ix_in, wx_bf, pay, oh, rank, loc, ssem, rsem):
    row_id = lax.axis_index('rows')
    other = {'rows': (row_id + 2) % 4}
    barrier = pltpu.get_barrier_semaphore()
    pl.semaphore_signal(barrier, inc=1, device_id=other, device_id_type=pl.DeviceIdType.MESH)
    pairs = [(iy_ref, iy_in), (ix_ref, ix_in), (wx_ref, wx_in), (wy_ref, wy_in), (y_ref, y_in)]
    locs = [pltpu.make_async_copy(a, b, loc.at[i]) for i, (a, b) in enumerate(pairs)]
    for cp in locs:
        cp.start()
    moves = [(y_ref, y_out), (wy_ref, wy_out), (key_own, key_out), (wx_bf, wx_out)]
    sends = [pltpu.make_async_remote_copy(src_ref=a, dst_ref=b, send_sem=ssem.at[i], recv_sem=rsem.at[i], device_id=other, device_id_type=pl.DeviceIdType.MESH) for i, (a, b) in enumerate(moves)]
    pl.semaphore_wait(barrier, 1)
    sends[0].start()
    sends[1].start()
    for cp in locs[:3]:
        cp.wait()
    slot = lax.broadcasted_iota(jnp.int32, iy_in.shape, 1)
    key_own[...] = jnp.where(slot < n_ref[0], (iy_in[...] - row_id * 256) * GRID + ix_in[...], -1000 * GRID)
    wx_bf[...] = wx_in[...].astype(BF)
    sends[2].start()
    sends[3].start()
    for cp in locs[3:]:
        cp.wait()
    payload(y_in, wy_in, wx_bf, key_own, pay)
    ranks(key_own, oh, rank)

    @pl.loop(0, SAMPLES // RUN // 2)
    def _(sp):
        reorder(sp, pay, rank, d_out)

    for cp in sends:
        cp.wait()


def sort_scratch():
    return [pltpu.VMEM((160, SAMPLES), BF), pltpu.VMEM((80 * (SAMPLES // RUN), RUN), BF), pltpu.VMEM((SAMPLES, 128), F32)]


def exchange(y, wy, wx, iy, ix, n):
    vm = pl.BlockSpec(memory_space=pltpu.VMEM)
    anym = pl.BlockSpec(memory_space=pl.ANY)
    dma = pltpu.SemaphoreType.DMA
    shape = jax.ShapeDtypeStruct
    return pl.pallas_call(
        exchange_kernel,
        out_shape=(shape(y.shape, F32), shape(wy.shape, F32), shape(wx.shape, BF), shape(iy.shape, jnp.int32), shape(iy.shape, jnp.int32), shape((SAMPLES // RUN, 160, RUN), BF)),
        in_specs=[anym] * 5 + [pl.BlockSpec(memory_space=pltpu.SMEM)],
        out_specs=(vm,) * 6,
        scratch_shapes=[pltpu.VMEM(v.shape, v.dtype) for v in (y, wy, wx, iy, ix)] + [pltpu.VMEM(wx.shape, BF)] + sort_scratch() + [dma((5,)), dma((4,)), dma((4,))],
        compiler_params=pltpu.CompilerParams(vmem_limit_bytes=12 * 2**20, collective_id=1, has_side_effects=True),
        cost_estimate=pl.CostEstimate(flops=10**9, bytes_accessed=10**6, transcendentals=0),
        name='exchange',
    )(y, wy, wx, iy, ix, n)


def spread_kernel(y_ref, wy_ref, wx_ref, key_ref, key_own, d_own, g_ref, e_ref, d_nb, pay, oh, rank, acc, b_buf):
    zero = jnp.zeros((16, RUN), BF)

    def window(d_ref, s, g0, right):
        rel = (d_ref[s, 128:144, :].astype(F32) - (g0 + 1).astype(F32)).astype(BF)
        left = []
        for q in range(2):
            e = [d_ref[s, 48 * q + 16 * j:48 * q + 16 * j + 16, :] for j in range(3)]
            for gi in range(WIN):
                m = [rel == jnp.array(gi - j, BF) for j in range(3)]
                left.append(jnp.where(m[0], e[0], jnp.where(m[1], e[1], jnp.where(m[2], e[2], zero))))
        prod = lax.dot_general(jnp.concatenate(left, axis=0), right, NT, preferred_element_type=F32)
        rows = pl.ds(pl.multiple_of(g0 * 16, 16), 16 * WIN)
        for q in range(2):
            acc[q, rows, :] += prod[16 * WIN * q:16 * WIN * (q + 1)]

    def run(d_ref, s):
        number = d_ref[s, 128:129, :].astype(F32)
        first = jnp.min(jnp.where(number > 0.0, number, 999.0)).astype(jnp.int32) - 1
        last = jnp.max(number).astype(jnp.int32) + 1
        uc = d_ref[s, 144:160, :]
        eb = [d_ref[s, 96 + 16 * j:112 + 16 * j, :] for j in range(2)]
        right = jnp.concatenate([jnp.where(uc == jnp.array(g, BF), eb[0], jnp.where(uc == jnp.array((g - 1) % 64, BF), eb[1], zero)) for g in range(64)], axis=0)
        b_buf[...] = right
        window(d_ref, s, first, right)

        @pl.loop(1, (last - first + WIN) // WIN)
        def _(w):
            window(d_ref, s, first + WIN * w, b_buf[...])

    def block(o, d_ref, n_runs):
        acc[:, :1056] = jnp.zeros((2, 1056, GRID), F32)

        @pl.loop(0, n_runs)
        def _(s):
            run(d_ref, s)

        for q in range(2):
            e_ref[o, q, 0:32] = acc[q, 0:32, :]
            e_ref[o, q, 32:64] = acc[q, 1024:1056, :]
            g_ref[o, :, GRID * q:GRID * (q + 1)] = acc[q, 16:1040, :].astype(BF)

    n_own, n_nb = [(jnp.sum(jnp.where(k[...] >= 0, 1.0, 0.0)).astype(jnp.int32) + (RUN - 1)) // RUN for k in (key_own, key_ref)]
    payload(y_ref, wy_ref, wx_ref, key_ref, pay)
    ranks(key_ref, oh, rank)

    @pl.loop(0, (n_nb + 1) // 2)
    def _(sp):
        reorder(sp, pay, rank, d_nb)

    block(0, d_own, n_own)
    block(1, d_nb, n_nb)


def spread(y, wy, wx, key, key_own, d_own):
    vm = pl.BlockSpec(memory_space=pltpu.VMEM)
    return pl.pallas_call(
        spread_kernel,
        out_shape=(jax.ShapeDtypeStruct((2, 1024, 2 * GRID), BF), jax.ShapeDtypeStruct((2, 2, 64, GRID), F32)),
        in_specs=[vm] * 6,
        out_specs=(vm, vm),
        scratch_shapes=[pltpu.VMEM((SAMPLES // RUN, 160, RUN), BF)] + sort_scratch() + [
            pltpu.VMEM((2, 16 * (66 + WIN), GRID), F32),
            pltpu.VMEM((GRID, RUN), BF),
        ],
        compiler_params=pltpu.CompilerParams(vmem_limit_bytes=28 * 2**20),
        cost_estimate=pl.CostEstimate(flops=13 * 10**9, bytes_accessed=4 * 2**20, transcendentals=0),
        name='spread',
    )(y, wy, wx, key, key_own, d_own)


def combine_kernel(gg, ee, tab, maps, dd, out_ref, hbuf, hs, ge, rx, s_all, part, rx2, scale,
                   esend, erecv, ssem, hsend, hrecv, ysend, yrecv):
    row_id = lax.axis_index('rows')
    y_id = lax.axis_index('coil')
    core = row_id % 2
    x_id = row_id // 2
    sib_row = row_id + 1 - 2 * core
    sib = {'rows': sib_row}
    mate = {'coil': 1 - y_id, 'rows': sib_row}
    blocks = [row_id, (row_id + 2) % 4]

    barrier = pltpu.get_barrier_semaphore()
    pl.semaphore_signal(barrier, inc=1, device_id=sib, device_id_type=pl.DeviceIdType.MESH)
    pl.semaphore_signal(barrier, inc=1, device_id=mate, device_id_type=pl.DeviceIdType.MESH)
    half = lambda y: pl.ds(pl.multiple_of(y * 256, 256), 256)
    s_copy = pltpu.make_async_copy(maps.at[:, :, half(y_id)], s_all.at[core], ssem.at[0])
    s_copy.start()
    row_scale = jnp.broadcast_to(dd[:, half(y_id)], (128, 256)).T
    scale[...] = row_scale * dd[:, pl.ds(pl.multiple_of(row_id * 128, 128), 128)]
    pl.semaphore_wait(barrier, 2)

    def remote(src, dst, send, recv, dev):
        return pltpu.make_async_remote_copy(src_ref=src, dst_ref=dst, send_sem=send, recv_sem=recv, device_id=dev, device_id_type=pl.DeviceIdType.MESH)

    e_copies = []
    for o in range(2):
        low = o * core + (1 - o) * (1 - core)
        high = o * (1 - core) + (1 - o) * core
        for k, (slot, end, row0) in enumerate(((low, 1, 0), (high, 0, 48))):
            e_copies.append(remote(ee.at[o, :, pl.ds(row0, 16)], rx.at[slot, end], esend.at[2 * o + k], erecv.at[slot, end], sib))
    for cp in e_copies:
        cp.start()
    s_send = remote(maps.at[:, :, half(1 - y_id)], s_all.at[core], ssem.at[1], ssem.at[2], sib)
    s_send.start()
    s_recv = remote(maps.at[:, :, half(1 - y_id)], s_all.at[1 - core], ssem.at[1], ssem.at[2], sib)

    def columns(hc, lhs):
        cols = pl.ds(pl.multiple_of(x_id * 256 + hc * 128, 128), 128)
        t2 = jnp.concatenate([tab[0, cols, :], tab[1, cols, :]], axis=0)
        pr = lax.dot_general(lhs(0), t2, NT, preferred_element_type=F32)
        pi = lax.dot_general(lhs(1), t2, NT, preferred_element_type=F32)
        return pr[:, :128] - pi[:, 128:], pr[:, 128:] + pi[:, :128]

    def transform(hc, o, k):
        rows = slice(512 * k, 512 * k + 512)
        pair = columns(hc, lambda q: gg[o, rows, GRID * q:GRID * (q + 1)])
        for e in range(2):
            hs[o, e, rows] = pair[e]

    def take_halos():
        for cp in e_copies:
            cp.wait_send()
        for o in range(2):
            for end in range(2):
                remote(rx.at[o, end], rx.at[o, end], esend.at[2 * o + end], erecv.at[o, end], sib).wait_recv()
                for q in range(2):
                    ge[32 * o + 16 * end:32 * o + 16 * end + 16, GRID * q:GRID * (q + 1)] = (ee[o, q, 16 + 16 * end:32 + 16 * end, :] + rx[o, end, q]).astype(BF)

    def patch(hc):
        pair = columns(hc, lambda q: ge[:, GRID * q:GRID * (q + 1)])
        return pair

    def piece(hc, o, k):
        return remote(hbuf.at[hc, blocks[o], :, pl.ds(128 * k, 128)], hbuf.at[hc, blocks[o], :, pl.ds(128 * k, 128)], hsend.at[hc, o, k], hrecv.at[hc, o, k], sib)

    h_copies = [[piece(hc, o, k) for o in range(2) for k in range(2)] for hc in range(2)]

    def send(hc, o, k, pair):
        for e in range(2):
            hs[o, e, 1008 * k:1008 * k + 16] = pair[e][32 * o + 16 * k:32 * o + 16 * k + 16]
            for c in range(4):
                hbuf[hc, blocks[o], e, 128 * k:128 * k + 128, 128 * c:128 * c + 128] = hs[o, e, pl.ds(512 * k + c, 128, stride=4), :].astype(BF)
        h_copies[hc][2 * o + k].start()

    def image(hc):
        first = 256 * (y_id + (1 - 2 * y_id) * (core + hc - 2 * core * hc))
        for k in range(2):
            rows = pl.ds(pl.multiple_of(first + 128 * k, 128), 128)
            lhs = jnp.concatenate([tab[0, rows, :], tab[1, rows, :]], axis=0)
            mr = jnp.dot(lhs, hbuf[hc, :, 0].reshape(1024, 512), preferred_element_type=F32)
            mi = jnp.dot(lhs, hbuf[hc, :, 1].reshape(1024, 512), preferred_element_type=F32)
            re = mr[:128] - mi[128:]
            im = mr[128:] + mi[:128]
            xr = jnp.zeros((128, 128), F32)
            xi = jnp.zeros((128, 128), F32)
            sl = slice(128 * k, 128 * k + 128)
            for c in range(4):
                ir = re[:, 128 * c:128 * c + 128]
                ii = im[:, 128 * c:128 * c + 128]
                sr = s_all[hc, 0, c, sl, :]
                si = s_all[hc, 1, c, sl, :]
                xr = xr + (sr * ir + si * ii)
                xi = xi + (sr * ii - si * ir)
            part[hc, 0, sl] = xr
            part[hc, 1, sl] = xi

            @pl.when(core != hc)
            def _():
                y_copies[k].start()

    y_copies = [remote(part.at[1 - core, :, pl.ds(128 * k, 128)], rx2.at[:, pl.ds(128 * k, 128)], ysend.at[k], yrecv.at[k], mate) for k in range(2)]

    transform(0, 0, 0)
    transform(0, 0, 1)
    take_halos()
    pair = patch(0)
    send(0, 0, 0, pair)
    send(0, 0, 1, pair)
    for k in range(2):
        transform(0, 1, k)
        send(0, 1, k, pair)
    pair = patch(1)
    for k in range(2):
        transform(1, 0, k)
        send(1, 0, k, pair)
    s_copy.wait()
    s_send.wait_send()
    s_recv.wait_recv()
    for cp in h_copies[0]:
        cp.wait()
    image(0)
    for k in range(2):
        transform(1, 1, k)
        send(1, 1, k, pair)
    for cp in h_copies[1]:
        cp.wait()
    image(1)
    for k in range(2):
        y_copies[k].wait()
        sl = slice(128 * k, 128 * k + 128)
        for e in range(2):
            out_ref[e, sl] = (part[core, e, sl] + rx2[e, sl]) * scale[sl]


def combine(gg, ee, tab, maps, dd):
    vm = pl.BlockSpec(memory_space=pltpu.VMEM)
    dma = pltpu.SemaphoreType.DMA
    return pl.pallas_call(
        combine_kernel,
        out_shape=jax.ShapeDtypeStruct((2, 256, 128), F32),
        in_specs=[vm] * 5,
        out_specs=vm,
        scratch_shapes=[
            pltpu.VMEM((2, 4, 2, 256, 512), BF),
            pltpu.VMEM((2, 2, 1024, 128), F32),
            pltpu.VMEM((64, 2 * GRID), BF),
            pltpu.VMEM((2, 2, 2, 16, GRID), F32),
            pltpu.VMEM((2, 2, 4, 256, 128), F32),
            pltpu.VMEM((2, 2, 256, 128), F32),
            pltpu.VMEM((2, 256, 128), F32),
            pltpu.VMEM((256, 128), F32),
            dma((4,)), dma((2, 2)), dma((3,)), dma((2, 2, 2)), dma((2, 2, 2)), dma((2,)), dma((2,)),
        ],
        compiler_params=pltpu.CompilerParams(vmem_limit_bytes=24 * 2**20, collective_id=0, has_side_effects=True),
        cost_estimate=pl.CostEstimate(flops=7 * 10**9, bytes_accessed=12 * 2**20, transcendentals=0),
        name='combine',
    )(gg, ee, tab, maps, dd)


def solution(mesh):
    def local_part(kspace, weight_row, weight_col, grid_row, grid_col, valid_count, coil_maps, deapod):
        n_img = deapod.shape[0]
        hbm = [pltpu.with_memory_space_constraint(v, pltpu.HBM) for v in (kspace, weight_row, weight_col, grid_row[None], grid_col[None])]
        stacked = exchange(*hbm, valid_count)
        tab = jnp.asarray(tables(n_img))
        gg, ee = spread(*stacked)
        return combine(gg, ee, tab, coil_maps, deapod[None])

    spec_samples = P(None, 'coil', ('slab', 'rows'))
    spec_weights = P(None, ('slab', 'rows'))
    spec_index = P(('slab', 'rows'))
    return jax.shard_map(local_part, mesh=mesh, in_specs=(spec_samples, spec_weights, spec_weights, spec_index, spec_index, spec_index, P(None, 'coil', 'slab', 'rows'), P()), out_specs=P(None, ('slab', 'coil'), 'rows'), check_vma=False)
```

```python
import math
import functools
import numpy as np
import jax
import jax.numpy as jnp
from jax import lax
from jax.experimental import pallas as pl
from jax.experimental.pallas import tpu as pltpu
from jax.sharding import PartitionSpec as P

F32 = jnp.float32
BF = jnp.bfloat16
NT = (((1,), (1,)), ((), ()))
KC = 512
GRID = 1024
SAMPLES = 2048
RUN = 256
WIN = 16


def tables(n_img):
    n_grid = 2 * n_img
    pix = np.arange(n_img) - n_img // 2
    freq = np.arange(n_grid) - n_img
    ang = np.mod(pix[:, None] * freq[None, :], n_grid) * (2.0 * math.pi / n_grid)
    return np.stack([np.cos(ang), np.sin(ang)]).astype(np.float32).astype(BF)


def payload(y_ref, wy_ref, wx_ref, key_ref, pay):
    @pl.loop(0, SAMPLES // KC)
    def _(s):
        cols = pl.ds(pl.multiple_of(s * KC, KC), KC)
        sub = lax.broadcasted_iota(jnp.int32, (16, KC), 0)
        key = key_ref[:, cols]
        r0 = (key >> 10) + 1
        counted = r0 > 0
        t = jnp.where(counted, (sub >> 2) - (r0 & 3), 100)
        for q in range(2):
            y16 = jnp.zeros((16, KC), F32)
            for c in range(4):
                y16 = jnp.where((sub & 3) == c, y_ref[q, c:c + 1, cols], y16)
            coef = [y16 * wy_ref[a:a + 1, cols] for a in range(6)]
            for j in range(3):
                e = jnp.zeros((16, KC), F32)
                for a in range(6):
                    if -3 <= a - 4 * j <= 3:
                        e = jnp.where(t == a - 4 * j, coef[a], e)
                pay[48 * q + 16 * j:48 * q + 16 * j + 16, cols] = e.astype(BF)
        c0 = ((key & (GRID - 1)) + (GRID - 3)) & (GRID - 1)
        wx = wx_ref[:, cols].astype(F32)
        tc = jnp.where(counted, sub - (c0 & 15), 100)
        for j in range(2):
            e = jnp.zeros((16, KC), F32)
            for b in range(6):
                e = jnp.where(tc == b - 16 * j, wx[b:b + 1], e)
            pay[96 + 16 * j:112 + 16 * j, cols] = e.astype(BF)
        pay[128:144, cols] = jnp.broadcast_to(((r0 >> 2) + 1).astype(F32), (16, KC)).astype(BF)
        pay[144:160, cols] = jnp.broadcast_to((c0 >> 4).astype(F32), (16, KC)).astype(BF)


def iota16():
    return lax.broadcasted_iota(jnp.int32, (16, 1), 0).astype(F32)


def tiles(ch):
    first = 4 * (ch // 2) + ch % 2
    return first, first + 2


def ranks(key_ref, oh, rank):
    n_chunk = SAMPLES // RUN
    one, zero = jnp.ones((), BF), jnp.zeros((), BF)
    for ch in range(n_chunk):
        for k, t in enumerate(tiles(ch)):
            bucket = jnp.broadcast_to((((key_ref[:, 128 * t:128 * t + 128] >> 10) + 1) >> 2).astype(F32), (16, 128)).astype(BF)
            for g in range(5):
                oh[80 * ch + 16 * g:80 * ch + 16 * g + 16, 128 * k:128 * k + 128] = jnp.where(bucket == (iota16() + 16 * g).astype(BF), one, zero)
    lower = lax.broadcasted_iota(jnp.int32, (RUN, RUN + 128), 0)
    upper = lax.broadcasted_iota(jnp.int32, (RUN, RUN + 128), 1)
    tri = jnp.where((lower < upper) | (upper >= RUN), 1.0, 0.0).astype(BF)
    pre = jnp.dot(oh[...], tri, preferred_element_type=F32)
    counts = [pre[80 * ch:80 * ch + 80, RUN:] for ch in range(n_chunk)]
    strict = jnp.where(lax.broadcasted_iota(jnp.int32, (80, 80), 1) < lax.broadcasted_iota(jnp.int32, (80, 80), 0), 1.0, 0.0).astype(BF)
    for h in range(2):
        total = counts[h]
        for ch in range(h + 2, n_chunk, 2):
            total = total + counts[ch]
        high = jnp.floor(total * (1.0 / 256.0))
        low = total - 256.0 * high
        base = 256.0 * jnp.dot(strict, high.astype(BF), preferred_element_type=F32) + jnp.dot(strict, low.astype(BF), preferred_element_type=F32)
        for ch in range(h, n_chunk, 2):
            for k, t in enumerate(tiles(ch)):
                place = pre[80 * ch:80 * ch + 80, 128 * k:128 * k + 128] + base
                place = jnp.sum(oh[80 * ch:80 * ch + 80, 128 * k:128 * k + 128].astype(F32) * place, axis=0, keepdims=True)
                place = jnp.where(key_ref[:, 128 * t:128 * t + 128] >= 0, place, -1.0)
                rank[128 * t:128 * t + 128, :] = jnp.broadcast_to(place, (128, 128)).T
            base = base + counts[ch]


def reorder(sp, pay, rank, d_ref):
    lane = lax.broadcasted_iota(jnp.int32, (1, 128), 1).astype(F32)
    one, zero = jnp.ones((), BF), jnp.zeros((), BF)
    for h in range(2):
        total = None
        for ch in range(h, SAMPLES // RUN, 2):
            rows = []
            for t in tiles(ch):
                place = (rank[128 * t:128 * t + 128, :] - (sp * 256).astype(F32)).astype(BF)
                rows.append(jnp.concatenate([jnp.where(place == (lane + 128 * k).astype(BF), one, zero) for k in range(2)], axis=1))
            block = jnp.concatenate(rows, axis=0)
            values = jnp.concatenate([pay[:, 128 * t:128 * t + 128] for t in tiles(ch)], axis=1)
            part = jnp.dot(values, block, preferred_element_type=F32)
            total = part if total is None else total + part
        total = total.astype(BF)
        for k in range(2):
            d_ref[2 * sp + k, :, 128 * h:128 * h + 128] = total[:, 128 * k:128 * k + 128]


def exchange_kernel(y_ref, wy_ref, wx_ref, iy_ref, ix_ref, n_ref, y_out, wy_out, wx_out, key_out, key_own, d_out,
                    y_in, wy_in, wx_in, iy_in, ix_in, wx_bf, pay, oh, rank, loc, ssem, rsem):
    row_id = lax.axis_index('rows')
    other = {'rows': (row_id + 2) % 4}
    barrier = pltpu.get_barrier_semaphore()
    pl.semaphore_signal(barrier, inc=1, device_id=other, device_id_type=pl.DeviceIdType.MESH)
    pairs = [(iy_ref, iy_in), (ix_ref, ix_in), (wx_ref, wx_in), (wy_ref, wy_in), (y_ref, y_in)]
    locs = [pltpu.make_async_copy(a, b, loc.at[i]) for i, (a, b) in enumerate(pairs)]
    for cp in locs:
        cp.start()
    moves = [(y_ref, y_out), (wy_ref, wy_out), (key_own, key_out), (wx_bf, wx_out)]
    sends = [pltpu.make_async_remote_copy(src_ref=a, dst_ref=b, send_sem=ssem.at[i], recv_sem=rsem.at[i], device_id=other, device_id_type=pl.DeviceIdType.MESH) for i, (a, b) in enumerate(moves)]
    pl.semaphore_wait(barrier, 1)
    sends[0].start()
    sends[1].start()
    for cp in locs[:3]:
        cp.wait()
    slot = lax.broadcasted_iota(jnp.int32, iy_in.shape, 1)
    key_own[...] = jnp.where(slot < n_ref[0], (iy_in[...] - row_id * 256) * GRID + ix_in[...], -1000 * GRID)
    wx_bf[...] = wx_in[...].astype(BF)
    sends[2].start()
    sends[3].start()
    for cp in locs[3:]:
        cp.wait()
    payload(y_in, wy_in, wx_bf, key_own, pay)
    ranks(key_own, oh, rank)

    @pl.loop(0, SAMPLES // RUN // 2)
    def _(sp):
        reorder(sp, pay, rank, d_out)

    for cp in sends:
        cp.wait()


def sort_scratch():
    return [pltpu.VMEM((160, SAMPLES), BF), pltpu.VMEM((80 * (SAMPLES // RUN), RUN), BF), pltpu.VMEM((SAMPLES, 128), F32)]


def exchange(y, wy, wx, iy, ix, n):
    vm = pl.BlockSpec(memory_space=pltpu.VMEM)
    anym = pl.BlockSpec(memory_space=pl.ANY)
    dma = pltpu.SemaphoreType.DMA
    shape = jax.ShapeDtypeStruct
    return pl.pallas_call(
        exchange_kernel,
        out_shape=(shape(y.shape, F32), shape(wy.shape, F32), shape(wx.shape, BF), shape(iy.shape, jnp.int32), shape(iy.shape, jnp.int32), shape((SAMPLES // RUN, 160, RUN), BF)),
        in_specs=[anym] * 5 + [pl.BlockSpec(memory_space=pltpu.SMEM)],
        out_specs=(vm,) * 6,
        scratch_shapes=[pltpu.VMEM(v.shape, v.dtype) for v in (y, wy, wx, iy, ix)] + [pltpu.VMEM(wx.shape, BF)] + sort_scratch() + [dma((5,)), dma((4,)), dma((4,))],
        compiler_params=pltpu.CompilerParams(vmem_limit_bytes=12 * 2**20, collective_id=1, has_side_effects=True),
        cost_estimate=pl.CostEstimate(flops=10**9, bytes_accessed=10**6, transcendentals=0),
        name='exchange',
    )(y, wy, wx, iy, ix, n)


def spread_kernel(y_ref, wy_ref, wx_ref, key_ref, key_own, d_own, g_ref, e_ref, d_nb, pay, oh, rank, acc, b_buf):
    zero = jnp.zeros((16, RUN), BF)

    def window(d_ref, s, g0, right):
        rel = (d_ref[s, 128:144, :].astype(F32) - (g0 + 1).astype(F32)).astype(BF)
        left = []
        for q in range(2):
            e = [d_ref[s, 48 * q + 16 * j:48 * q + 16 * j + 16, :] for j in range(3)]
            for gi in range(WIN):
                m = [rel == jnp.array(gi - j, BF) for j in range(3)]
                left.append(jnp.where(m[0], e[0], jnp.where(m[1], e[1], jnp.where(m[2], e[2], zero))))
        prod = lax.dot_general(jnp.concatenate(left, axis=0), right, NT, preferred_element_type=F32)
        rows = pl.ds(pl.multiple_of(g0 * 16, 16), 16 * WIN)
        for q in range(2):
            acc[q, rows, :] += prod[16 * WIN * q:16 * WIN * (q + 1)]

    def run(d_ref, s):
        number = d_ref[s, 128:129, :].astype(F32)
        first = jnp.min(jnp.where(number > 0.0, number, 999.0)).astype(jnp.int32) - 1
        last = jnp.max(number).astype(jnp.int32) + 1
        uc = d_ref[s, 144:160, :]
        eb = [d_ref[s, 96 + 16 * j:112 + 16 * j, :] for j in range(2)]
        right = jnp.concatenate([jnp.where(uc == jnp.array(g, BF), eb[0], jnp.where(uc == jnp.array((g - 1) % 64, BF), eb[1], zero)) for g in range(64)], axis=0)
        b_buf[...] = right
        window(d_ref, s, first, right)

        @pl.loop(1, (last - first + WIN) // WIN)
        def _(w):
            window(d_ref, s, first + WIN * w, b_buf[...])

    def block(o, d_ref, n_runs):
        acc[:, :1056] = jnp.zeros((2, 1056, GRID), F32)

        @pl.loop(0, n_runs)
        def _(s):
            run(d_ref, s)

        for q in range(2):
            e_ref[o, q, 0:32] = acc[q, 0:32, :]
            e_ref[o, q, 32:64] = acc[q, 1024:1056, :]
            g_ref[o, :, GRID * q:GRID * (q + 1)] = acc[q, 16:1040, :].astype(BF)

    n_own, n_nb = [(jnp.sum(jnp.where(k[...] >= 0, 1.0, 0.0)).astype(jnp.int32) + (RUN - 1)) // RUN for k in (key_own, key_ref)]
    payload(y_ref, wy_ref, wx_ref, key_ref, pay)
    ranks(key_ref, oh, rank)

    @pl.loop(0, (n_nb + 1) // 2)
    def _(sp):
        reorder(sp, pay, rank, d_nb)

    block(0, d_own, n_own)
    block(1, d_nb, n_nb)


def spread(y, wy, wx, key, key_own, d_own):
    vm = pl.BlockSpec(memory_space=pltpu.VMEM)
    return pl.pallas_call(
        spread_kernel,
        out_shape=(jax.ShapeDtypeStruct((2, 1024, 2 * GRID), BF), jax.ShapeDtypeStruct((2, 2, 64, GRID), F32)),
        in_specs=[vm] * 6,
        out_specs=(vm, vm),
        scratch_shapes=[pltpu.VMEM((SAMPLES // RUN, 160, RUN), BF)] + sort_scratch() + [
            pltpu.VMEM((2, 16 * (66 + WIN), GRID), F32),
            pltpu.VMEM((GRID, RUN), BF),
        ],
        compiler_params=pltpu.CompilerParams(vmem_limit_bytes=28 * 2**20),
        cost_estimate=pl.CostEstimate(flops=13 * 10**9, bytes_accessed=4 * 2**20, transcendentals=0),
        name='spread',
    )(y, wy, wx, key, key_own, d_own)


def combine_kernel(gg, ee, tab, maps, dd, out_ref, hbuf, hs, ge, rx, s_all, part, near, far, scale,
                   esend, erecv, ssend, srecv, hsend, hrecv, ysend, yrecv, nsend, nrecv):
    row_id = lax.axis_index('rows')
    y_id = lax.axis_index('coil')
    core = row_id % 2
    x_id = row_id // 2
    sib_row = row_id + 1 - 2 * core
    sib = {'rows': sib_row}
    blocks = [row_id, (row_id + 2) % 4]

    barrier = pltpu.get_barrier_semaphore()
    for dev in (sib, {'coil': 1 - y_id}, {'coil': 1 - y_id, 'rows': sib_row}):
        pl.semaphore_signal(barrier, inc=1, device_id=dev, device_id_type=pl.DeviceIdType.MESH)

    def rows_of(a, c):
        return pl.ds(pl.multiple_of(256 * a + 128 * c, 128), 128)

    for a in range(2):
        s_all[core, a] = maps[:, :, rows_of(a, core), :]
    row_scale = jnp.broadcast_to(dd[:, pl.ds(pl.multiple_of(y_id * 256, 256), 256)], (128, 256)).T
    scale[...] = row_scale * dd[:, pl.ds(pl.multiple_of(row_id * 128, 128), 128)]
    pl.semaphore_wait(barrier, 3)

    def remote(src, dst, send, recv, dev):
        return pltpu.make_async_remote_copy(src_ref=src, dst_ref=dst, send_sem=send, recv_sem=recv, device_id=dev, device_id_type=pl.DeviceIdType.MESH)

    e_copies = []
    for o in range(2):
        low = o * core + (1 - o) * (1 - core)
        high = o * (1 - core) + (1 - o) * core
        for k, (slot, end, row0) in enumerate(((low, 1, 0), (high, 0, 48))):
            e_copies.append(remote(ee.at[o, :, pl.ds(row0, 16)], rx.at[slot, end], esend.at[2 * o + k], erecv.at[slot, end], sib))
    for cp in e_copies:
        cp.start()
    s_copies = [remote(maps.at[:, :, rows_of(a, 1 - core)], s_all.at[core, a], ssend.at[a], srecv.at[a], sib) for a in range(2)]
    for cp in s_copies:
        cp.start()

    def columns(hc, lhs):
        cols = pl.ds(pl.multiple_of(x_id * 256 + hc * 128, 128), 128)
        t2 = jnp.concatenate([tab[0, cols, :], tab[1, cols, :]], axis=0)
        prod = lax.dot_general(lhs, t2, NT, preferred_element_type=F32)
        n = lhs.shape[0] // 2
        return prod[:n, :128] - prod[n:, 128:], prod[:n, 128:] + prod[n:, :128]

    def transform(hc, o, k):
        for j in range(2):
            rows = slice(512 * k + 256 * j, 512 * k + 256 * j + 256)
            pair = columns(hc, jnp.concatenate([gg[o, rows, :GRID], gg[o, rows, GRID:]], axis=0))
            for e in range(2):
                hs[o, e, rows] = pair[e]

    def take_halos():
        for cp in e_copies:
            cp.wait_send()
        for o in range(2):
            for end in range(2):
                remote(rx.at[o, end], rx.at[o, end], esend.at[2 * o + end], erecv.at[o, end], sib).wait_recv()
                for q in range(2):
                    ge[64 * q + 32 * o + 16 * end:64 * q + 32 * o + 16 * end + 16, :] = (ee[o, q, 16 + 16 * end:32 + 16 * end, :] + rx[o, end, q]).astype(BF)

    def patch(hc):
        return columns(hc, ge[...])

    def piece(hc, o, k):
        return remote(hbuf.at[hc, blocks[o], :, pl.ds(128 * k, 128)], hbuf.at[hc, blocks[o], :, pl.ds(128 * k, 128)], hsend.at[hc, o, k], hrecv.at[hc, o, k], sib)

    h_copies = [[piece(hc, o, k) for o in range(2) for k in range(2)] for hc in range(2)]

    def send(hc, o, k, pair):
        for e in range(2):
            hs[o, e, 1008 * k:1008 * k + 16] = pair[e][32 * o + 16 * k:32 * o + 16 * k + 16]
            for c in range(4):
                hbuf[hc, blocks[o], e, 128 * k:128 * k + 128, 128 * c:128 * c + 128] = hs[o, e, pl.ds(512 * k + c, 128, stride=4), :].astype(BF)
        h_copies[hc][2 * o + k].start()

    def image(hc, a):
        rows = rows_of(a, core)
        cos, sin = tab[0, rows, :], tab[1, rows, :]
        quarter = [slice(256 * p, 256 * p + 256) for p in range(4)]
        top = jnp.concatenate([v[:, q] for q in quarter for v in (cos, -sin)], axis=1)
        bottom = jnp.concatenate([v[:, q] for q in quarter for v in (sin, cos)], axis=1)
        both = jnp.dot(jnp.concatenate([top, bottom], axis=0), hbuf[hc].reshape(2048, 512), preferred_element_type=F32)
        re, im = both[:128], both[128:]
        xr = jnp.zeros((128, 128), F32)
        xi = jnp.zeros((128, 128), F32)
        for c in range(4):
            ir = re[:, 128 * c:128 * c + 128]
            ii = im[:, 128 * c:128 * c + 128]
            sr = s_all[hc, a, 0, c]
            si = s_all[hc, a, 1, c]
            xr = xr + (sr * ir + si * ii)
            xi = xi + (sr * ii - si * ir)
        part[hc, a, 0] = xr
        part[hc, a, 1] = xi

    y_copies = [remote(part.at[hc, 1 - y_id], far.at[core], ysend.at[hc], yrecv.at[core], {'coil': 1 - y_id, 'rows': 2 * x_id + hc}) for hc in range(2)]
    n_copy = remote(part.at[1 - core, y_id], near, nsend.at[0], nrecv.at[0], sib)

    for k in range(2):
        transform(0, 0, k)
    take_halos()
    pair = patch(0)
    for k in range(2):
        send(0, 0, k, pair)
    for k in range(2):
        transform(0, 1, k)
        send(0, 1, k, pair)
    pair = patch(1)
    transform(1, 0, 0)
    send(1, 0, 0, pair)
    for cp in s_copies + h_copies[0]:
        cp.wait()
    image(0, 1 - y_id)
    y_copies[0].start()
    transform(1, 0, 1)
    send(1, 0, 1, pair)
    for k in range(2):
        transform(1, 1, k)
        send(1, 1, k, pair)
    image(0, y_id)
    for cp in h_copies[1]:
        cp.wait()
    image(1, 1 - y_id)
    y_copies[1].start()
    image(1, y_id)
    n_copy.start()
    for cp in y_copies:
        cp.wait_send()
    n_copy.wait()
    mine = pl.ds(pl.multiple_of(128 * core, 128), 128)
    other = pl.ds(pl.multiple_of(128 * (1 - core), 128), 128)
    for e in range(2):
        out_ref[e, mine] = part[core, y_id, e]
        out_ref[e, other] = near[e]
    for k in range(2):
        remote(far.at[k], far.at[k], ysend.at[k], yrecv.at[k], {'coil': 1 - y_id}).wait_recv()
        sl = slice(128 * k, 128 * k + 128)
        for e in range(2):
            out_ref[e, sl] = (out_ref[e, sl] + far[k, e]) * scale[sl]


def combine(gg, ee, tab, maps, dd):
    vm = pl.BlockSpec(memory_space=pltpu.VMEM)
    dma = pltpu.SemaphoreType.DMA
    return pl.pallas_call(
        combine_kernel,
        out_shape=jax.ShapeDtypeStruct((2, 256, 128), F32),
        in_specs=[vm] * 5,
        out_specs=vm,
        scratch_shapes=[
            pltpu.VMEM((2, 4, 2, 256, 512), BF),
            pltpu.VMEM((2, 2, 1024, 128), F32),
            pltpu.VMEM((128, GRID), BF),
            pltpu.VMEM((2, 2, 2, 16, GRID), F32),
            pltpu.VMEM((2, 2, 2, 4, 128, 128), F32),
            pltpu.VMEM((2, 2, 2, 128, 128), F32),
            pltpu.VMEM((2, 128, 128), F32),
            pltpu.VMEM((2, 2, 128, 128), F32),
            pltpu.VMEM((256, 128), F32),
            dma((4,)), dma((2, 2)), dma((2,)), dma((2,)), dma((2, 2, 2)), dma((2, 2, 2)), dma((2,)), dma((2,)), dma((1,)), dma((1,)),
        ],
        compiler_params=pltpu.CompilerParams(vmem_limit_bytes=24 * 2**20, collective_id=0, has_side_effects=True),
        cost_estimate=pl.CostEstimate(flops=7 * 10**9, bytes_accessed=12 * 2**20, transcendentals=0),
        name='combine',
    )(gg, ee, tab, maps, dd)


def solution(mesh):
    def local_part(kspace, weight_row, weight_col, grid_row, grid_col, valid_count, coil_maps, deapod):
        n_img = deapod.shape[0]
        hbm = [pltpu.with_memory_space_constraint(v, pltpu.HBM) for v in (kspace, weight_row, weight_col, grid_row[None], grid_col[None])]
        stacked = exchange(*hbm, valid_count)
        tab = jnp.asarray(tables(n_img))
        gg, ee = spread(*stacked)
        return combine(gg, ee, tab, coil_maps, deapod[None])

    spec_samples = P(None, 'coil', ('slab', 'rows'))
    spec_weights = P(None, ('slab', 'rows'))
    spec_index = P(('slab', 'rows'))
    return jax.shard_map(local_part, mesh=mesh, in_specs=(spec_samples, spec_weights, spec_weights, spec_index, spec_index, spec_index, P(None, 'coil', 'slab', 'rows'), P()), out_specs=P(None, ('slab', 'coil'), 'rows'), check_vma=False)
```

```python
import math
import functools
import numpy as np
import jax
import jax.numpy as jnp
from jax import lax
from jax.experimental import pallas as pl
from jax.experimental.pallas import tpu as pltpu
from jax.sharding import PartitionSpec as P

F32 = jnp.float32
BF = jnp.bfloat16
NT = (((1,), (1,)), ((), ()))
KC = 512
GRID = 1024
SAMPLES = 2048
RUN = 256
WIN = 16


def tables(n_img):
    n_grid = 2 * n_img
    pix = np.arange(n_img) - n_img // 2
    freq = np.arange(n_grid) - n_img
    ang = np.mod(pix[:, None] * freq[None, :], n_grid) * (2.0 * math.pi / n_grid)
    return np.stack([np.cos(ang), np.sin(ang)]).astype(np.float32).astype(BF)


def payload(y_ref, wy_ref, wx_ref, key_ref, pay, clear=None):
    @pl.loop(0, SAMPLES // KC)
    def _(s):
        cols = pl.ds(pl.multiple_of(s * KC, KC), KC)
        sub = lax.broadcasted_iota(jnp.int32, (16, KC), 0)
        if clear is not None:
            clear[:, pl.ds(pl.multiple_of(s * 176, 16), 176), :] = jnp.zeros((2, 176, GRID), F32)
        key = key_ref[:, cols]
        r0 = (key >> 10) + 1
        counted = r0 > 0
        t = jnp.where(counted, (sub >> 2) - (r0 & 3), 100)
        for q in range(2):
            y16 = jnp.zeros((16, KC), F32)
            for c in range(4):
                y16 = jnp.where((sub & 3) == c, y_ref[q, c:c + 1, cols], y16)
            coef = [y16 * wy_ref[a:a + 1, cols] for a in range(6)]
            for j in range(3):
                e = jnp.zeros((16, KC), F32)
                for a in range(6):
                    if -3 <= a - 4 * j <= 3:
                        e = jnp.where(t == a - 4 * j, coef[a], e)
                pay[48 * q + 16 * j:48 * q + 16 * j + 16, cols] = e.astype(BF)
        c0 = ((key & (GRID - 1)) + (GRID - 3)) & (GRID - 1)
        wx = wx_ref[:, cols].astype(F32)
        tc = jnp.where(counted, sub - (c0 & 15), 100)
        for j in range(2):
            e = jnp.zeros((16, KC), F32)
            for b in range(6):
                e = jnp.where(tc == b - 16 * j, wx[b:b + 1], e)
            pay[96 + 16 * j:112 + 16 * j, cols] = e.astype(BF)
        pay[128:144, cols] = jnp.broadcast_to(((r0 >> 2) + 1).astype(F32), (16, KC)).astype(BF)
        pay[144:160, cols] = jnp.broadcast_to((c0 >> 4).astype(F32), (16, KC)).astype(BF)


def iota16():
    return lax.broadcasted_iota(jnp.int32, (16, 1), 0).astype(F32)


def tiles(ch):
    first = 4 * (ch // 2) + ch % 2
    return first, first + 2


def ranks(key_ref, oh, rank):
    n_chunk = SAMPLES // RUN
    one, zero = jnp.ones((), BF), jnp.zeros((), BF)
    for ch in range(n_chunk):
        for k, t in enumerate(tiles(ch)):
            bucket = jnp.broadcast_to((((key_ref[:, 128 * t:128 * t + 128] >> 10) + 1) >> 2).astype(F32), (16, 128)).astype(BF)
            for g in range(5):
                oh[80 * ch + 16 * g:80 * ch + 16 * g + 16, 128 * k:128 * k + 128] = jnp.where(bucket == (iota16() + 16 * g).astype(BF), one, zero)
    lower = lax.broadcasted_iota(jnp.int32, (RUN, RUN + 128), 0)
    upper = lax.broadcasted_iota(jnp.int32, (RUN, RUN + 128), 1)
    tri = jnp.where((lower < upper) | (upper >= RUN), 1.0, 0.0).astype(BF)
    pre = jnp.dot(oh[...], tri, preferred_element_type=F32)
    counts = [pre[80 * ch:80 * ch + 80, RUN:] for ch in range(n_chunk)]
    strict = jnp.where(lax.broadcasted_iota(jnp.int32, (80, 80), 1) < lax.broadcasted_iota(jnp.int32, (80, 80), 0), 1.0, 0.0).astype(BF)
    for h in range(2):
        total = counts[h]
        for ch in range(h + 2, n_chunk, 2):
            total = total + counts[ch]
        high = jnp.floor(total * (1.0 / 256.0))
        low = total - 256.0 * high
        base = 256.0 * jnp.dot(strict, high.astype(BF), preferred_element_type=F32) + jnp.dot(strict, low.astype(BF), preferred_element_type=F32)
        for ch in range(h, n_chunk, 2):
            for k, t in enumerate(tiles(ch)):
                place = pre[80 * ch:80 * ch + 80, 128 * k:128 * k + 128] + base
                place = jnp.sum(oh[80 * ch:80 * ch + 80, 128 * k:128 * k + 128].astype(F32) * place, axis=0, keepdims=True)
                place = jnp.where(key_ref[:, 128 * t:128 * t + 128] >= 0, place, -1.0)
                rank[128 * t:128 * t + 128, :] = jnp.broadcast_to(place, (128, 128)).T
            base = base + counts[ch]


def reorder(sp, pay, rank, d_ref):
    lane = lax.broadcasted_iota(jnp.int32, (1, 128), 1).astype(F32)
    one, zero = jnp.ones((), BF), jnp.zeros((), BF)
    for h in range(2):
        total = None
        for ch in range(h, SAMPLES // RUN, 2):
            rows = []
            for t in tiles(ch):
                place = (rank[128 * t:128 * t + 128, :] - (sp * 256).astype(F32)).astype(BF)
                rows.append(jnp.concatenate([jnp.where(place == (lane + 128 * k).astype(BF), one, zero) for k in range(2)], axis=1))
            block = jnp.concatenate(rows, axis=0)
            values = jnp.concatenate([pay[:, 128 * t:128 * t + 128] for t in tiles(ch)], axis=1)
            part = jnp.dot(values, block, preferred_element_type=F32)
            total = part if total is None else total + part
        total = total.astype(BF)
        for k in range(2):
            d_ref[2 * sp + k, :, 128 * h:128 * h + 128] = total[:, 128 * k:128 * k + 128]


def exchange_kernel(y_ref, wy_ref, wx_ref, iy_ref, ix_ref, n_ref, y_out, wy_out, wx_out, key_out, key_own, d_out,
                    y_in, wy_in, wx_in, iy_in, ix_in, wx_bf, pay, oh, rank, loc, ssem, rsem):
    row_id = lax.axis_index('rows')
    other = {'rows': (row_id + 2) % 4}
    barrier = pltpu.get_barrier_semaphore()
    pl.semaphore_signal(barrier, inc=1, device_id=other, device_id_type=pl.DeviceIdType.MESH)
    pairs = [(iy_ref, iy_in), (ix_ref, ix_in), (wx_ref, wx_in), (wy_ref, wy_in), (y_ref, y_in)]
    locs = [pltpu.make_async_copy(a, b, loc.at[i]) for i, (a, b) in enumerate(pairs)]
    for cp in locs:
        cp.start()
    moves = [(y_ref, y_out), (wy_ref, wy_out), (key_own, key_out), (wx_bf, wx_out)]
    sends = [pltpu.make_async_remote_copy(src_ref=a, dst_ref=b, send_sem=ssem.at[i], recv_sem=rsem.at[i], device_id=other, device_id_type=pl.DeviceIdType.MESH) for i, (a, b) in enumerate(moves)]
    pl.semaphore_wait(barrier, 1)
    sends[0].start()
    sends[1].start()
    for cp in locs[:3]:
        cp.wait()
    slot = lax.broadcasted_iota(jnp.int32, iy_in.shape, 1)
    key_own[...] = jnp.where(slot < n_ref[0], (iy_in[...] - row_id * 256) * GRID + ix_in[...], -1000 * GRID)
    wx_bf[...] = wx_in[...].astype(BF)
    sends[2].start()
    sends[3].start()
    for cp in locs[3:]:
        cp.wait()
    payload(y_in, wy_in, wx_bf, key_own, pay)
    ranks(key_own, oh, rank)

    @pl.loop(0, SAMPLES // RUN // 2)
    def _(sp):
        reorder(sp, pay, rank, d_out)

    for cp in sends:
        cp.wait()


def sort_scratch():
    return [pltpu.VMEM((160, SAMPLES), BF), pltpu.VMEM((80 * (SAMPLES // RUN), RUN), BF), pltpu.VMEM((SAMPLES, 128), F32)]


def exchange(y, wy, wx, iy, ix, n):
    vm = pl.BlockSpec(memory_space=pltpu.VMEM)
    anym = pl.BlockSpec(memory_space=pl.ANY)
    dma = pltpu.SemaphoreType.DMA
    shape = jax.ShapeDtypeStruct
    return pl.pallas_call(
        exchange_kernel,
        out_shape=(shape(y.shape, F32), shape(wy.shape, F32), shape(wx.shape, BF), shape(iy.shape, jnp.int32), shape(iy.shape, jnp.int32), shape((SAMPLES // RUN, 160, RUN), BF)),
        in_specs=[anym] * 5 + [pl.BlockSpec(memory_space=pltpu.SMEM)],
        out_specs=(vm,) * 6,
        scratch_shapes=[pltpu.VMEM(v.shape, v.dtype) for v in (y, wy, wx, iy, ix)] + [pltpu.VMEM(wx.shape, BF)] + sort_scratch() + [dma((5,)), dma((4,)), dma((4,))],
        compiler_params=pltpu.CompilerParams(vmem_limit_bytes=12 * 2**20, collective_id=1, has_side_effects=True),
        cost_estimate=pl.CostEstimate(flops=10**9, bytes_accessed=10**6, transcendentals=0),
        name='exchange',
    )(y, wy, wx, iy, ix, n)


def spread_kernel(y_ref, wy_ref, wx_ref, key_ref, key_own, d_own, g_ref, e_ref, d_nb, pay, oh, rank, acc, *b_bufs):
    zero = jnp.zeros((16, RUN), BF)

    def product(d_ref, s, g0, right):
        rel = (d_ref[s, 128:144, :].astype(F32) - (g0 + 1).astype(F32)).astype(BF)
        left = []
        for q in range(2):
            e = [d_ref[s, 48 * q + 16 * j:48 * q + 16 * j + 16, :] for j in range(3)]
            for gi in range(WIN):
                m = [rel == jnp.array(gi - j, BF) for j in range(3)]
                left.append(jnp.where(m[0], e[0], jnp.where(m[1], e[1], jnp.where(m[2], e[2], zero))))
        return lax.dot_general(jnp.concatenate(left, axis=0), right, NT, preferred_element_type=F32)

    def add(g0, prod):
        rows = pl.ds(pl.multiple_of(g0 * 16, 16), 16 * WIN)
        for q in range(2):
            acc[q, rows, :] += prod[16 * WIN * q:16 * WIN * (q + 1)]

    def run_pair(d_ref, sp):
        first, last, prods = [], [], []
        for k in range(2):
            number = d_ref[2 * sp + k, 128:129, :].astype(F32)
            first.append(jnp.min(jnp.where(number > 0.0, number, 66.0)).astype(jnp.int32) - 1)
            last.append(jnp.max(number).astype(jnp.int32) + 1)
        for k in range(2):
            s = 2 * sp + k
            uc = d_ref[s, 144:160, :]
            eb = [d_ref[s, 96 + 16 * j:112 + 16 * j, :] for j in range(2)]
            right = jnp.concatenate([jnp.where(uc == jnp.array(g, BF), eb[0], jnp.where(uc == jnp.array((g - 1) % 64, BF), eb[1], zero)) for g in range(64)], axis=0)
            b_bufs[k][...] = right
            prods.append(product(d_ref, s, first[k], right))
        for k in range(2):
            add(first[k], prods[k])
        for k in range(2):
            @pl.loop(1, (last[k] - first[k] + WIN) // WIN)
            def _(w):
                g0 = first[k] + WIN * w
                add(g0, product(d_ref, 2 * sp + k, g0, b_bufs[k][...]))

    def block(o, d_ref, n_runs):
        if o:
            acc[:, :1056] = jnp.zeros((2, 1056, GRID), F32)


        @pl.loop(0, (n_runs + 1) // 2)
        def _(sp):
            run_pair(d_ref, sp)

        for q in range(2):
            e_ref[o, q, 0:32] = acc[q, 0:32, :]
            e_ref[o, q, 32:64] = acc[q, 1024:1056, :]
            g_ref[o, :, GRID * q:GRID * (q + 1)] = acc[q, 16:1040, :].astype(BF)

    n_own, n_nb = [(jnp.sum(jnp.where(k[...] >= 0, 1.0, 0.0)).astype(jnp.int32) + (RUN - 1)) // RUN for k in (key_own, key_ref)]
    payload(y_ref, wy_ref, wx_ref, key_ref, pay, acc)
    acc[:, 704:1056] = jnp.zeros((2, 352, GRID), F32)
    ranks(key_ref, oh, rank)

    @pl.loop(0, (n_nb + 1) // 2)
    def _(sp):
        reorder(sp, pay, rank, d_nb)

    block(0, d_own, n_own)
    block(1, d_nb, n_nb)


def spread(y, wy, wx, key, key_own, d_own):
    vm = pl.BlockSpec(memory_space=pltpu.VMEM)
    return pl.pallas_call(
        spread_kernel,
        out_shape=(jax.ShapeDtypeStruct((2, 1024, 2 * GRID), BF), jax.ShapeDtypeStruct((2, 2, 64, GRID), F32)),
        in_specs=[vm] * 6,
        out_specs=(vm, vm),
        scratch_shapes=[pltpu.VMEM((SAMPLES // RUN, 160, RUN), BF)] + sort_scratch() + [
            pltpu.VMEM((2, 16 * (66 + WIN), GRID), F32),
            pltpu.VMEM((GRID, RUN), BF),
            pltpu.VMEM((GRID, RUN), BF),
        ],
        compiler_params=pltpu.CompilerParams(vmem_limit_bytes=28 * 2**20),
        cost_estimate=pl.CostEstimate(flops=13 * 10**9, bytes_accessed=4 * 2**20, transcendentals=0),
        name='spread',
    )(y, wy, wx, key, key_own, d_own)


def combine_kernel(gg, ee, tab, maps, dd, out_ref, hbuf, hs, ge, rx, s_all, part, near, far, scale,
                   esend, erecv, ssend, srecv, hsend, hrecv, ysend, yrecv, nsend, nrecv):
    row_id = lax.axis_index('rows')
    y_id = lax.axis_index('coil')
    core = row_id % 2
    x_id = row_id // 2
    sib_row = row_id + 1 - 2 * core
    sib = {'rows': sib_row}
    blocks = [row_id, (row_id + 2) % 4]

    barrier = pltpu.get_barrier_semaphore()
    for dev in (sib, {'coil': 1 - y_id}, {'coil': 1 - y_id, 'rows': sib_row}):
        pl.semaphore_signal(barrier, inc=1, device_id=dev, device_id_type=pl.DeviceIdType.MESH)

    def rows_of(a, c):
        return pl.ds(pl.multiple_of(256 * a + 128 * c, 128), 128)

    for a in range(2):
        s_all[core, a] = maps[:, :, rows_of(a, core), :]
    row_scale = jnp.broadcast_to(dd[:, pl.ds(pl.multiple_of(y_id * 256, 256), 256)], (128, 256)).T
    scale[...] = row_scale * dd[:, pl.ds(pl.multiple_of(row_id * 128, 128), 128)]
    pl.semaphore_wait(barrier, 3)

    def remote(src, dst, send, recv, dev):
        return pltpu.make_async_remote_copy(src_ref=src, dst_ref=dst, send_sem=send, recv_sem=recv, device_id=dev, device_id_type=pl.DeviceIdType.MESH)

    e_copies = []
    for o in range(2):
        low = o * core + (1 - o) * (1 - core)
        high = o * (1 - core) + (1 - o) * core
        for k, (slot, end, row0) in enumerate(((low, 1, 0), (high, 0, 48))):
            e_copies.append(remote(ee.at[o, :, pl.ds(row0, 16)], rx.at[slot, end], esend.at[2 * o + k], erecv.at[slot, end], sib))
    for cp in e_copies:
        cp.start()
    s_copies = [remote(maps.at[:, :, rows_of(a, 1 - core)], s_all.at[core, a], ssend.at[a], srecv.at[a], sib) for a in range(2)]
    for cp in s_copies:
        cp.start()

    def columns(hc, lhs):
        cols = pl.ds(pl.multiple_of(x_id * 256 + hc * 128, 128), 128)
        t2 = jnp.concatenate([tab[0, cols, :], tab[1, cols, :]], axis=0)
        prod = lax.dot_general(lhs, t2, NT, preferred_element_type=F32)
        n = lhs.shape[0] // 2
        return prod[:n, :128] - prod[n:, 128:], prod[:n, 128:] + prod[n:, :128]

    def transform(hc, o, k):
        for j in range(2):
            rows = slice(512 * k + 256 * j, 512 * k + 256 * j + 256)
            pair = columns(hc, jnp.concatenate([gg[o, rows, :GRID], gg[o, rows, GRID:]], axis=0))
            for e in range(2):
                hs[o, e, rows] = pair[e]

    def take_halos():
        for cp in e_copies:
            cp.wait_send()
        for o in range(2):
            for end in range(2):
                remote(rx.at[o, end], rx.at[o, end], esend.at[2 * o + end], erecv.at[o, end], sib).wait_recv()
                for q in range(2):
                    ge[64 * q + 32 * o + 16 * end:64 * q + 32 * o + 16 * end + 16, :] = (ee[o, q, 16 + 16 * end:32 + 16 * end, :] + rx[o, end, q]).astype(BF)

    def patch(hc):
        return columns(hc, ge[...])

    def piece(hc, o, k):
        return remote(hbuf.at[hc, blocks[o], :, pl.ds(128 * k, 128)], hbuf.at[hc, blocks[o], :, pl.ds(128 * k, 128)], hsend.at[hc, o, k], hrecv.at[hc, o, k], sib)

    h_copies = [[piece(hc, o, k) for o in range(2) for k in range(2)] for hc in range(2)]

    def send(hc, o, k, pair):
        for e in range(2):
            hs[o, e, 1008 * k:1008 * k + 16] = pair[e][32 * o + 16 * k:32 * o + 16 * k + 16]
            for c in range(4):
                hbuf[hc, blocks[o], e, 128 * k:128 * k + 128, 128 * c:128 * c + 128] = hs[o, e, pl.ds(512 * k + c, 128, stride=4), :].astype(BF)
        h_copies[hc][2 * o + k].start()

    def image(hc, a):
        rows = rows_of(a, core)
        cos, sin = tab[0, rows, :], tab[1, rows, :]
        quarter = [slice(256 * p, 256 * p + 256) for p in range(4)]
        top = jnp.concatenate([v[:, q] for q in quarter for v in (cos, -sin)], axis=1)
        bottom = jnp.concatenate([v[:, q] for q in quarter for v in (sin, cos)], axis=1)
        both = jnp.dot(jnp.concatenate([top, bottom], axis=0), hbuf[hc].reshape(2048, 512), preferred_element_type=F32)
        re, im = both[:128], both[128:]
        xr = jnp.zeros((128, 128), F32)
        xi = jnp.zeros((128, 128), F32)
        for c in range(4):
            ir = re[:, 128 * c:128 * c + 128]
            ii = im[:, 128 * c:128 * c + 128]
            sr = s_all[hc, a, 0, c]
            si = s_all[hc, a, 1, c]
            xr = xr + (sr * ir + si * ii)
            xi = xi + (sr * ii - si * ir)
        part[hc, a, 0] = xr
        part[hc, a, 1] = xi

    y_copies = [remote(part.at[hc, 1 - y_id], far.at[core], ysend.at[hc], yrecv.at[core], {'coil': 1 - y_id, 'rows': 2 * x_id + hc}) for hc in range(2)]
    n_copy = remote(part.at[1 - core, y_id], near, nsend.at[0], nrecv.at[0], sib)

    for k in range(2):
        transform(0, 0, k)
    take_halos()
    pair = patch(0)
    for k in range(2):
        send(0, 0, k, pair)
    for k in range(2):
        transform(0, 1, k)
        send(0, 1, k, pair)
    pair = patch(1)
    for k in range(2):
        transform(1, 0, k)
        send(1, 0, k, pair)
    for cp in s_copies + h_copies[0]:
        cp.wait()
    image(0, 1 - y_id)
    y_copies[0].start()
    for k in range(2):
        transform(1, 1, k)
        send(1, 1, k, pair)
    image(0, y_id)
    for cp in h_copies[1]:
        cp.wait()
    image(1, 1 - y_id)
    y_copies[1].start()
    image(1, y_id)
    n_copy.start()
    for cp in y_copies:
        cp.wait_send()
    n_copy.wait()
    mine = pl.ds(pl.multiple_of(128 * core, 128), 128)
    other = pl.ds(pl.multiple_of(128 * (1 - core), 128), 128)
    for e in range(2):
        out_ref[e, mine] = part[core, y_id, e]
        out_ref[e, other] = near[e]
    for k in range(2):
        remote(far.at[k], far.at[k], ysend.at[k], yrecv.at[k], {'coil': 1 - y_id}).wait_recv()
        sl = slice(128 * k, 128 * k + 128)
        for e in range(2):
            out_ref[e, sl] = (out_ref[e, sl] + far[k, e]) * scale[sl]


def combine(gg, ee, tab, maps, dd):
    vm = pl.BlockSpec(memory_space=pltpu.VMEM)
    dma = pltpu.SemaphoreType.DMA
    return pl.pallas_call(
        combine_kernel,
        out_shape=jax.ShapeDtypeStruct((2, 256, 128), F32),
        in_specs=[vm] * 5,
        out_specs=vm,
        scratch_shapes=[
            pltpu.VMEM((2, 4, 2, 256, 512), BF),
            pltpu.VMEM((2, 2, 1024, 128), F32),
            pltpu.VMEM((128, GRID), BF),
            pltpu.VMEM((2, 2, 2, 16, GRID), F32),
            pltpu.VMEM((2, 2, 2, 4, 128, 128), F32),
            pltpu.VMEM((2, 2, 2, 128, 128), F32),
            pltpu.VMEM((2, 128, 128), F32),
            pltpu.VMEM((2, 2, 128, 128), F32),
            pltpu.VMEM((256, 128), F32),
            dma((4,)), dma((2, 2)), dma((2,)), dma((2,)), dma((2, 2, 2)), dma((2, 2, 2)), dma((2,)), dma((2,)), dma((1,)), dma((1,)),
        ],
        compiler_params=pltpu.CompilerParams(vmem_limit_bytes=24 * 2**20, collective_id=0, has_side_effects=True),
        cost_estimate=pl.CostEstimate(flops=7 * 10**9, bytes_accessed=12 * 2**20, transcendentals=0),
        name='combine',
    )(gg, ee, tab, maps, dd)


def solution(mesh):
    def local_part(kspace, weight_row, weight_col, grid_row, grid_col, valid_count, coil_maps, deapod):
        n_img = deapod.shape[0]
        hbm = [pltpu.with_memory_space_constraint(v, pltpu.HBM) for v in (kspace, weight_row, weight_col, grid_row[None], grid_col[None])]
        stacked = exchange(*hbm, valid_count)
        tab = jnp.asarray(tables(n_img))
        gg, ee = spread(*stacked)
        return combine(gg, ee, tab, coil_maps, deapod[None])

    spec_samples = P(None, 'coil', ('slab', 'rows'))
    spec_weights = P(None, ('slab', 'rows'))
    spec_index = P(('slab', 'rows'))
    return jax.shard_map(local_part, mesh=mesh, in_specs=(spec_samples, spec_weights, spec_weights, spec_index, spec_index, spec_index, P(None, 'coil', 'slab', 'rows'), P()), out_specs=P(None, ('slab', 'coil'), 'rows'), check_vma=False)
```

```python
import math
import functools
import numpy as np
import jax
import jax.numpy as jnp
from jax import lax
from jax.experimental import pallas as pl
from jax.experimental.pallas import tpu as pltpu
from jax.sharding import PartitionSpec as P

F32 = jnp.float32
BF = jnp.bfloat16
NT = (((1,), (1,)), ((), ()))
KC = 512
GRID = 1024
SAMPLES = 2048
RUN = 256
WIN = 16


def tables(n_img):
    n_grid = 2 * n_img
    pix = np.arange(n_img) - n_img // 2
    freq = np.arange(n_grid) - n_img
    ang = np.mod(pix[:, None] * freq[None, :], n_grid) * (2.0 * math.pi / n_grid)
    return np.stack([np.cos(ang), np.sin(ang)]).astype(np.float32).astype(BF)


def payload(y_ref, wy_ref, wx_ref, key_ref, pay, clear=None):
    @pl.loop(0, SAMPLES // KC)
    def _(s):
        cols = pl.ds(pl.multiple_of(s * KC, KC), KC)
        sub = lax.broadcasted_iota(jnp.int32, (16, KC), 0)
        if clear is not None:
            clear[:, pl.ds(pl.multiple_of(s * 176, 16), 176), :] = jnp.zeros((2, 176, GRID), F32)
        key = key_ref[:, cols]
        r0 = (key >> 10) + 1
        counted = r0 > 0
        t = jnp.where(counted, (sub >> 2) - (r0 & 3), 100)
        for q in range(2):
            y16 = jnp.zeros((16, KC), F32)
            for c in range(4):
                y16 = jnp.where((sub & 3) == c, y_ref[q, c:c + 1, cols], y16)
            coef = [y16 * wy_ref[a:a + 1, cols] for a in range(6)]
            for j in range(3):
                e = jnp.zeros((16, KC), F32)
                for a in range(6):
                    if -3 <= a - 4 * j <= 3:
                        e = jnp.where(t == a - 4 * j, coef[a], e)
                pay[48 * q + 16 * j:48 * q + 16 * j + 16, cols] = e.astype(BF)
        c0 = ((key & (GRID - 1)) + (GRID - 3)) & (GRID - 1)
        wx = wx_ref[:, cols].astype(F32)
        tc = jnp.where(counted, sub - (c0 & 15), 100)
        for j in range(2):
            e = jnp.zeros((16, KC), F32)
            for b in range(6):
                e = jnp.where(tc == b - 16 * j, wx[b:b + 1], e)
            pay[96 + 16 * j:112 + 16 * j, cols] = e.astype(BF)
        pay[128:144, cols] = jnp.broadcast_to(((r0 >> 2) + 1).astype(F32), (16, KC)).astype(BF)
        pay[144:160, cols] = jnp.broadcast_to((c0 >> 4).astype(F32), (16, KC)).astype(BF)


def iota16():
    return lax.broadcasted_iota(jnp.int32, (16, 1), 0).astype(F32)


def tiles(ch):
    first = 4 * (ch // 2) + ch % 2
    return first, first + 2


def ranks(key_ref, oh, rank):
    n_chunk = SAMPLES // RUN
    one, zero = jnp.ones((), BF), jnp.zeros((), BF)
    for ch in range(n_chunk):
        for k, t in enumerate(tiles(ch)):
            bucket = jnp.broadcast_to((((key_ref[:, 128 * t:128 * t + 128] >> 10) + 1) >> 2).astype(F32), (16, 128)).astype(BF)
            for g in range(5):
                oh[80 * ch + 16 * g:80 * ch + 16 * g + 16, 128 * k:128 * k + 128] = jnp.where(bucket == (iota16() + 16 * g).astype(BF), one, zero)
    lower = lax.broadcasted_iota(jnp.int32, (RUN, RUN + 128), 0)
    upper = lax.broadcasted_iota(jnp.int32, (RUN, RUN + 128), 1)
    tri = jnp.where((lower < upper) | (upper >= RUN), 1.0, 0.0).astype(BF)
    pre = jnp.dot(oh[...], tri, preferred_element_type=F32)
    counts = [pre[80 * ch:80 * ch + 80, RUN:] for ch in range(n_chunk)]
    strict = jnp.where(lax.broadcasted_iota(jnp.int32, (80, 80), 1) < lax.broadcasted_iota(jnp.int32, (80, 80), 0), 1.0, 0.0).astype(BF)
    for h in range(2):
        total = counts[h]
        for ch in range(h + 2, n_chunk, 2):
            total = total + counts[ch]
        high = jnp.floor(total * (1.0 / 256.0))
        low = total - 256.0 * high
        base = 256.0 * jnp.dot(strict, high.astype(BF), preferred_element_type=F32) + jnp.dot(strict, low.astype(BF), preferred_element_type=F32)
        for ch in range(h, n_chunk, 2):
            for k, t in enumerate(tiles(ch)):
                place = pre[80 * ch:80 * ch + 80, 128 * k:128 * k + 128] + base
                place = jnp.sum(oh[80 * ch:80 * ch + 80, 128 * k:128 * k + 128].astype(F32) * place, axis=0, keepdims=True)
                place = jnp.where(key_ref[:, 128 * t:128 * t + 128] >= 0, place, -1.0)
                rank[128 * t:128 * t + 128, :] = jnp.broadcast_to(place, (128, 128)).T
            base = base + counts[ch]


def reorder(sp, pay, rank, d_ref):
    lane = lax.broadcasted_iota(jnp.int32, (1, 128), 1).astype(F32)
    one, zero = jnp.ones((), BF), jnp.zeros((), BF)
    for h in range(2):
        total = None
        for ch in range(h, SAMPLES // RUN, 2):
            rows = []
            for t in tiles(ch):
                place = (rank[128 * t:128 * t + 128, :] - (sp * 256).astype(F32)).astype(BF)
                rows.append(jnp.concatenate([jnp.where(place == (lane + 128 * k).astype(BF), one, zero) for k in range(2)], axis=1))
            block = jnp.concatenate(rows, axis=0)
            values = jnp.concatenate([pay[:, 128 * t:128 * t + 128] for t in tiles(ch)], axis=1)
            part = jnp.dot(values, block, preferred_element_type=F32)
            total = part if total is None else total + part
        total = total.astype(BF)
        for k in range(2):
            d_ref[2 * sp + k, :, 128 * h:128 * h + 128] = total[:, 128 * k:128 * k + 128]


def exchange_kernel(y_ref, wy_ref, wx_ref, iy_ref, ix_ref, n_ref, y_out, wy_out, wx_out, key_out, key_own, d_out,
                    y_in, wy_in, wx_in, iy_in, ix_in, wx_bf, pay, oh, rank, loc, ssem, rsem):
    row_id = lax.axis_index('rows')
    other = {'rows': (row_id + 2) % 4}
    barrier = pltpu.get_barrier_semaphore()
    pl.semaphore_signal(barrier, inc=1, device_id=other, device_id_type=pl.DeviceIdType.MESH)
    pairs = [(iy_ref, iy_in), (ix_ref, ix_in), (wx_ref, wx_in), (wy_ref, wy_in), (y_ref, y_in)]
    locs = [pltpu.make_async_copy(a, b, loc.at[i]) for i, (a, b) in enumerate(pairs)]
    for cp in locs:
        cp.start()
    moves = [(y_ref, y_out), (wy_ref, wy_out), (key_own, key_out), (wx_bf, wx_out)]
    sends = [pltpu.make_async_remote_copy(src_ref=a, dst_ref=b, send_sem=ssem.at[i], recv_sem=rsem.at[i], device_id=other, device_id_type=pl.DeviceIdType.MESH) for i, (a, b) in enumerate(moves)]
    pl.semaphore_wait(barrier, 1)
    sends[0].start()
    sends[1].start()
    for cp in locs[:3]:
        cp.wait()
    slot = lax.broadcasted_iota(jnp.int32, iy_in.shape, 1)
    key_own[...] = jnp.where(slot < n_ref[0], (iy_in[...] - row_id * 256) * GRID + ix_in[...], -1000 * GRID)
    wx_bf[...] = wx_in[...].astype(BF)
    sends[2].start()
    sends[3].start()
    for cp in locs[3:]:
        cp.wait()
    payload(y_in, wy_in, wx_bf, key_own, pay)
    ranks(key_own, oh, rank)

    @pl.loop(0, SAMPLES // RUN // 2)
    def _(sp):
        reorder(sp, pay, rank, d_out)

    for cp in sends:
        cp.wait()


def sort_scratch():
    return [pltpu.VMEM((160, SAMPLES), BF), pltpu.VMEM((80 * (SAMPLES // RUN), RUN), BF), pltpu.VMEM((SAMPLES, 128), F32)]


def exchange(y, wy, wx, iy, ix, n):
    vm = pl.BlockSpec(memory_space=pltpu.VMEM)
    anym = pl.BlockSpec(memory_space=pl.ANY)
    dma = pltpu.SemaphoreType.DMA
    shape = jax.ShapeDtypeStruct
    return pl.pallas_call(
        exchange_kernel,
        out_shape=(shape(y.shape, F32), shape(wy.shape, F32), shape(wx.shape, BF), shape(iy.shape, jnp.int32), shape(iy.shape, jnp.int32), shape((SAMPLES // RUN, 160, RUN), BF)),
        in_specs=[anym] * 5 + [pl.BlockSpec(memory_space=pltpu.SMEM)],
        out_specs=(vm,) * 6,
        scratch_shapes=[pltpu.VMEM(v.shape, v.dtype) for v in (y, wy, wx, iy, ix)] + [pltpu.VMEM(wx.shape, BF)] + sort_scratch() + [dma((5,)), dma((4,)), dma((4,))],
        compiler_params=pltpu.CompilerParams(vmem_limit_bytes=12 * 2**20, collective_id=1, has_side_effects=True),
        cost_estimate=pl.CostEstimate(flops=10**9, bytes_accessed=10**6, transcendentals=0),
        name='exchange',
    )(y, wy, wx, iy, ix, n)


def spread_kernel(y_ref, wy_ref, wx_ref, key_ref, key_own, d_own, g_ref, e_ref, d_nb, pay, oh, rank, acc, *b_bufs):
    zero = jnp.zeros((16, RUN), BF)

    def product(d_ref, s, g0, right):
        rel = (d_ref[s, 128:144, :].astype(F32) - (g0 + 1).astype(F32)).astype(BF)
        left = []
        for q in range(2):
            e = [d_ref[s, 48 * q + 16 * j:48 * q + 16 * j + 16, :] for j in range(3)]
            for gi in range(WIN):
                m = [rel == jnp.array(gi - j, BF) for j in range(3)]
                left.append(jnp.where(m[0], e[0], jnp.where(m[1], e[1], jnp.where(m[2], e[2], zero))))
        return lax.dot_general(jnp.concatenate(left, axis=0), right, NT, preferred_element_type=F32)

    def add(g0, prod):
        rows = pl.ds(pl.multiple_of(g0 * 16, 16), 16 * WIN)
        for q in range(2):
            acc[q, rows, :] += prod[16 * WIN * q:16 * WIN * (q + 1)]

    def run_pair(d_ref, sp):
        first, last, prods = [], [], []
        for k in range(2):
            number = d_ref[2 * sp + k, 128:129, :].astype(F32)
            first.append(jnp.min(jnp.where(number > 0.0, number, 66.0)).astype(jnp.int32) - 1)
            last.append(jnp.max(number).astype(jnp.int32) + 1)
        for k in range(2):
            s = 2 * sp + k
            uc = d_ref[s, 144:160, :]
            eb = [d_ref[s, 96 + 16 * j:112 + 16 * j, :] for j in range(2)]
            right = jnp.concatenate([jnp.where(uc == jnp.array(g, BF), eb[0], jnp.where(uc == jnp.array((g - 1) % 64, BF), eb[1], zero)) for g in range(64)], axis=0)
            b_bufs[k][...] = right
            prods.append(product(d_ref, s, first[k], right))
        for k in range(2):
            add(first[k], prods[k])
        for k in range(2):
            @pl.loop(1, (last[k] - first[k] + WIN) // WIN)
            def _(w):
                g0 = first[k] + WIN * w
                add(g0, product(d_ref, 2 * sp + k, g0, b_bufs[k][...]))

    def block(o, d_ref, n_runs):
        if o:
            acc[:, :1056] = jnp.zeros((2, 1056, GRID), F32)


        @pl.loop(0, (n_runs + 1) // 2)
        def _(sp):
            run_pair(d_ref, sp)

        for q in range(2):
            e_ref[o, q, 0:32] = acc[q, 0:32, :]
            e_ref[o, q, 32:64] = acc[q, 1024:1056, :]
            g_ref[o, :, GRID * q:GRID * (q + 1)] = acc[q, 16:1040, :].astype(BF)

    n_own, n_nb = [(jnp.sum(jnp.where(k[...] >= 0, 1.0, 0.0)).astype(jnp.int32) + (RUN - 1)) // RUN for k in (key_own, key_ref)]
    payload(y_ref, wy_ref, wx_ref, key_ref, pay, acc)
    acc[:, 704:1056] = jnp.zeros((2, 352, GRID), F32)
    ranks(key_ref, oh, rank)

    @pl.loop(0, (n_nb + 1) // 2)
    def _(sp):
        reorder(sp, pay, rank, d_nb)

    block(0, d_own, n_own)
    block(1, d_nb, n_nb)


def spread(y, wy, wx, key, key_own, d_own):
    vm = pl.BlockSpec(memory_space=pltpu.VMEM)
    return pl.pallas_call(
        spread_kernel,
        out_shape=(jax.ShapeDtypeStruct((2, 1024, 2 * GRID), BF), jax.ShapeDtypeStruct((2, 2, 64, GRID), F32)),
        in_specs=[vm] * 6,
        out_specs=(vm, vm),
        scratch_shapes=[pltpu.VMEM((SAMPLES // RUN, 160, RUN), BF)] + sort_scratch() + [
            pltpu.VMEM((2, 16 * (66 + WIN), GRID), F32),
            pltpu.VMEM((GRID, RUN), BF),
            pltpu.VMEM((GRID, RUN), BF),
        ],
        compiler_params=pltpu.CompilerParams(vmem_limit_bytes=28 * 2**20),
        cost_estimate=pl.CostEstimate(flops=13 * 10**9, bytes_accessed=4 * 2**20, transcendentals=0),
        name='spread',
    )(y, wy, wx, key, key_own, d_own)


def combine_kernel(gg, ee, tab, maps, dd, out_ref, hbuf, hs, ge, rx, s_all, part, near, far, scale,
                   esend, erecv, ssend, srecv, hsend, hrecv, ysend, yrecv, nsend, nrecv):
    row_id = lax.axis_index('rows')
    y_id = lax.axis_index('coil')
    core = row_id % 2
    x_id = row_id // 2
    sib = {'rows': row_id + 1 - 2 * core}
    blocks = [row_id, (row_id + 2) % 4]

    barrier = pltpu.get_barrier_semaphore()
    mate = {'coil': 1 - y_id}
    for dev in (sib, mate):
        pl.semaphore_signal(barrier, inc=1, device_id=dev, device_id_type=pl.DeviceIdType.MESH)

    def rows_of(a, c):
        return pl.ds(pl.multiple_of(256 * a + 128 * c, 128), 128)

    for k in range(2):
        s_all[core, k] = maps[:, :, rows_of(1 - y_id, k), :]
    row_scale = jnp.broadcast_to(dd[:, pl.ds(pl.multiple_of(y_id * 256, 256), 256)], (128, 256)).T
    scale[...] = row_scale * dd[:, pl.ds(pl.multiple_of(row_id * 128, 128), 128)]
    pl.semaphore_wait(barrier, 2)

    def remote(src, dst, send, recv, dev):
        return pltpu.make_async_remote_copy(src_ref=src, dst_ref=dst, send_sem=send, recv_sem=recv, device_id=dev, device_id_type=pl.DeviceIdType.MESH)

    e_copies = []
    for o in range(2):
        low = o * core + (1 - o) * (1 - core)
        high = o * (1 - core) + (1 - o) * core
        for k, (slot, end, row0) in enumerate(((low, 1, 0), (high, 0, 48))):
            e_copies.append(remote(ee.at[o, :, pl.ds(row0, 16)], rx.at[slot, end], esend.at[2 * o + k], erecv.at[slot, end], sib))
    for cp in e_copies:
        cp.start()
    s_copies = [remote(maps.at[:, :, rows_of(y_id, k)], s_all.at[core, k], ssend.at[k], srecv.at[k], sib) for k in range(2)]
    for cp in s_copies:
        cp.start()

    def columns(hc, lhs):
        cols = pl.ds(pl.multiple_of(x_id * 256 + hc * 128, 128), 128)
        t2 = jnp.concatenate([tab[0, cols, :], tab[1, cols, :]], axis=0)
        prod = lax.dot_general(lhs, t2, NT, preferred_element_type=F32)
        n = lhs.shape[0] // 2
        return prod[:n, :128] - prod[n:, 128:], prod[:n, 128:] + prod[n:, :128]

    def transform(hc, o, k):
        for j in range(2):
            rows = slice(512 * k + 256 * j, 512 * k + 256 * j + 256)
            pair = columns(hc, jnp.concatenate([gg[o, rows, :GRID], gg[o, rows, GRID:]], axis=0))
            for e in range(2):
                hs[o, e, rows] = pair[e]

    def take_halos():
        for cp in e_copies:
            cp.wait_send()
        for o in range(2):
            for end in range(2):
                remote(rx.at[o, end], rx.at[o, end], esend.at[2 * o + end], erecv.at[o, end], sib).wait_recv()
                for q in range(2):
                    ge[64 * q + 32 * o + 16 * end:64 * q + 32 * o + 16 * end + 16, :] = (ee[o, q, 16 + 16 * end:32 + 16 * end, :] + rx[o, end, q]).astype(BF)

    def patch(hc):
        return columns(hc, ge[...])

    def piece(hc, o, k):
        return remote(hbuf.at[hc, blocks[o], :, pl.ds(128 * k, 128)], hbuf.at[hc, blocks[o], :, pl.ds(128 * k, 128)], hsend.at[hc, o, k], hrecv.at[hc, o, k], sib)

    h_copies = [[piece(hc, o, k) for o in range(2) for k in range(2)] for hc in range(2)]

    def send(hc, o, k, pair):
        for e in range(2):
            hs[o, e, 1008 * k:1008 * k + 16] = pair[e][32 * o + 16 * k:32 * o + 16 * k + 16]
            for c in range(4):
                hbuf[hc, blocks[o], e, 128 * k:128 * k + 128, 128 * c:128 * c + 128] = hs[o, e, pl.ds(512 * k + c, 128, stride=4), :].astype(BF)
        h_copies[hc][2 * o + k].start()

    def image(hc, k):
        rows = rows_of(y_id + (1 - 2 * y_id) * (1 - core - hc + 2 * core * hc), k)
        cos, sin = tab[0, rows, :], tab[1, rows, :]
        quarter = [slice(256 * p, 256 * p + 256) for p in range(4)]
        top = jnp.concatenate([v[:, q] for q in quarter for v in (cos, -sin)], axis=1)
        bottom = jnp.concatenate([v[:, q] for q in quarter for v in (sin, cos)], axis=1)
        both = jnp.dot(jnp.concatenate([top, bottom], axis=0), hbuf[hc].reshape(2048, 512), preferred_element_type=F32)
        re, im = both[:128], both[128:]
        xr = jnp.zeros((128, 128), F32)
        xi = jnp.zeros((128, 128), F32)
        for c in range(4):
            ir = re[:, 128 * c:128 * c + 128]
            ii = im[:, 128 * c:128 * c + 128]
            sr = s_all[hc, k, 0, c]
            si = s_all[hc, k, 1, c]
            xr = xr + (sr * ir + si * ii)
            xi = xi + (sr * ii - si * ir)
        part[hc, k, 0] = xr
        part[hc, k, 1] = xi

        @pl.when(core == hc)
        def _():
            y_copies[k].start()

        @pl.when(core != hc)
        def _():
            n_copies[k].start()

    y_copies = [remote(part.at[core, k], far.at[k], ysend.at[k], yrecv.at[k], mate) for k in range(2)]
    n_copies = [remote(part.at[1 - core, k], near.at[k], nsend.at[k], nrecv.at[k], sib) for k in range(2)]

    for k in range(2):
        transform(0, 0, k)
    take_halos()
    pair = patch(0)
    for k in range(2):
        send(0, 0, k, pair)
    for k in range(2):
        transform(0, 1, k)
        send(0, 1, k, pair)
    pair = patch(1)
    for k in range(2):
        transform(1, 0, k)
        send(1, 0, k, pair)
    for cp in s_copies + h_copies[0]:
        cp.wait()
    image(0, 0)
    for k in range(2):
        transform(1, 1, k)
        send(1, 1, k, pair)
    image(0, 1)
    for cp in h_copies[1]:
        cp.wait()
    for k in range(2):
        image(1, k)
    for k in range(2):
        n_copies[k].wait()
        y_copies[k].wait()
        sl = slice(128 * k, 128 * k + 128)
        for e in range(2):
            out_ref[e, sl] = (near[k, e] + far[k, e]) * scale[sl]


def combine(gg, ee, tab, maps, dd):
    vm = pl.BlockSpec(memory_space=pltpu.VMEM)
    dma = pltpu.SemaphoreType.DMA
    return pl.pallas_call(
        combine_kernel,
        out_shape=jax.ShapeDtypeStruct((2, 256, 128), F32),
        in_specs=[vm] * 5,
        out_specs=vm,
        scratch_shapes=[
            pltpu.VMEM((2, 4, 2, 256, 512), BF),
            pltpu.VMEM((2, 2, 1024, 128), F32),
            pltpu.VMEM((128, GRID), BF),
            pltpu.VMEM((2, 2, 2, 16, GRID), F32),
            pltpu.VMEM((2, 2, 2, 4, 128, 128), F32),
            pltpu.VMEM((2, 2, 2, 128, 128), F32),
            pltpu.VMEM((2, 2, 128, 128), F32),
            pltpu.VMEM((2, 2, 128, 128), F32),
            pltpu.VMEM((256, 128), F32),
            dma((4,)), dma((2, 2)), dma((2,)), dma((2,)), dma((2, 2, 2)), dma((2, 2, 2)), dma((2,)), dma((2,)), dma((2,)), dma((2,)),
        ],
        compiler_params=pltpu.CompilerParams(vmem_limit_bytes=24 * 2**20, collective_id=0, has_side_effects=True),
        cost_estimate=pl.CostEstimate(flops=7 * 10**9, bytes_accessed=12 * 2**20, transcendentals=0),
        name='combine',
    )(gg, ee, tab, maps, dd)


def solution(mesh):
    def local_part(kspace, weight_row, weight_col, grid_row, grid_col, valid_count, coil_maps, deapod):
        n_img = deapod.shape[0]
        hbm = [pltpu.with_memory_space_constraint(v, pltpu.HBM) for v in (kspace, weight_row, weight_col, grid_row[None], grid_col[None])]
        stacked = exchange(*hbm, valid_count)
        tab = jnp.asarray(tables(n_img))
        gg, ee = spread(*stacked)
        return combine(gg, ee, tab, coil_maps, deapod[None])

    spec_samples = P(None, 'coil', ('slab', 'rows'))
    spec_weights = P(None, ('slab', 'rows'))
    spec_index = P(('slab', 'rows'))
    return jax.shard_map(local_part, mesh=mesh, in_specs=(spec_samples, spec_weights, spec_weights, spec_index, spec_index, spec_index, P(None, 'coil', 'slab', 'rows'), P()), out_specs=P(None, ('slab', 'coil'), 'rows'), check_vma=False)
```

```python
import math
import functools
import numpy as np
import jax
import jax.numpy as jnp
from jax import lax
from jax.experimental import pallas as pl
from jax.experimental.pallas import tpu as pltpu
from jax.sharding import PartitionSpec as P

F32 = jnp.float32
BF = jnp.bfloat16
NT = (((1,), (1,)), ((), ()))
KC = 512
GRID = 1024
SAMPLES = 2048
RUN = 256
WIN = 16


def tables(n_img):
    n_grid = 2 * n_img
    pix = np.arange(n_img) - n_img // 2
    freq = np.arange(n_grid) - n_img
    ang = np.mod(pix[:, None] * freq[None, :], n_grid) * (2.0 * math.pi / n_grid)
    return np.stack([np.cos(ang), np.sin(ang)]).astype(np.float32).astype(BF)


def payload(y_ref, wy_ref, wx_ref, key_ref, pay, clear=None):
    for s in range(SAMPLES // KC):
        cols = slice(s * KC, s * KC + KC)
        sub = lax.broadcasted_iota(jnp.int32, (16, KC), 0)
        if clear is not None:
            clear[:, 176 * s:176 * s + 176, :] = jnp.zeros((2, 176, GRID), F32)
        key = key_ref[:, cols]
        r0 = (key >> 10) + 1
        counted = r0 > 0
        t = jnp.where(counted, (sub >> 2) - (r0 & 3), 100)
        for q in range(2):
            y16 = jnp.zeros((16, KC), F32)
            for c in range(4):
                y16 = jnp.where((sub & 3) == c, y_ref[q, c:c + 1, cols], y16)
            coef = [y16 * wy_ref[a:a + 1, cols] for a in range(6)]
            for j in range(3):
                e = jnp.zeros((16, KC), F32)
                for a in range(6):
                    if -3 <= a - 4 * j <= 3:
                        e = jnp.where(t == a - 4 * j, coef[a], e)
                pay[48 * q + 16 * j:48 * q + 16 * j + 16, cols] = e.astype(BF)
        c0 = ((key & (GRID - 1)) + (GRID - 3)) & (GRID - 1)
        wx = wx_ref[:, cols].astype(F32)
        tc = jnp.where(counted, sub - (c0 & 15), 100)
        for j in range(2):
            e = jnp.zeros((16, KC), F32)
            for b in range(6):
                e = jnp.where(tc == b - 16 * j, wx[b:b + 1], e)
            pay[96 + 16 * j:112 + 16 * j, cols] = e.astype(BF)
        pay[128:144, cols] = jnp.broadcast_to(((r0 >> 2) + 1).astype(F32), (16, KC)).astype(BF)
        pay[144:160, cols] = jnp.broadcast_to((c0 >> 4).astype(F32), (16, KC)).astype(BF)


def iota16():
    return lax.broadcasted_iota(jnp.int32, (16, 1), 0).astype(F32)


def tiles(ch):
    first = 4 * (ch // 2) + ch % 2
    return first, first + 2


def ranks(key_ref, oh, rank):
    n_chunk = SAMPLES // RUN
    one, zero = jnp.ones((), BF), jnp.zeros((), BF)
    for ch in range(n_chunk):
        for k, t in enumerate(tiles(ch)):
            bucket = jnp.broadcast_to((((key_ref[:, 128 * t:128 * t + 128] >> 10) + 1) >> 2).astype(F32), (16, 128)).astype(BF)
            for g in range(5):
                oh[80 * ch + 16 * g:80 * ch + 16 * g + 16, 128 * k:128 * k + 128] = jnp.where(bucket == (iota16() + 16 * g).astype(BF), one, zero)
    lower = lax.broadcasted_iota(jnp.int32, (RUN, RUN + 128), 0)
    upper = lax.broadcasted_iota(jnp.int32, (RUN, RUN + 128), 1)
    tri = jnp.where((lower < upper) | (upper >= RUN), 1.0, 0.0).astype(BF)
    pre = jnp.dot(oh[...], tri, preferred_element_type=F32)
    counts = [pre[80 * ch:80 * ch + 80, RUN:] for ch in range(n_chunk)]
    strict = jnp.where(lax.broadcasted_iota(jnp.int32, (80, 80), 1) < lax.broadcasted_iota(jnp.int32, (80, 80), 0), 1.0, 0.0).astype(BF)
    for h in range(2):
        total = counts[h]
        for ch in range(h + 2, n_chunk, 2):
            total = total + counts[ch]
        high = jnp.floor(total * (1.0 / 256.0))
        low = total - 256.0 * high
        base = 256.0 * jnp.dot(strict, high.astype(BF), preferred_element_type=F32) + jnp.dot(strict, low.astype(BF), preferred_element_type=F32)
        for ch in range(h, n_chunk, 2):
            for k, t in enumerate(tiles(ch)):
                place = pre[80 * ch:80 * ch + 80, 128 * k:128 * k + 128] + base
                place = jnp.sum(oh[80 * ch:80 * ch + 80, 128 * k:128 * k + 128].astype(F32) * place, axis=0, keepdims=True)
                place = jnp.where(key_ref[:, 128 * t:128 * t + 128] >= 0, place, -1.0)
                rank[128 * t:128 * t + 128, :] = jnp.broadcast_to(place, (128, 128)).T
            base = base + counts[ch]


def reorder(sp, pay, rank, d_ref):
    lane = lax.broadcasted_iota(jnp.int32, (1, 128), 1).astype(F32)
    one, zero = jnp.ones((), BF), jnp.zeros((), BF)
    for h in range(2):
        total = None
        for ch in range(h, SAMPLES // RUN, 2):
            rows = []
            for t in tiles(ch):
                place = (rank[128 * t:128 * t + 128, :] - (sp * 256).astype(F32)).astype(BF)
                rows.append(jnp.concatenate([jnp.where(place == (lane + 128 * k).astype(BF), one, zero) for k in range(2)], axis=1))
            block = jnp.concatenate(rows, axis=0)
            values = jnp.concatenate([pay[:, 128 * t:128 * t + 128] for t in tiles(ch)], axis=1)
            part = jnp.dot(values, block, preferred_element_type=F32)
            total = part if total is None else total + part
        total = total.astype(BF)
        for k in range(2):
            d_ref[2 * sp + k, :, 128 * h:128 * h + 128] = total[:, 128 * k:128 * k + 128]


def exchange_kernel(y_ref, wy_ref, wx_ref, iy_ref, ix_ref, n_ref, y_out, wy_out, wx_out, key_out, key_own, d_out,
                    y_in, wy_in, wx_in, iy_in, ix_in, wx_bf, pay, oh, rank, loc, ssem, rsem):
    row_id = lax.axis_index('rows')
    other = {'rows': (row_id + 2) % 4}
    barrier = pltpu.get_barrier_semaphore()
    pl.semaphore_signal(barrier, inc=1, device_id=other, device_id_type=pl.DeviceIdType.MESH)
    pairs = [(iy_ref, iy_in), (ix_ref, ix_in), (wx_ref, wx_in), (wy_ref, wy_in), (y_ref, y_in)]
    locs = [pltpu.make_async_copy(a, b, loc.at[i]) for i, (a, b) in enumerate(pairs)]
    for cp in locs:
        cp.start()
    moves = [(y_ref, y_out), (wy_ref, wy_out), (key_own, key_out), (wx_bf, wx_out)]
    sends = [pltpu.make_async_remote_copy(src_ref=a, dst_ref=b, send_sem=ssem.at[i], recv_sem=rsem.at[i], device_id=other, device_id_type=pl.DeviceIdType.MESH) for i, (a, b) in enumerate(moves)]
    pl.semaphore_wait(barrier, 1)
    sends[0].start()
    sends[1].start()
    for cp in locs[:3]:
        cp.wait()
    slot = lax.broadcasted_iota(jnp.int32, iy_in.shape, 1)
    key_own[...] = jnp.where(slot < n_ref[0], (iy_in[...] - row_id * 256) * GRID + ix_in[...], -1000 * GRID)
    wx_bf[...] = wx_in[...].astype(BF)
    sends[2].start()
    sends[3].start()
    for cp in locs[3:]:
        cp.wait()
    payload(y_in, wy_in, wx_bf, key_own, pay)
    ranks(key_own, oh, rank)

    @pl.loop(0, SAMPLES // RUN // 2)
    def _(sp):
        reorder(sp, pay, rank, d_out)

    for cp in sends:
        cp.wait()


def sort_scratch():
    return [pltpu.VMEM((160, SAMPLES), BF), pltpu.VMEM((80 * (SAMPLES // RUN), RUN), BF), pltpu.VMEM((SAMPLES, 128), F32)]


def exchange(y, wy, wx, iy, ix, n):
    vm = pl.BlockSpec(memory_space=pltpu.VMEM)
    anym = pl.BlockSpec(memory_space=pl.ANY)
    dma = pltpu.SemaphoreType.DMA
    shape = jax.ShapeDtypeStruct
    return pl.pallas_call(
        exchange_kernel,
        out_shape=(shape(y.shape, F32), shape(wy.shape, F32), shape(wx.shape, BF), shape(iy.shape, jnp.int32), shape(iy.shape, jnp.int32), shape((SAMPLES // RUN, 160, RUN), BF)),
        in_specs=[anym] * 5 + [pl.BlockSpec(memory_space=pltpu.SMEM)],
        out_specs=(vm,) * 6,
        scratch_shapes=[pltpu.VMEM(v.shape, v.dtype) for v in (y, wy, wx, iy, ix)] + [pltpu.VMEM(wx.shape, BF)] + sort_scratch() + [dma((5,)), dma((4,)), dma((4,))],
        compiler_params=pltpu.CompilerParams(vmem_limit_bytes=12 * 2**20, collective_id=1, has_side_effects=True),
        cost_estimate=pl.CostEstimate(flops=10**9, bytes_accessed=10**6, transcendentals=0),
        name='exchange',
    )(y, wy, wx, iy, ix, n)


def spread_kernel(y_ref, wy_ref, wx_ref, key_ref, key_own, d_own, g_ref, e_ref, d_nb, pay, oh, rank, acc, *b_bufs):
    zero = jnp.zeros((16, RUN), BF)

    def product(d_ref, s, g0, right):
        rel = (d_ref[s, 128:144, :].astype(F32) - (g0 + 1).astype(F32)).astype(BF)
        left = []
        for q in range(2):
            e = [d_ref[s, 48 * q + 16 * j:48 * q + 16 * j + 16, :] for j in range(3)]
            for gi in range(WIN):
                m = [rel == jnp.array(gi - j, BF) for j in range(3)]
                left.append(jnp.where(m[0], e[0], jnp.where(m[1], e[1], jnp.where(m[2], e[2], zero))))
        return jnp.dot(jnp.concatenate(left, axis=0), right, preferred_element_type=F32)

    def add(g0, prod):
        rows = pl.ds(pl.multiple_of(g0 * 16, 16), 16 * WIN)
        for q in range(2):
            acc[q, rows, :] += prod[16 * WIN * q:16 * WIN * (q + 1)]

    def run_pair(d_ref, sp):
        first, last, prods = [], [], []
        for k in range(2):
            number = d_ref[2 * sp + k, 128:129, :].astype(F32)
            first.append(jnp.min(jnp.where(number > 0.0, number, 66.0)).astype(jnp.int32) - 1)
            last.append(jnp.max(number).astype(jnp.int32) + 1)
        for k in range(2):
            s = 2 * sp + k
            uc = d_ref[s, 144:160, :]
            eb = [d_ref[s, 96 + 16 * j:112 + 16 * j, :] for j in range(2)]
            right = jnp.concatenate([jnp.where(uc == jnp.array(g, BF), eb[0], jnp.where(uc == jnp.array((g - 1) % 64, BF), eb[1], zero)) for g in range(64)], axis=0)
            b_bufs[k][...] = right.T
        for k in range(2):
            prods.append(product(d_ref, 2 * sp + k, first[k], b_bufs[k][...]))
        for k in range(2):
            add(first[k], prods[k])
        for k in range(2):
            @pl.loop(1, (last[k] - first[k] + WIN) // WIN)
            def _(w):
                g0 = first[k] + WIN * w
                add(g0, product(d_ref, 2 * sp + k, g0, b_bufs[k][...]))

    def block(o, d_ref, n_runs):
        if o:
            acc[:, :1056] = jnp.zeros((2, 1056, GRID), F32)


        @pl.loop(0, (n_runs + 1) // 2)
        def _(sp):
            run_pair(d_ref, sp)

        for q in range(2):
            e_ref[o, q, 0:32] = acc[q, 0:32, :]
            e_ref[o, q, 32:64] = acc[q, 1024:1056, :]
            g_ref[o, :, GRID * q:GRID * (q + 1)] = acc[q, 16:1040, :].astype(BF)

    n_own, n_nb = [(jnp.sum(jnp.where(k[...] >= 0, 1.0, 0.0)).astype(jnp.int32) + (RUN - 1)) // RUN for k in (key_own, key_ref)]
    payload(y_ref, wy_ref, wx_ref, key_ref, pay, acc)
    acc[:, 704:1056] = jnp.zeros((2, 352, GRID), F32)
    ranks(key_ref, oh, rank)

    @pl.loop(0, (n_nb + 1) // 2)
    def _(sp):
        reorder(sp, pay, rank, d_nb)

    block(0, d_own, n_own)
    block(1, d_nb, n_nb)


def spread(y, wy, wx, key, key_own, d_own):
    vm = pl.BlockSpec(memory_space=pltpu.VMEM)
    return pl.pallas_call(
        spread_kernel,
        out_shape=(jax.ShapeDtypeStruct((2, 1024, 2 * GRID), BF), jax.ShapeDtypeStruct((2, 2, 64, GRID), F32)),
        in_specs=[vm] * 6,
        out_specs=(vm, vm),
        scratch_shapes=[pltpu.VMEM((SAMPLES // RUN, 160, RUN), BF)] + sort_scratch() + [
            pltpu.VMEM((2, 16 * (66 + WIN), GRID), F32),
            pltpu.VMEM((RUN, GRID), BF),
            pltpu.VMEM((RUN, GRID), BF),
        ],
        compiler_params=pltpu.CompilerParams(vmem_limit_bytes=28 * 2**20),
        cost_estimate=pl.CostEstimate(flops=13 * 10**9, bytes_accessed=4 * 2**20, transcendentals=0),
        name='spread',
    )(y, wy, wx, key, key_own, d_own)


def combine_kernel(gg, ee, tab, maps, dd, out_ref, hbuf, hs, ge, rx, s_all, part, near, far, scale,
                   esend, erecv, ssend, srecv, hsend, hrecv, ysend, yrecv, nsend, nrecv):
    row_id = lax.axis_index('rows')
    y_id = lax.axis_index('coil')
    core = row_id % 2
    x_id = row_id // 2
    sib_row = row_id + 1 - 2 * core
    sib = {'rows': sib_row}
    blocks = [row_id, (row_id + 2) % 4]

    barrier = pltpu.get_barrier_semaphore()
    for dev in (sib, {'coil': 1 - y_id}, {'coil': 1 - y_id, 'rows': sib_row}):
        pl.semaphore_signal(barrier, inc=1, device_id=dev, device_id_type=pl.DeviceIdType.MESH)

    def rows_of(a, c):
        return pl.ds(pl.multiple_of(256 * a + 128 * c, 128), 128)

    for a in range(2):
        s_all[core, a] = maps[:, :, rows_of(a, core), :]
    row_scale = jnp.broadcast_to(dd[:, pl.ds(pl.multiple_of(y_id * 256, 256), 256)], (128, 256)).T
    scale[...] = row_scale * dd[:, pl.ds(pl.multiple_of(row_id * 128, 128), 128)]
    pl.semaphore_wait(barrier, 3)

    def remote(src, dst, send, recv, dev):
        return pltpu.make_async_remote_copy(src_ref=src, dst_ref=dst, send_sem=send, recv_sem=recv, device_id=dev, device_id_type=pl.DeviceIdType.MESH)

    e_copies = []
    for o in range(2):
        low = o * core + (1 - o) * (1 - core)
        high = o * (1 - core) + (1 - o) * core
        for k, (slot, end, row0) in enumerate(((low, 1, 0), (high, 0, 48))):
            e_copies.append(remote(ee.at[o, :, pl.ds(row0, 16)], rx.at[slot, end], esend.at[2 * o + k], erecv.at[slot, end], sib))
    for cp in e_copies:
        cp.start()
    s_copies = [remote(maps.at[:, :, rows_of(a, 1 - core)], s_all.at[core, a], ssend.at[a], srecv.at[a], sib) for a in range(2)]
    for cp in s_copies:
        cp.start()

    def columns(hc, lhs):
        cols = pl.ds(pl.multiple_of(x_id * 256 + hc * 128, 128), 128)
        t2 = jnp.concatenate([tab[0, cols, :], tab[1, cols, :]], axis=0)
        prod = lax.dot_general(lhs, t2, NT, preferred_element_type=F32)
        n = lhs.shape[0] // 2
        return prod[:n, :128] - prod[n:, 128:], prod[:n, 128:] + prod[n:, :128]

    def transform(hc, o, k):
        for j in range(2):
            rows = slice(512 * k + 256 * j, 512 * k + 256 * j + 256)
            pair = columns(hc, jnp.concatenate([gg[o, rows, :GRID], gg[o, rows, GRID:]], axis=0))
            for e in range(2):
                hs[o, e, rows] = pair[e]

    def take_halos():
        for cp in e_copies:
            cp.wait_send()
        for o in range(2):
            for end in range(2):
                remote(rx.at[o, end], rx.at[o, end], esend.at[2 * o + end], erecv.at[o, end], sib).wait_recv()
                for q in range(2):
                    ge[64 * q + 32 * o + 16 * end:64 * q + 32 * o + 16 * end + 16, :] = (ee[o, q, 16 + 16 * end:32 + 16 * end, :] + rx[o, end, q]).astype(BF)

    def patch(hc):
        return columns(hc, ge[...])

    def piece(hc, o, k):
        return remote(hbuf.at[hc, blocks[o], :, pl.ds(128 * k, 128)], hbuf.at[hc, blocks[o], :, pl.ds(128 * k, 128)], hsend.at[hc, o, k], hrecv.at[hc, o, k], sib)

    h_copies = [[piece(hc, o, k) for o in range(2) for k in range(2)] for hc in range(2)]

    def send(hc, o, k, pair):
        for e in range(2):
            hs[o, e, 1008 * k:1008 * k + 16] = pair[e][32 * o + 16 * k:32 * o + 16 * k + 16]
            for c in range(4):
                hbuf[hc, blocks[o], e, 128 * k:128 * k + 128, 128 * c:128 * c + 128] = hs[o, e, pl.ds(512 * k + c, 128, stride=4), :].astype(BF)
        h_copies[hc][2 * o + k].start()

    def image(hc, a):
        rows = rows_of(a, core)
        cos, sin = tab[0, rows, :], tab[1, rows, :]
        quarter = [slice(256 * p, 256 * p + 256) for p in range(4)]
        top = jnp.concatenate([v[:, q] for q in quarter for v in (cos, -sin)], axis=1)
        bottom = jnp.concatenate([v[:, q] for q in quarter for v in (sin, cos)], axis=1)
        both = jnp.dot(jnp.concatenate([top, bottom], axis=0), hbuf[hc].reshape(2048, 512), preferred_element_type=F32)
        re, im = both[:128], both[128:]
        xr = jnp.zeros((128, 128), F32)
        xi = jnp.zeros((128, 128), F32)
        for c in range(4):
            ir = re[:, 128 * c:128 * c + 128]
            ii = im[:, 128 * c:128 * c + 128]
            sr = s_all[hc, a, 0, c]
            si = s_all[hc, a, 1, c]
            xr = xr + (sr * ir + si * ii)
            xi = xi + (sr * ii - si * ir)
        part[hc, a, 0] = xr
        part[hc, a, 1] = xi

    y_copies = [remote(part.at[hc, 1 - y_id], far.at[core], ysend.at[hc], yrecv.at[core], {'coil': 1 - y_id, 'rows': 2 * x_id + hc}) for hc in range(2)]
    n_copy = remote(part.at[1 - core, y_id], near, nsend.at[0], nrecv.at[0], sib)

    for k in range(2):
        transform(0, 0, k)
    take_halos()
    pair = patch(0)
    for k in range(2):
        send(0, 0, k, pair)
    for k in range(2):
        transform(0, 1, k)
        send(0, 1, k, pair)
    pair = patch(1)
    for k in range(2):
        transform(1, 0, k)
        send(1, 0, k, pair)
    for cp in s_copies + h_copies[0]:
        cp.wait()
    image(0, 1 - y_id)
    y_copies[0].start()
    for k in range(2):
        transform(1, 1, k)
        send(1, 1, k, pair)
    image(0, y_id)
    for cp in h_copies[1]:
        cp.wait()
    image(1, 1 - y_id)
    y_copies[1].start()
    image(1, y_id)
    n_copy.start()
    for cp in y_copies:
        cp.wait_send()
    n_copy.wait()
    mine = pl.ds(pl.multiple_of(128 * core, 128), 128)
    other = pl.ds(pl.multiple_of(128 * (1 - core), 128), 128)
    for e in range(2):
        out_ref[e, mine] = part[core, y_id, e]
        out_ref[e, other] = near[e]
    for k in range(2):
        remote(far.at[k], far.at[k], ysend.at[k], yrecv.at[k], {'coil': 1 - y_id}).wait_recv()
        sl = slice(128 * k, 128 * k + 128)
        for e in range(2):
            out_ref[e, sl] = (out_ref[e, sl] + far[k, e]) * scale[sl]


def combine(gg, ee, tab, maps, dd):
    vm = pl.BlockSpec(memory_space=pltpu.VMEM)
    dma = pltpu.SemaphoreType.DMA
    return pl.pallas_call(
        combine_kernel,
        out_shape=jax.ShapeDtypeStruct((2, 256, 128), F32),
        in_specs=[vm] * 5,
        out_specs=vm,
        scratch_shapes=[
            pltpu.VMEM((2, 4, 2, 256, 512), BF),
            pltpu.VMEM((2, 2, 1024, 128), F32),
            pltpu.VMEM((128, GRID), BF),
            pltpu.VMEM((2, 2, 2, 16, GRID), F32),
            pltpu.VMEM((2, 2, 2, 4, 128, 128), F32),
            pltpu.VMEM((2, 2, 2, 128, 128), F32),
            pltpu.VMEM((2, 128, 128), F32),
            pltpu.VMEM((2, 2, 128, 128), F32),
            pltpu.VMEM((256, 128), F32),
            dma((4,)), dma((2, 2)), dma((2,)), dma((2,)), dma((2, 2, 2)), dma((2, 2, 2)), dma((2,)), dma((2,)), dma((1,)), dma((1,)),
        ],
        compiler_params=pltpu.CompilerParams(vmem_limit_bytes=24 * 2**20, collective_id=0, has_side_effects=True),
        cost_estimate=pl.CostEstimate(flops=7 * 10**9, bytes_accessed=12 * 2**20, transcendentals=0),
        name='combine',
    )(gg, ee, tab, maps, dd)


def solution(mesh):
    def local_part(kspace, weight_row, weight_col, grid_row, grid_col, valid_count, coil_maps, deapod):
        n_img = deapod.shape[0]
        hbm = [pltpu.with_memory_space_constraint(v, pltpu.HBM) for v in (kspace, weight_row, weight_col, grid_row[None], grid_col[None])]
        stacked = exchange(*hbm, valid_count)
        tab = jnp.asarray(tables(n_img))
        gg, ee = spread(*stacked)
        return combine(gg, ee, tab, coil_maps, deapod[None])

    spec_samples = P(None, 'coil', ('slab', 'rows'))
    spec_weights = P(None, ('slab', 'rows'))
    spec_index = P(('slab', 'rows'))
    return jax.shard_map(local_part, mesh=mesh, in_specs=(spec_samples, spec_weights, spec_weights, spec_index, spec_index, spec_index, P(None, 'coil', 'slab', 'rows'), P()), out_specs=P(None, ('slab', 'coil'), 'rows'), check_vma=False)
```

```python
import math
import functools
import numpy as np
import jax
import jax.numpy as jnp
from jax import lax
from jax.experimental import pallas as pl
from jax.experimental.pallas import tpu as pltpu
from jax.sharding import PartitionSpec as P

F32 = jnp.float32
BF = jnp.bfloat16
NT = (((1,), (1,)), ((), ()))
KC = 512
GRID = 1024
SAMPLES = 2048
RUN = 256
WIN = 16


def tables(n_img):
    n_grid = 2 * n_img
    pix = np.arange(n_img) - n_img // 2
    freq = np.arange(n_grid) - n_img
    ang = np.mod(pix[:, None] * freq[None, :], n_grid) * (2.0 * math.pi / n_grid)
    return np.stack([np.cos(ang), np.sin(ang)]).astype(np.float32).astype(BF)


def payload(y_ref, wy_ref, wx_ref, key_ref, pay, clear=None):
    for s in range(SAMPLES // KC):
        cols = slice(s * KC, s * KC + KC)
        sub = lax.broadcasted_iota(jnp.int32, (16, KC), 0)
        if clear is not None:
            clear[:, 176 * s:176 * s + 176, :] = jnp.zeros((2, 176, GRID), F32)
        key = key_ref[:, cols]
        r0 = (key >> 10) + 1
        counted = r0 > 0
        t = jnp.where(counted, (sub >> 2) - (r0 & 3), 100)
        for q in range(2):
            y16 = jnp.zeros((16, KC), F32)
            for c in range(4):
                y16 = jnp.where((sub & 3) == c, y_ref[q, c:c + 1, cols], y16)
            coef = [y16 * wy_ref[a:a + 1, cols] for a in range(6)]
            for j in range(3):
                e = jnp.zeros((16, KC), F32)
                for a in range(6):
                    if -3 <= a - 4 * j <= 3:
                        e = jnp.where(t == a - 4 * j, coef[a], e)
                pay[48 * q + 16 * j:48 * q + 16 * j + 16, cols] = e.astype(BF)
        c0 = ((key & (GRID - 1)) + (GRID - 3)) & (GRID - 1)
        wx = wx_ref[:, cols].astype(F32)
        tc = jnp.where(counted, sub - (c0 & 15), 100)
        for j in range(2):
            e = jnp.zeros((16, KC), F32)
            for b in range(6):
                e = jnp.where(tc == b - 16 * j, wx[b:b + 1], e)
            pay[96 + 16 * j:112 + 16 * j, cols] = e.astype(BF)
        pay[128:144, cols] = jnp.broadcast_to(((r0 >> 2) + 1).astype(F32), (16, KC)).astype(BF)
        pay[144:160, cols] = jnp.broadcast_to((c0 >> 4).astype(F32), (16, KC)).astype(BF)


def iota16():
    return lax.broadcasted_iota(jnp.int32, (16, 1), 0).astype(F32)


def tiles(ch):
    first = 4 * (ch // 2) + ch % 2
    return first, first + 2


def ranks(key_ref, oh, rank):
    n_chunk = SAMPLES // RUN
    one, zero = jnp.ones((), BF), jnp.zeros((), BF)
    for ch in range(n_chunk):
        for k, t in enumerate(tiles(ch)):
            bucket = jnp.broadcast_to((((key_ref[:, 128 * t:128 * t + 128] >> 10) + 1) >> 2).astype(F32), (16, 128)).astype(BF)
            for g in range(5):
                oh[80 * ch + 16 * g:80 * ch + 16 * g + 16, 128 * k:128 * k + 128] = jnp.where(bucket == (iota16() + 16 * g).astype(BF), one, zero)
    lower = lax.broadcasted_iota(jnp.int32, (RUN, RUN + 128), 0)
    upper = lax.broadcasted_iota(jnp.int32, (RUN, RUN + 128), 1)
    tri = jnp.where((lower < upper) | (upper >= RUN), 1.0, 0.0).astype(BF)
    pre = jnp.dot(oh[...], tri, preferred_element_type=F32)
    counts = [pre[80 * ch:80 * ch + 80, RUN:] for ch in range(n_chunk)]
    strict = jnp.where(lax.broadcasted_iota(jnp.int32, (80, 80), 1) < lax.broadcasted_iota(jnp.int32, (80, 80), 0), 1.0, 0.0).astype(BF)
    for h in range(2):
        total = counts[h]
        for ch in range(h + 2, n_chunk, 2):
            total = total + counts[ch]
        high = jnp.floor(total * (1.0 / 256.0))
        low = total - 256.0 * high
        base = 256.0 * jnp.dot(strict, high.astype(BF), preferred_element_type=F32) + jnp.dot(strict, low.astype(BF), preferred_element_type=F32)
        for ch in range(h, n_chunk, 2):
            for k, t in enumerate(tiles(ch)):
                place = pre[80 * ch:80 * ch + 80, 128 * k:128 * k + 128] + base
                place = jnp.sum(oh[80 * ch:80 * ch + 80, 128 * k:128 * k + 128].astype(F32) * place, axis=0, keepdims=True)
                place = jnp.where(key_ref[:, 128 * t:128 * t + 128] >= 0, place, -1.0)
                rank[128 * t:128 * t + 128, :] = jnp.broadcast_to(place, (128, 128)).T
            base = base + counts[ch]


def reorder(sp, pay, rank, d_ref):
    lane = lax.broadcasted_iota(jnp.int32, (1, 128), 1).astype(F32)
    one, zero = jnp.ones((), BF), jnp.zeros((), BF)
    for h in range(2):
        total = None
        for ch in range(h, SAMPLES // RUN, 2):
            rows = []
            for t in tiles(ch):
                place = (rank[128 * t:128 * t + 128, :] - (sp * 256).astype(F32)).astype(BF)
                rows.append(jnp.concatenate([jnp.where(place == (lane + 128 * k).astype(BF), one, zero) for k in range(2)], axis=1))
            block = jnp.concatenate(rows, axis=0)
            values = jnp.concatenate([pay[:, 128 * t:128 * t + 128] for t in tiles(ch)], axis=1)
            part = jnp.dot(values, block, preferred_element_type=F32)
            total = part if total is None else total + part
        total = total.astype(BF)
        for k in range(2):
            d_ref[2 * sp + k, :, 128 * h:128 * h + 128] = total[:, 128 * k:128 * k + 128]


def exchange_kernel(y_ref, wy_ref, wx_ref, iy_ref, ix_ref, n_ref, y_out, wy_out, wx_out, key_out, key_own, d_out,
                    y_in, wy_in, wx_in, iy_in, ix_in, wx_bf, pay, oh, rank, loc, ssem, rsem):
    row_id = lax.axis_index('rows')
    other = {'rows': (row_id + 2) % 4}
    barrier = pltpu.get_barrier_semaphore()
    pl.semaphore_signal(barrier, inc=1, device_id=other, device_id_type=pl.DeviceIdType.MESH)
    pairs = [(iy_ref, iy_in), (ix_ref, ix_in), (wx_ref, wx_in), (wy_ref, wy_in), (y_ref, y_in)]
    locs = [pltpu.make_async_copy(a, b, loc.at[i]) for i, (a, b) in enumerate(pairs)]
    for cp in locs:
        cp.start()
    moves = [(y_ref, y_out), (wy_ref, wy_out), (key_own, key_out), (wx_bf, wx_out)]
    sends = [pltpu.make_async_remote_copy(src_ref=a, dst_ref=b, send_sem=ssem.at[i], recv_sem=rsem.at[i], device_id=other, device_id_type=pl.DeviceIdType.MESH) for i, (a, b) in enumerate(moves)]
    pl.semaphore_wait(barrier, 1)
    sends[0].start()
    sends[1].start()
    for cp in locs[:3]:
        cp.wait()
    slot = lax.broadcasted_iota(jnp.int32, iy_in.shape, 1)
    key_own[...] = jnp.where(slot < n_ref[0], (iy_in[...] - row_id * 256) * GRID + ix_in[...], -1000 * GRID)
    wx_bf[...] = wx_in[...].astype(BF)
    sends[2].start()
    sends[3].start()
    for cp in locs[3:]:
        cp.wait()
    payload(y_in, wy_in, wx_bf, key_own, pay)
    ranks(key_own, oh, rank)

    @pl.loop(0, SAMPLES // RUN // 2)
    def _(sp):
        reorder(sp, pay, rank, d_out)

    for cp in sends:
        cp.wait()


def sort_scratch():
    return [pltpu.VMEM((160, SAMPLES), BF), pltpu.VMEM((80 * (SAMPLES // RUN), RUN), BF), pltpu.VMEM((SAMPLES, 128), F32)]


def exchange(y, wy, wx, iy, ix, n):
    vm = pl.BlockSpec(memory_space=pltpu.VMEM)
    anym = pl.BlockSpec(memory_space=pl.ANY)
    dma = pltpu.SemaphoreType.DMA
    shape = jax.ShapeDtypeStruct
    return pl.pallas_call(
        exchange_kernel,
        out_shape=(shape(y.shape, F32), shape(wy.shape, F32), shape(wx.shape, BF), shape(iy.shape, jnp.int32), shape(iy.shape, jnp.int32), shape((SAMPLES // RUN, 160, RUN), BF)),
        in_specs=[anym] * 5 + [pl.BlockSpec(memory_space=pltpu.SMEM)],
        out_specs=(vm,) * 6,
        scratch_shapes=[pltpu.VMEM(v.shape, v.dtype) for v in (y, wy, wx, iy, ix)] + [pltpu.VMEM(wx.shape, BF)] + sort_scratch() + [dma((5,)), dma((4,)), dma((4,))],
        compiler_params=pltpu.CompilerParams(vmem_limit_bytes=12 * 2**20, collective_id=1, has_side_effects=True),
        cost_estimate=pl.CostEstimate(flops=10**9, bytes_accessed=10**6, transcendentals=0),
        name='exchange',
    )(y, wy, wx, iy, ix, n)


def spread_kernel(y_ref, wy_ref, wx_ref, key_ref, key_own, d_own, g_ref, e_ref, d_nb, pay, oh, rank, acc, *b_bufs):
    zero = jnp.zeros((16, RUN), BF)

    def product(d_ref, s, g0, right):
        rel = (d_ref[s, 128:144, :].astype(F32) - (g0 + 1).astype(F32)).astype(BF)
        left = []
        for q in range(2):
            e = [d_ref[s, 48 * q + 16 * j:48 * q + 16 * j + 16, :] for j in range(3)]
            for gi in range(WIN):
                m = [rel == jnp.array(gi - j, BF) for j in range(3)]
                left.append(jnp.where(m[0], e[0], jnp.where(m[1], e[1], jnp.where(m[2], e[2], zero))))
        return jnp.dot(jnp.concatenate(left, axis=0), right, preferred_element_type=F32)

    def add(g0, prod):
        rows = pl.ds(pl.multiple_of(g0 * 16, 16), 16 * WIN)
        for q in range(2):
            acc[q, rows, :] += prod[16 * WIN * q:16 * WIN * (q + 1)]

    def run_pair(d_ref, sp):
        first, last, prods = [], [], []
        for k in range(2):
            number = d_ref[2 * sp + k, 128:129, :].astype(F32)
            first.append(jnp.min(jnp.where(number > 0.0, number, 66.0)).astype(jnp.int32) - 1)
            last.append(jnp.max(number).astype(jnp.int32) + 1)
        for k in range(2):
            s = 2 * sp + k
            uc = d_ref[s, 144:160, :]
            eb = [d_ref[s, 96 + 16 * j:112 + 16 * j, :] for j in range(2)]
            right = jnp.concatenate([jnp.where(uc == jnp.array(g, BF), eb[0], jnp.where(uc == jnp.array((g - 1) % 64, BF), eb[1], zero)) for g in range(64)], axis=0)
            b_bufs[k][...] = right.T
        for k in range(2):
            prods.append(product(d_ref, 2 * sp + k, first[k], b_bufs[k][...]))
        for k in range(2):
            add(first[k], prods[k])
        for k in range(2):
            @pl.loop(1, (last[k] - first[k] + WIN) // WIN)
            def _(w):
                g0 = first[k] + WIN * w
                add(g0, product(d_ref, 2 * sp + k, g0, b_bufs[k][...]))

    def block(o, d_ref, n_runs):
        if o:
            acc[:, :1056] = jnp.zeros((2, 1056, GRID), F32)


        @pl.loop(0, (n_runs + 1) // 2)
        def _(sp):
            run_pair(d_ref, sp)

        for q in range(2):
            e_ref[o, q, 0:32] = acc[q, 0:32, :]
            e_ref[o, q, 32:64] = acc[q, 1024:1056, :]
            g_ref[o, :, GRID * q:GRID * (q + 1)] = acc[q, 16:1040, :].astype(BF)

    n_own, n_nb = [(jnp.sum(jnp.where(k[...] >= 0, 1.0, 0.0)).astype(jnp.int32) + (RUN - 1)) // RUN for k in (key_own, key_ref)]
    payload(y_ref, wy_ref, wx_ref, key_ref, pay, acc)
    acc[:, 704:1056] = jnp.zeros((2, 352, GRID), F32)
    ranks(key_ref, oh, rank)

    @pl.loop(0, (n_nb + 1) // 2)
    def _(sp):
        reorder(sp, pay, rank, d_nb)

    block(0, d_own, n_own)
    block(1, d_nb, n_nb)


def spread(y, wy, wx, key, key_own, d_own):
    vm = pl.BlockSpec(memory_space=pltpu.VMEM)
    return pl.pallas_call(
        spread_kernel,
        out_shape=(jax.ShapeDtypeStruct((2, 1024, 2 * GRID), BF), jax.ShapeDtypeStruct((2, 2, 64, GRID), F32)),
        in_specs=[vm] * 6,
        out_specs=(vm, vm),
        scratch_shapes=[pltpu.VMEM((SAMPLES // RUN, 160, RUN), BF)] + sort_scratch() + [
            pltpu.VMEM((2, 16 * (66 + WIN), GRID), F32),
            pltpu.VMEM((RUN, GRID), BF),
            pltpu.VMEM((RUN, GRID), BF),
        ],
        compiler_params=pltpu.CompilerParams(vmem_limit_bytes=28 * 2**20),
        cost_estimate=pl.CostEstimate(flops=13 * 10**9, bytes_accessed=4 * 2**20, transcendentals=0),
        name='spread',
    )(y, wy, wx, key, key_own, d_own)


def combine_kernel(gg, ee, tab, maps, dd, out_ref, hbuf, hs, ge, rx, s_all, part, near, far, scale, table,
                   esend, erecv, ssend, srecv, hsend, hrecv, ysend, yrecv, nsend, nrecv):
    row_id = lax.axis_index('rows')
    y_id = lax.axis_index('coil')
    core = row_id % 2
    x_id = row_id // 2
    sib_row = row_id + 1 - 2 * core
    sib = {'rows': sib_row}
    blocks = [row_id, (row_id + 2) % 4]

    barrier = pltpu.get_barrier_semaphore()
    for dev in (sib, {'coil': 1 - y_id}, {'coil': 1 - y_id, 'rows': sib_row}):
        pl.semaphore_signal(barrier, inc=1, device_id=dev, device_id_type=pl.DeviceIdType.MESH)

    def rows_of(a, c):
        return pl.ds(pl.multiple_of(256 * a + 128 * c, 128), 128)

    for a in range(2):
        s_all[core, a] = maps[:, :, rows_of(a, core), :]
    row_scale = jnp.broadcast_to(dd[:, pl.ds(pl.multiple_of(y_id * 256, 256), 256)], (128, 256)).T
    scale[...] = row_scale * dd[:, pl.ds(pl.multiple_of(row_id * 128, 128), 128)]
    pl.semaphore_wait(barrier, 3)

    def remote(src, dst, send, recv, dev):
        return pltpu.make_async_remote_copy(src_ref=src, dst_ref=dst, send_sem=send, recv_sem=recv, device_id=dev, device_id_type=pl.DeviceIdType.MESH)

    e_copies = []
    for o in range(2):
        low = o * core + (1 - o) * (1 - core)
        high = o * (1 - core) + (1 - o) * core
        for k, (slot, end, row0) in enumerate(((low, 1, 0), (high, 0, 48))):
            e_copies.append(remote(ee.at[o, :, pl.ds(row0, 16)], rx.at[slot, end], esend.at[2 * o + k], erecv.at[slot, end], sib))
    for cp in e_copies:
        cp.start()
    s_copies = [remote(maps.at[:, :, rows_of(a, 1 - core)], s_all.at[core, a], ssend.at[a], srecv.at[a], sib) for a in range(2)]
    for cp in s_copies:
        cp.start()
    for hc in range(2):
        cols = pl.ds(pl.multiple_of(x_id * 256 + hc * 128, 128), 128)
        table[hc] = jnp.concatenate([tab[0, cols, :], tab[1, cols, :]], axis=0).T

    def columns(hc, lhs):
        t2 = table[hc]
        prod = jnp.dot(lhs, t2, preferred_element_type=F32)
        n = lhs.shape[0] // 2
        return prod[:n, :128] - prod[n:, 128:], prod[:n, 128:] + prod[n:, :128]

    def transform(hc, o, k):
        for j in range(2):
            rows = slice(512 * k + 256 * j, 512 * k + 256 * j + 256)
            pair = columns(hc, jnp.concatenate([gg[o, rows, :GRID], gg[o, rows, GRID:]], axis=0))
            for e in range(2):
                hs[o, e, rows] = pair[e]

    def take_halos():
        for cp in e_copies:
            cp.wait_send()
        for o in range(2):
            for end in range(2):
                remote(rx.at[o, end], rx.at[o, end], esend.at[2 * o + end], erecv.at[o, end], sib).wait_recv()
                for q in range(2):
                    ge[64 * q + 32 * o + 16 * end:64 * q + 32 * o + 16 * end + 16, :] = (ee[o, q, 16 + 16 * end:32 + 16 * end, :] + rx[o, end, q]).astype(BF)

    def patch(hc):
        return columns(hc, ge[...])

    def piece(hc, o, k):
        return remote(hbuf.at[hc, blocks[o], :, pl.ds(128 * k, 128)], hbuf.at[hc, blocks[o], :, pl.ds(128 * k, 128)], hsend.at[hc, o, k], hrecv.at[hc, o, k], sib)

    h_copies = [[piece(hc, o, k) for o in range(2) for k in range(2)] for hc in range(2)]

    def send(hc, o, k, pair):
        for e in range(2):
            hs[o, e, 1008 * k:1008 * k + 16] = pair[e][32 * o + 16 * k:32 * o + 16 * k + 16]
            for c in range(4):
                hbuf[hc, blocks[o], e, 128 * k:128 * k + 128, 128 * c:128 * c + 128] = hs[o, e, pl.ds(512 * k + c, 128, stride=4), :].astype(BF)
        h_copies[hc][2 * o + k].start()

    def image(hc, a):
        rows = rows_of(a, core)
        cos, sin = tab[0, rows, :], tab[1, rows, :]
        quarter = [slice(256 * p, 256 * p + 256) for p in range(4)]
        top = jnp.concatenate([v[:, q] for q in quarter for v in (cos, -sin)], axis=1)
        bottom = jnp.concatenate([v[:, q] for q in quarter for v in (sin, cos)], axis=1)
        both = jnp.dot(jnp.concatenate([top, bottom], axis=0), hbuf[hc].reshape(2048, 512), preferred_element_type=F32)
        re, im = both[:128], both[128:]
        xr = jnp.zeros((128, 128), F32)
        xi = jnp.zeros((128, 128), F32)
        for c in range(4):
            ir = re[:, 128 * c:128 * c + 128]
            ii = im[:, 128 * c:128 * c + 128]
            sr = s_all[hc, a, 0, c]
            si = s_all[hc, a, 1, c]
            xr = xr + (sr * ir + si * ii)
            xi = xi + (sr * ii - si * ir)
        part[hc, a, 0] = xr
        part[hc, a, 1] = xi

    y_copies = [remote(part.at[hc, 1 - y_id], far.at[core], ysend.at[hc], yrecv.at[core], {'coil': 1 - y_id, 'rows': 2 * x_id + hc}) for hc in range(2)]
    n_copy = remote(part.at[1 - core, y_id], near, nsend.at[0], nrecv.at[0], sib)

    for k in range(2):
        transform(0, 0, k)
    take_halos()
    pair = patch(0)
    for k in range(2):
        send(0, 0, k, pair)
    for k in range(2):
        transform(0, 1, k)
        send(0, 1, k, pair)
    pair = patch(1)
    for k in range(2):
        transform(1, 0, k)
        send(1, 0, k, pair)
    for cp in s_copies + h_copies[0]:
        cp.wait()
    image(0, 1 - y_id)
    y_copies[0].start()
    for k in range(2):
        transform(1, 1, k)
        send(1, 1, k, pair)
    image(0, y_id)
    for cp in h_copies[1]:
        cp.wait()
    image(1, 1 - y_id)
    y_copies[1].start()
    image(1, y_id)
    n_copy.start()
    for cp in y_copies:
        cp.wait_send()
    n_copy.wait()
    mine = pl.ds(pl.multiple_of(128 * core, 128), 128)
    other = pl.ds(pl.multiple_of(128 * (1 - core), 128), 128)
    for e in range(2):
        out_ref[e, mine] = part[core, y_id, e]
        out_ref[e, other] = near[e]
    for k in range(2):
        remote(far.at[k], far.at[k], ysend.at[k], yrecv.at[k], {'coil': 1 - y_id}).wait_recv()
        sl = slice(128 * k, 128 * k + 128)
        for e in range(2):
            out_ref[e, sl] = (out_ref[e, sl] + far[k, e]) * scale[sl]


def combine(gg, ee, tab, maps, dd):
    vm = pl.BlockSpec(memory_space=pltpu.VMEM)
    dma = pltpu.SemaphoreType.DMA
    return pl.pallas_call(
        combine_kernel,
        out_shape=jax.ShapeDtypeStruct((2, 256, 128), F32),
        in_specs=[vm] * 5,
        out_specs=vm,
        scratch_shapes=[
            pltpu.VMEM((2, 4, 2, 256, 512), BF),
            pltpu.VMEM((2, 2, 1024, 128), F32),
            pltpu.VMEM((128, GRID), BF),
            pltpu.VMEM((2, 2, 2, 16, GRID), F32),
            pltpu.VMEM((2, 2, 2, 4, 128, 128), F32),
            pltpu.VMEM((2, 2, 2, 128, 128), F32),
            pltpu.VMEM((2, 128, 128), F32),
            pltpu.VMEM((2, 2, 128, 128), F32),
            pltpu.VMEM((256, 128), F32),
            pltpu.VMEM((2, GRID, 256), BF),
            dma((4,)), dma((2, 2)), dma((2,)), dma((2,)), dma((2, 2, 2)), dma((2, 2, 2)), dma((2,)), dma((2,)), dma((1,)), dma((1,)),
        ],
        compiler_params=pltpu.CompilerParams(vmem_limit_bytes=24 * 2**20, collective_id=0, has_side_effects=True),
        cost_estimate=pl.CostEstimate(flops=7 * 10**9, bytes_accessed=12 * 2**20, transcendentals=0),
        name='combine',
    )(gg, ee, tab, maps, dd)


def solution(mesh):
    def local_part(kspace, weight_row, weight_col, grid_row, grid_col, valid_count, coil_maps, deapod):
        n_img = deapod.shape[0]
        hbm = [pltpu.with_memory_space_constraint(v, pltpu.HBM) for v in (kspace, weight_row, weight_col, grid_row[None], grid_col[None])]
        stacked = exchange(*hbm, valid_count)
        tab = jnp.asarray(tables(n_img))
        gg, ee = spread(*stacked)
        return combine(gg, ee, tab, coil_maps, deapod[None])

    spec_samples = P(None, 'coil', ('slab', 'rows'))
    spec_weights = P(None, ('slab', 'rows'))
    spec_index = P(('slab', 'rows'))
    return jax.shard_map(local_part, mesh=mesh, in_specs=(spec_samples, spec_weights, spec_weights, spec_index, spec_index, spec_index, P(None, 'coil', 'slab', 'rows'), P()), out_specs=P(None, ('slab', 'coil'), 'rows'), check_vma=False)
```

```python
import math
import functools
import numpy as np
import jax
import jax.numpy as jnp
from jax import lax
from jax.experimental import pallas as pl
from jax.experimental.pallas import tpu as pltpu
from jax.sharding import PartitionSpec as P

F32 = jnp.float32
BF = jnp.bfloat16
NT = (((1,), (1,)), ((), ()))
KC = 512
GRID = 1024
SAMPLES = 2048
RUN = 256
WIN = 16


def tables(n_img):
    n_grid = 2 * n_img
    pix = np.arange(n_img) - n_img // 2
    freq = np.arange(n_grid) - n_img
    ang = np.mod(pix[:, None] * freq[None, :], n_grid) * (2.0 * math.pi / n_grid)
    return np.stack([np.cos(ang), np.sin(ang)]).astype(np.float32).astype(BF)


def payload(y_ref, wy_ref, wx_ref, key_ref, pay, clear=None):
    for s in range(SAMPLES // KC):
        cols = slice(s * KC, s * KC + KC)
        sub = lax.broadcasted_iota(jnp.int32, (16, KC), 0)
        if clear is not None:
            clear[:, 176 * s:176 * s + 176, :] = jnp.zeros((2, 176, GRID), F32)
        key = key_ref[:, cols]
        r0 = (key >> 10) + 1
        counted = r0 > 0
        t = jnp.where(counted, (sub >> 2) - (r0 & 3), 100)
        for q in range(2):
            y16 = jnp.zeros((16, KC), F32)
            for c in range(4):
                y16 = jnp.where((sub & 3) == c, y_ref[q, c:c + 1, cols], y16)
            coef = [y16 * wy_ref[a:a + 1, cols] for a in range(6)]
            for j in range(3):
                e = jnp.zeros((16, KC), F32)
                for a in range(6):
                    if -3 <= a - 4 * j <= 3:
                        e = jnp.where(t == a - 4 * j, coef[a], e)
                pay[48 * q + 16 * j:48 * q + 16 * j + 16, cols] = e.astype(BF)
        c0 = ((key & (GRID - 1)) + (GRID - 3)) & (GRID - 1)
        wx = wx_ref[:, cols].astype(F32)
        tc = jnp.where(counted, sub - (c0 & 15), 100)
        for j in range(2):
            e = jnp.zeros((16, KC), F32)
            for b in range(6):
                e = jnp.where(tc == b - 16 * j, wx[b:b + 1], e)
            pay[96 + 16 * j:112 + 16 * j, cols] = e.astype(BF)
        pay[128:144, cols] = jnp.broadcast_to(((r0 >> 2) + 1).astype(F32), (16, KC)).astype(BF)
        pay[144:160, cols] = jnp.broadcast_to((c0 >> 4).astype(F32), (16, KC)).astype(BF)


def iota16():
    return lax.broadcasted_iota(jnp.int32, (16, 1), 0).astype(F32)


def tiles(ch):
    first = 4 * (ch // 2) + ch % 2
    return first, first + 2


def ranks(key_ref, oh, rank):
    n_chunk = SAMPLES // RUN
    one, zero = jnp.ones((), BF), jnp.zeros((), BF)
    for ch in range(n_chunk):
        for k, t in enumerate(tiles(ch)):
            bucket = jnp.broadcast_to((((key_ref[:, 128 * t:128 * t + 128] >> 10) + 1) >> 2).astype(F32), (16, 128)).astype(BF)
            for g in range(5):
                oh[80 * ch + 16 * g:80 * ch + 16 * g + 16, 128 * k:128 * k + 128] = jnp.where(bucket == (iota16() + 16 * g).astype(BF), one, zero)
    lower = lax.broadcasted_iota(jnp.int32, (RUN, RUN + 128), 0)
    upper = lax.broadcasted_iota(jnp.int32, (RUN, RUN + 128), 1)
    tri = jnp.where((lower < upper) | (upper >= RUN), 1.0, 0.0).astype(BF)
    pre = jnp.dot(oh[...], tri, preferred_element_type=F32)
    counts = [pre[80 * ch:80 * ch + 80, RUN:] for ch in range(n_chunk)]
    strict = jnp.where(lax.broadcasted_iota(jnp.int32, (80, 80), 1) < lax.broadcasted_iota(jnp.int32, (80, 80), 0), 1.0, 0.0).astype(BF)
    for h in range(2):
        total = counts[h]
        for ch in range(h + 2, n_chunk, 2):
            total = total + counts[ch]
        high = jnp.floor(total * (1.0 / 256.0))
        low = total - 256.0 * high
        base = 256.0 * jnp.dot(strict, high.astype(BF), preferred_element_type=F32) + jnp.dot(strict, low.astype(BF), preferred_element_type=F32)
        for ch in range(h, n_chunk, 2):
            for k, t in enumerate(tiles(ch)):
                place = pre[80 * ch:80 * ch + 80, 128 * k:128 * k + 128] + base
                place = jnp.sum(oh[80 * ch:80 * ch + 80, 128 * k:128 * k + 128].astype(F32) * place, axis=0, keepdims=True)
                place = jnp.where(key_ref[:, 128 * t:128 * t + 128] >= 0, place, -1.0)
                rank[128 * t:128 * t + 128, :] = jnp.broadcast_to(place, (128, 128)).T
            base = base + counts[ch]


def reorder(sp, pay, rank, d_ref):
    lane = lax.broadcasted_iota(jnp.int32, (1, 128), 1).astype(F32)
    one, zero = jnp.ones((), BF), jnp.zeros((), BF)
    for h in range(2):
        total = None
        for ch in range(h, SAMPLES // RUN, 2):
            rows = []
            for t in tiles(ch):
                place = (rank[128 * t:128 * t + 128, :] - (sp * 256).astype(F32)).astype(BF)
                rows.append(jnp.concatenate([jnp.where(place == (lane + 128 * k).astype(BF), one, zero) for k in range(2)], axis=1))
            block = jnp.concatenate(rows, axis=0)
            values = jnp.concatenate([pay[:, 128 * t:128 * t + 128] for t in tiles(ch)], axis=1)
            part = jnp.dot(values, block, preferred_element_type=F32)
            total = part if total is None else total + part
        total = total.astype(BF)
        for k in range(2):
            d_ref[2 * sp + k, :, 128 * h:128 * h + 128] = total[:, 128 * k:128 * k + 128]


def exchange_kernel(y_ref, wy_ref, wx_ref, iy_ref, ix_ref, n_ref, y_out, wy_out, wx_out, key_out, key_own, d_out,
                    y_in, wy_in, wx_in, iy_in, ix_in, wx_bf, pay, oh, rank, loc, ssem, rsem):
    row_id = lax.axis_index('rows')
    other = {'rows': (row_id + 2) % 4}
    barrier = pltpu.get_barrier_semaphore()
    pl.semaphore_signal(barrier, inc=1, device_id=other, device_id_type=pl.DeviceIdType.MESH)
    pairs = [(iy_ref, iy_in), (ix_ref, ix_in), (wx_ref, wx_in), (wy_ref, wy_in), (y_ref, y_in)]
    locs = [pltpu.make_async_copy(a, b, loc.at[i]) for i, (a, b) in enumerate(pairs)]
    for cp in locs:
        cp.start()
    moves = [(y_ref, y_out), (wy_ref, wy_out), (key_own, key_out), (wx_bf, wx_out)]
    sends = [pltpu.make_async_remote_copy(src_ref=a, dst_ref=b, send_sem=ssem.at[i], recv_sem=rsem.at[i], device_id=other, device_id_type=pl.DeviceIdType.MESH) for i, (a, b) in enumerate(moves)]
    pl.semaphore_wait(barrier, 1)
    sends[0].start()
    sends[1].start()
    for cp in locs[:3]:
        cp.wait()
    slot = lax.broadcasted_iota(jnp.int32, iy_in.shape, 1)
    key_own[...] = jnp.where(slot < n_ref[0], (iy_in[...] - row_id * 256) * GRID + ix_in[...], -1000 * GRID)
    wx_bf[...] = wx_in[...].astype(BF)
    sends[2].start()
    sends[3].start()
    for cp in locs[3:]:
        cp.wait()
    payload(y_in, wy_in, wx_bf, key_own, pay)
    ranks(key_own, oh, rank)

    @pl.loop(0, SAMPLES // RUN // 2)
    def _(sp):
        reorder(sp, pay, rank, d_out)

    for cp in sends:
        cp.wait()


def sort_scratch():
    return [pltpu.VMEM((160, SAMPLES), BF), pltpu.VMEM((80 * (SAMPLES // RUN), RUN), BF), pltpu.VMEM((SAMPLES, 128), F32)]


def exchange(y, wy, wx, iy, ix, n):
    vm = pl.BlockSpec(memory_space=pltpu.VMEM)
    anym = pl.BlockSpec(memory_space=pl.ANY)
    dma = pltpu.SemaphoreType.DMA
    shape = jax.ShapeDtypeStruct
    return pl.pallas_call(
        exchange_kernel,
        out_shape=(shape(y.shape, F32), shape(wy.shape, F32), shape(wx.shape, BF), shape(iy.shape, jnp.int32), shape(iy.shape, jnp.int32), shape((SAMPLES // RUN, 160, RUN), BF)),
        in_specs=[anym] * 5 + [pl.BlockSpec(memory_space=pltpu.SMEM)],
        out_specs=(vm,) * 6,
        scratch_shapes=[pltpu.VMEM(v.shape, v.dtype) for v in (y, wy, wx, iy, ix)] + [pltpu.VMEM(wx.shape, BF)] + sort_scratch() + [dma((5,)), dma((4,)), dma((4,))],
        compiler_params=pltpu.CompilerParams(vmem_limit_bytes=12 * 2**20, collective_id=1, has_side_effects=True),
        cost_estimate=pl.CostEstimate(flops=10**9, bytes_accessed=10**6, transcendentals=0),
        name='exchange',
    )(y, wy, wx, iy, ix, n)


def spread_kernel(y_ref, wy_ref, wx_ref, key_ref, key_own, d_own, g_ref, e_ref, d_nb, pay, oh, rank, acc, *b_bufs):
    zero = jnp.zeros((16, RUN), BF)

    def product(d_ref, s, g0, right):
        rel = (d_ref[s, 128:144, :].astype(F32) - (g0 + 1).astype(F32)).astype(BF)
        left = []
        for q in range(2):
            e = [d_ref[s, 48 * q + 16 * j:48 * q + 16 * j + 16, :] for j in range(3)]
            for gi in range(WIN):
                m = [rel == jnp.array(gi - j, BF) for j in range(3)]
                left.append(jnp.where(m[0], e[0], jnp.where(m[1], e[1], jnp.where(m[2], e[2], zero))))
        return jnp.dot(jnp.concatenate(left, axis=0), right, preferred_element_type=F32)

    def add(g0, prod):
        rows = pl.ds(pl.multiple_of(g0 * 16, 16), 16 * WIN)
        for q in range(2):
            acc[q, rows, :] += prod[16 * WIN * q:16 * WIN * (q + 1)]

    def run_pair(d_ref, sp):
        first, last, prods = [], [], []
        for k in range(2):
            number = d_ref[2 * sp + k, 128:129, :].astype(F32)
            first.append(jnp.min(jnp.where(number > 0.0, number, 66.0)).astype(jnp.int32) - 1)
            last.append(jnp.max(number).astype(jnp.int32) + 1)
        for k in range(2):
            s = 2 * sp + k
            uc = d_ref[s, 144:160, :]
            eb = [d_ref[s, 96 + 16 * j:112 + 16 * j, :] for j in range(2)]
            right = jnp.concatenate([jnp.where(uc == jnp.array(g, BF), eb[0], jnp.where(uc == jnp.array((g - 1) % 64, BF), eb[1], zero)) for g in range(64)], axis=0)
            b_bufs[k][...] = right.T
        for k in range(2):
            prods.append(product(d_ref, 2 * sp + k, first[k], b_bufs[k][...]))
        for k in range(2):
            add(first[k], prods[k])
        for k in range(2):
            @pl.loop(1, (last[k] - first[k] + WIN) // WIN)
            def _(w):
                g0 = first[k] + WIN * w
                add(g0, product(d_ref, 2 * sp + k, g0, b_bufs[k][...]))

    def block(o, d_ref, n_runs):
        if o:
            acc[:, :1056] = jnp.zeros((2, 1056, GRID), F32)


        @pl.loop(0, (n_runs + 1) // 2)
        def _(sp):
            run_pair(d_ref, sp)

        for q in range(2):
            e_ref[o, q, 0:32] = acc[q, 0:32, :]
            e_ref[o, q, 32:64] = acc[q, 1024:1056, :]
            g_ref[o, :, GRID * q:GRID * (q + 1)] = acc[q, 16:1040, :].astype(BF)

    n_own, n_nb = [(jnp.sum(jnp.where(k[...] >= 0, 1.0, 0.0)).astype(jnp.int32) + (RUN - 1)) // RUN for k in (key_own, key_ref)]
    payload(y_ref, wy_ref, wx_ref, key_ref, pay, acc)
    acc[:, 704:1056] = jnp.zeros((2, 352, GRID), F32)
    ranks(key_ref, oh, rank)

    @pl.loop(0, (n_nb + 1) // 2)
    def _(sp):
        reorder(sp, pay, rank, d_nb)

    block(0, d_own, n_own)
    block(1, d_nb, n_nb)


def spread(y, wy, wx, key, key_own, d_own):
    vm = pl.BlockSpec(memory_space=pltpu.VMEM)
    return pl.pallas_call(
        spread_kernel,
        out_shape=(jax.ShapeDtypeStruct((2, 1024, 2 * GRID), BF), jax.ShapeDtypeStruct((2, 2, 64, GRID), F32)),
        in_specs=[vm] * 6,
        out_specs=(vm, vm),
        scratch_shapes=[pltpu.VMEM((SAMPLES // RUN, 160, RUN), BF)] + sort_scratch() + [
            pltpu.VMEM((2, 16 * (66 + WIN), GRID), F32),
            pltpu.VMEM((RUN, GRID), BF),
            pltpu.VMEM((RUN, GRID), BF),
        ],
        compiler_params=pltpu.CompilerParams(vmem_limit_bytes=28 * 2**20),
        cost_estimate=pl.CostEstimate(flops=13 * 10**9, bytes_accessed=4 * 2**20, transcendentals=0),
        name='spread',
    )(y, wy, wx, key, key_own, d_own)


def combine_kernel(gg, ee, tab, maps, dd, out_ref, hbuf, hs, ge, rx, s_all, part, near, far, scale, table,
                   esend, erecv, ssend, srecv, hsend, hrecv, ysend, yrecv, nsend, nrecv):
    row_id = lax.axis_index('rows')
    y_id = lax.axis_index('coil')
    core = row_id % 2
    x_id = row_id // 2
    sib_row = row_id + 1 - 2 * core
    sib = {'rows': sib_row}
    blocks = [row_id, (row_id + 2) % 4]

    barrier = pltpu.get_barrier_semaphore()
    for dev in (sib, {'coil': 1 - y_id}, {'coil': 1 - y_id, 'rows': sib_row}):
        pl.semaphore_signal(barrier, inc=1, device_id=dev, device_id_type=pl.DeviceIdType.MESH)

    def rows_of(a, c):
        return pl.ds(pl.multiple_of(256 * a + 128 * c, 128), 128)

    pl.semaphore_wait(barrier, 3)

    def remote(src, dst, send, recv, dev):
        return pltpu.make_async_remote_copy(src_ref=src, dst_ref=dst, send_sem=send, recv_sem=recv, device_id=dev, device_id_type=pl.DeviceIdType.MESH)

    e_copies = []
    for o in range(2):
        low = o * core + (1 - o) * (1 - core)
        high = o * (1 - core) + (1 - o) * core
        for k, (slot, end, row0) in enumerate(((low, 1, 0), (high, 0, 48))):
            e_copies.append(remote(ee.at[o, :, pl.ds(row0, 16)], rx.at[slot, end], esend.at[2 * o + k], erecv.at[slot, end], sib))
    for cp in e_copies:
        cp.start()
    s_copies = [remote(maps.at[:, :, rows_of(a, 1 - core)], s_all.at[core, a], ssend.at[a], srecv.at[a], sib) for a in range(2)]
    for cp in s_copies:
        cp.start()
    for a in range(2):
        s_all[core, a] = maps[:, :, rows_of(a, core), :]
    row_scale = jnp.broadcast_to(dd[:, pl.ds(pl.multiple_of(y_id * 256, 256), 256)], (128, 256)).T
    scale[...] = row_scale * dd[:, pl.ds(pl.multiple_of(row_id * 128, 128), 128)]
    for hc in range(2):
        cols = pl.ds(pl.multiple_of(x_id * 256 + hc * 128, 128), 128)
        table[hc] = jnp.concatenate([tab[0, cols, :], tab[1, cols, :]], axis=0).T

    def columns(hc, lhs):
        t2 = table[hc]
        prod = jnp.dot(lhs, t2, preferred_element_type=F32)
        n = lhs.shape[0] // 2
        return prod[:n, :128] - prod[n:, 128:], prod[:n, 128:] + prod[n:, :128]

    def transform(hc, o, k):
        for j in range(2):
            rows = slice(512 * k + 256 * j, 512 * k + 256 * j + 256)
            pair = columns(hc, jnp.concatenate([gg[o, rows, :GRID], gg[o, rows, GRID:]], axis=0))
            for e in range(2):
                hs[o, e, rows] = pair[e]

    def take_halos():
        for cp in e_copies:
            cp.wait_send()
        for o in range(2):
            for end in range(2):
                remote(rx.at[o, end], rx.at[o, end], esend.at[2 * o + end], erecv.at[o, end], sib).wait_recv()
                for q in range(2):
                    ge[64 * q + 32 * o + 16 * end:64 * q + 32 * o + 16 * end + 16, :] = (ee[o, q, 16 + 16 * end:32 + 16 * end, :] + rx[o, end, q]).astype(BF)

    def patch(hc):
        return columns(hc, ge[...])

    def piece(hc, o, k):
        return remote(hbuf.at[hc, blocks[o], :, pl.ds(128 * k, 128)], hbuf.at[hc, blocks[o], :, pl.ds(128 * k, 128)], hsend.at[hc, o, k], hrecv.at[hc, o, k], sib)

    h_copies = [[piece(hc, o, k) for o in range(2) for k in range(2)] for hc in range(2)]

    def send(hc, o, k, pair):
        for e in range(2):
            hs[o, e, 1008 * k:1008 * k + 16] = pair[e][32 * o + 16 * k:32 * o + 16 * k + 16]
            for c in range(4):
                hbuf[hc, blocks[o], e, 128 * k:128 * k + 128, 128 * c:128 * c + 128] = hs[o, e, pl.ds(512 * k + c, 128, stride=4), :].astype(BF)
        h_copies[hc][2 * o + k].start()

    def image(hc, a):
        rows = rows_of(a, core)
        cos, sin = tab[0, rows, :], tab[1, rows, :]
        quarter = [slice(256 * p, 256 * p + 256) for p in range(4)]
        top = jnp.concatenate([v[:, q] for q in quarter for v in (cos, -sin)], axis=1)
        bottom = jnp.concatenate([v[:, q] for q in quarter for v in (sin, cos)], axis=1)
        both = jnp.dot(jnp.concatenate([top, bottom], axis=0), hbuf[hc].reshape(2048, 512), preferred_element_type=F32)
        re, im = both[:128], both[128:]
        xr = jnp.zeros((128, 128), F32)
        xi = jnp.zeros((128, 128), F32)
        for c in range(4):
            ir = re[:, 128 * c:128 * c + 128]
            ii = im[:, 128 * c:128 * c + 128]
            sr = s_all[hc, a, 0, c]
            si = s_all[hc, a, 1, c]
            xr = xr + (sr * ir + si * ii)
            xi = xi + (sr * ii - si * ir)
        part[hc, a, 0] = xr
        part[hc, a, 1] = xi

    y_copies = [remote(part.at[hc, 1 - y_id], far.at[core], ysend.at[hc], yrecv.at[core], {'coil': 1 - y_id, 'rows': 2 * x_id + hc}) for hc in range(2)]
    n_copy = remote(part.at[1 - core, y_id], near, nsend.at[0], nrecv.at[0], sib)

    for k in range(2):
        transform(0, 0, k)
    take_halos()
    pair = patch(0)
    for k in range(2):
        send(0, 0, k, pair)
    for k in range(2):
        transform(0, 1, k)
        send(0, 1, k, pair)
    pair = patch(1)
    for k in range(2):
        transform(1, 0, k)
        send(1, 0, k, pair)
    for cp in s_copies + h_copies[0]:
        cp.wait()
    image(0, 1 - y_id)
    y_copies[0].start()
    for k in range(2):
        transform(1, 1, k)
        send(1, 1, k, pair)
    image(0, y_id)
    for cp in h_copies[1]:
        cp.wait()
    image(1, 1 - y_id)
    y_copies[1].start()
    image(1, y_id)
    n_copy.start()
    for cp in y_copies:
        cp.wait_send()
    n_copy.wait()
    mine = pl.ds(pl.multiple_of(128 * core, 128), 128)
    other = pl.ds(pl.multiple_of(128 * (1 - core), 128), 128)
    for e in range(2):
        out_ref[e, mine] = part[core, y_id, e]
        out_ref[e, other] = near[e]
    for k in range(2):
        remote(far.at[k], far.at[k], ysend.at[k], yrecv.at[k], {'coil': 1 - y_id}).wait_recv()
        sl = slice(128 * k, 128 * k + 128)
        for e in range(2):
            out_ref[e, sl] = (out_ref[e, sl] + far[k, e]) * scale[sl]


def combine(gg, ee, tab, maps, dd):
    vm = pl.BlockSpec(memory_space=pltpu.VMEM)
    dma = pltpu.SemaphoreType.DMA
    return pl.pallas_call(
        combine_kernel,
        out_shape=jax.ShapeDtypeStruct((2, 256, 128), F32),
        in_specs=[vm] * 5,
        out_specs=vm,
        scratch_shapes=[
            pltpu.VMEM((2, 4, 2, 256, 512), BF),
            pltpu.VMEM((2, 2, 1024, 128), F32),
            pltpu.VMEM((128, GRID), BF),
            pltpu.VMEM((2, 2, 2, 16, GRID), F32),
            pltpu.VMEM((2, 2, 2, 4, 128, 128), F32),
            pltpu.VMEM((2, 2, 2, 128, 128), F32),
            pltpu.VMEM((2, 128, 128), F32),
            pltpu.VMEM((2, 2, 128, 128), F32),
            pltpu.VMEM((256, 128), F32),
            pltpu.VMEM((2, GRID, 256), BF),
            dma((4,)), dma((2, 2)), dma((2,)), dma((2,)), dma((2, 2, 2)), dma((2, 2, 2)), dma((2,)), dma((2,)), dma((1,)), dma((1,)),
        ],
        compiler_params=pltpu.CompilerParams(vmem_limit_bytes=24 * 2**20, collective_id=0, has_side_effects=True),
        cost_estimate=pl.CostEstimate(flops=7 * 10**9, bytes_accessed=12 * 2**20, transcendentals=0),
        name='combine',
    )(gg, ee, tab, maps, dd)


def solution(mesh):
    def local_part(kspace, weight_row, weight_col, grid_row, grid_col, valid_count, coil_maps, deapod):
        n_img = deapod.shape[0]
        hbm = [pltpu.with_memory_space_constraint(v, pltpu.HBM) for v in (kspace, weight_row, weight_col, grid_row[None], grid_col[None])]
        stacked = exchange(*hbm, valid_count)
        tab = jnp.asarray(tables(n_img))
        gg, ee = spread(*stacked)
        return combine(gg, ee, tab, coil_maps, deapod[None])

    spec_samples = P(None, 'coil', ('slab', 'rows'))
    spec_weights = P(None, ('slab', 'rows'))
    spec_index = P(('slab', 'rows'))
    return jax.shard_map(local_part, mesh=mesh, in_specs=(spec_samples, spec_weights, spec_weights, spec_index, spec_index, spec_index, P(None, 'coil', 'slab', 'rows'), P()), out_specs=P(None, ('slab', 'coil'), 'rows'), check_vma=False)
```
